8 devices in a mesh: rep: 1 (over z), g: 8 (over y, x, core).
Axes of the slice: x: 2, y: 2, z: 1, core: 2. Of those that a mesh axis runs over, the one named last changes fastest.
Arguments:
- hidden: bfloat16 [256, 2048], P(('rep', 'g'))
- cache_lat: bfloat16 [256, 1024, 512], P(('rep', 'g'))
- cache_rope: bfloat16 [256, 1024, 64], P(('rep', 'g'))
- seq_lens: int32 [256], P(('rep', 'g'))
- gain_attn: bfloat16 [2048], replicated
- w_dq: bfloat16 [2048, 768], replicated
- gain_q: bfloat16 [768], replicated
- w_uq: bfloat16 [768, 20, 192], replicated
- w_qr: bfloat16 [768, 20, 64], replicated
- w_dkv: bfloat16 [2048, 576], replicated
- gain_kv: bfloat16 [512], replicated
- w_uk: bfloat16 [512, 20, 192], replicated
- w_uv: bfloat16 [512, 20, 256], replicated
- w_o: bfloat16 [5120, 2048], replicated
- gain_mlp: bfloat16 [2048], replicated
- w_gate: bfloat16 [2048, 10240], P(None, 'g')
- w_up: bfloat16 [2048, 10240], P(None, 'g')
- w_down: bfloat16 [10240, 2048], P('g')
Outputs:
- output 1: bfloat16 [256, 2048], P(('rep', 'g'))
- output 2: bfloat16 [256, 512], P(('rep', 'g'))
- output 3: bfloat16 [256, 64], P(('rep', 'g'))
All inputs are finite; a program needn't handle non-finite values.
Results may differ from the reference program's by a relative error of at most 0.0121209.
Values are sent between devices in bfloat16 or wider.
A program may use at most 1 GiB of HBM per device.

```python
import jax
import jax.numpy as jnp
from jax import lax

BATCH_ROWS = 256
CACHE_LEN = 1024
D_MODEL = 2048
NUM_HEADS = 20
Q_LORA = 768
KV_LORA = 512
ROPE_DIM = 64
NOPE_DIM = 192
V_DIM = 256
FFN_DIM = 10240


def rms_norm(values, gain_vec):
    mean_sq = jnp.mean(jnp.square(values), axis=-1, keepdims=True)
    return values * lax.rsqrt(mean_sq + 1e-6) * gain_vec.astype(jnp.float32)


def apply_rope(values, positions):
    half_dim = values.shape[-1] // 2
    inv_freq = 10000.0 ** (-jnp.arange(half_dim).astype(jnp.float32) / half_dim)
    angles = positions.astype(jnp.float32)[..., None] * inv_freq
    cos_part = jnp.cos(angles)
    sin_part = jnp.sin(angles)
    first_half = values[..., :half_dim]
    second_half = values[..., half_dim:]
    return jnp.concatenate([first_half * cos_part - second_half * sin_part, first_half * sin_part + second_half * cos_part], axis=-1)


def draw_normal(rand_key, arr_shape, spread):
    return (jax.random.normal(rand_key, arr_shape, jnp.float32) * spread).astype(jnp.bfloat16)


def draw_gain(rand_key, length):
    return jax.random.uniform(rand_key, (length,), jnp.float32, 0.5, 1.5).astype(jnp.bfloat16)


def draw_lens(rand_key):
    len_key, pick_key = jax.random.split(rand_key)
    lens_drawn = jax.random.randint(len_key, (BATCH_ROWS,), CACHE_LEN // 4, CACHE_LEN + 1, dtype=jnp.int32)
    pick_order = jax.random.permutation(pick_key, BATCH_ROWS)
    return lens_drawn.at[pick_order[0]].set(CACHE_LEN).at[pick_order[1]].set(CACHE_LEN // 4)


def setup_inputs(seed: int = 0, part: int = 0) -> dict:
    row_keys = jax.random.split(jax.random.fold_in(jax.random.key(seed), part), 4)
    weight_keys = jax.random.split(jax.random.key(seed + 1), 14)
    return {
        "hidden": draw_normal(row_keys[0], (BATCH_ROWS, D_MODEL), 1.0),
        "cache_lat": draw_normal(row_keys[1], (BATCH_ROWS, CACHE_LEN, KV_LORA), 1.0),
        "cache_rope": draw_normal(row_keys[2], (BATCH_ROWS, CACHE_LEN, ROPE_DIM), 1.0),
        "seq_lens": draw_lens(row_keys[3]),
        "gain_attn": draw_gain(weight_keys[0], D_MODEL),
        "w_dq": draw_normal(weight_keys[1], (D_MODEL, Q_LORA), D_MODEL ** -0.5),
        "gain_q": draw_gain(weight_keys[2], Q_LORA),
        "w_uq": draw_normal(weight_keys[3], (Q_LORA, NUM_HEADS, NOPE_DIM), Q_LORA ** -0.5),
        "w_qr": draw_normal(weight_keys[4], (Q_LORA, NUM_HEADS, ROPE_DIM), Q_LORA ** -0.5),
        "w_dkv": draw_normal(weight_keys[5], (D_MODEL, KV_LORA + ROPE_DIM), D_MODEL ** -0.5),
        "gain_kv": draw_gain(weight_keys[6], KV_LORA),
        "w_uk": draw_normal(weight_keys[7], (KV_LORA, NUM_HEADS, NOPE_DIM), (3 * NOPE_DIM) ** -0.5),
        "w_uv": draw_normal(weight_keys[8], (KV_LORA, NUM_HEADS, V_DIM), KV_LORA ** -0.5 * CACHE_LEN ** 0.5 / 4),
        "w_o": draw_normal(weight_keys[9], (NUM_HEADS * V_DIM, D_MODEL), (NUM_HEADS * V_DIM) ** -0.5),
        "gain_mlp": draw_gain(weight_keys[10], D_MODEL),
        "w_gate": draw_normal(weight_keys[11], (D_MODEL, FFN_DIM), D_MODEL ** -0.5),
        "w_up": draw_normal(weight_keys[12], (D_MODEL, FFN_DIM), D_MODEL ** -0.5),
        "w_down": draw_normal(weight_keys[13], (FFN_DIM, D_MODEL), FFN_DIM ** -0.5),
    }


def reference(hidden, cache_lat, cache_rope, seq_lens, gain_attn, w_dq, gain_q, w_uq, w_qr, w_dkv, gain_kv, w_uk, w_uv, w_o, gain_mlp, w_gate, w_up, w_down):
    normed = rms_norm(hidden.astype(jnp.float32), gain_attn).astype(jnp.bfloat16)
    q_in = rms_norm(jnp.dot(normed, w_dq, preferred_element_type=jnp.float32), gain_q).astype(jnp.bfloat16)
    q_nope = jnp.einsum("bq,qhn->bhn", q_in.astype(jnp.float32), w_uq.astype(jnp.float32)).astype(jnp.bfloat16)
    q_rope = apply_rope(jnp.einsum("bq,qhr->bhr", q_in.astype(jnp.float32), w_qr.astype(jnp.float32)), seq_lens[:, None]).astype(jnp.bfloat16)
    kv_raw = jnp.dot(normed, w_dkv, preferred_element_type=jnp.float32)
    new_lat = rms_norm(kv_raw[:, :KV_LORA], gain_kv).astype(jnp.bfloat16)
    new_rope = apply_rope(kv_raw[:, KV_LORA:], seq_lens).astype(jnp.bfloat16)
    q_abs = jnp.einsum("bhn,chn->bhc", q_nope.astype(jnp.float32), w_uk.astype(jnp.float32)).astype(jnp.bfloat16)
    score_scale = (NOPE_DIM + ROPE_DIM) ** -0.5
    key_pos = jnp.arange(CACHE_LEN)

    def one_row(row_data):
        q_lat, q_rot, lat_rows, rope_rows, row_len, lat_new, rope_new = row_data
        past_score = (jnp.einsum("hc,lc->hl", q_lat.astype(jnp.float32), lat_rows.astype(jnp.float32)) + jnp.einsum("hr,lr->hl", q_rot.astype(jnp.float32), rope_rows.astype(jnp.float32))) * score_scale
        own_score = (jnp.einsum("hc,c->h", q_lat.astype(jnp.float32), lat_new.astype(jnp.float32)) + jnp.einsum("hr,r->h", q_rot.astype(jnp.float32), rope_new.astype(jnp.float32))) * score_scale
        past_score = jnp.where(key_pos[None, :] < row_len, past_score, -jnp.inf)
        row_max = jnp.maximum(jnp.max(past_score, axis=-1), own_score)
        past_exp = jnp.exp(past_score - row_max[:, None])
        own_exp = jnp.exp(own_score - row_max)
        row_total = jnp.sum(past_exp, axis=-1) + own_exp
        past_prob = (past_exp / row_total[:, None]).astype(jnp.bfloat16)
        own_prob = (own_exp / row_total).astype(jnp.bfloat16)
        mixed_lat = jnp.einsum("hl,lc->hc", past_prob.astype(jnp.float32), lat_rows.astype(jnp.float32)) + own_prob.astype(jnp.float32)[:, None] * lat_new.astype(jnp.float32)[None, :]
        return mixed_lat.astype(jnp.bfloat16)

    out_lat = lax.map(one_row, (q_abs, q_rope, cache_lat, cache_rope, seq_lens, new_lat, new_rope))
    out_heads = jnp.einsum("bhc,chv->bhv", out_lat.astype(jnp.float32), w_uv.astype(jnp.float32)).astype(jnp.bfloat16)
    attn_out = jnp.dot(out_heads.reshape(BATCH_ROWS, NUM_HEADS * V_DIM), w_o, preferred_element_type=jnp.float32)
    resid_rows = (hidden.astype(jnp.float32) + attn_out).astype(jnp.bfloat16)
    mlp_in = rms_norm(resid_rows.astype(jnp.float32), gain_mlp).astype(jnp.bfloat16)
    gate_proj = jnp.dot(mlp_in, w_gate, preferred_element_type=jnp.float32)
    up_proj = jnp.dot(mlp_in, w_up, preferred_element_type=jnp.float32)
    act_vals = (jax.nn.silu(gate_proj) * up_proj).astype(jnp.bfloat16)
    out_hidden = (resid_rows.astype(jnp.float32) + jnp.dot(act_vals, w_down, preferred_element_type=jnp.float32)).astype(jnp.bfloat16)
    return out_hidden, new_lat, new_rope
```

```python
import jax
import jax.numpy as jnp
from jax import lax
from jax.experimental import pallas as pl
from jax.experimental.pallas import tpu as pltpu
from jax.sharding import PartitionSpec as P


def rms_norm(values, gain_vec):
    mean_sq = jnp.mean(jnp.square(values), axis=-1, keepdims=True)
    return values * lax.rsqrt(mean_sq + 1e-6) * gain_vec.astype(jnp.float32)


def apply_rope(values, positions):
    half_dim = values.shape[-1] // 2
    inv_freq = 10000.0 ** (-jnp.arange(half_dim).astype(jnp.float32) / half_dim)
    angles = positions.astype(jnp.float32)[..., None] * inv_freq
    cos_part = jnp.cos(angles)
    sin_part = jnp.sin(angles)
    first_half = values[..., :half_dim]
    second_half = values[..., half_dim:]
    return jnp.concatenate([first_half * cos_part - second_half * sin_part, first_half * sin_part + second_half * cos_part], axis=-1)


def attention_rows(hidden, cache_lat, cache_rope, seq_lens, gain_attn, w_dq, gain_q, w_uq, w_qr, w_dkv, gain_kv, w_uk, w_uv, w_o):
    kv_dim = w_uk.shape[0]
    cache_len = cache_lat.shape[1]
    score_scale = (w_uq.shape[2] + w_qr.shape[2]) ** -0.5
    normed = rms_norm(hidden.astype(jnp.float32), gain_attn).astype(jnp.bfloat16)
    q_in = rms_norm(jnp.dot(normed, w_dq, preferred_element_type=jnp.float32), gain_q).astype(jnp.bfloat16)
    q_nope = jnp.einsum("bq,qhn->bhn", q_in, w_uq, preferred_element_type=jnp.float32).astype(jnp.bfloat16)
    q_rope = apply_rope(jnp.einsum("bq,qhr->bhr", q_in, w_qr, preferred_element_type=jnp.float32), seq_lens[:, None]).astype(jnp.bfloat16)
    kv_raw = jnp.dot(normed, w_dkv, preferred_element_type=jnp.float32)
    new_lat = rms_norm(kv_raw[:, :kv_dim], gain_kv).astype(jnp.bfloat16)
    new_rope = apply_rope(kv_raw[:, kv_dim:], seq_lens).astype(jnp.bfloat16)
    q_abs = jnp.einsum("bhn,chn->bhc", q_nope, w_uk, preferred_element_type=jnp.float32).astype(jnp.bfloat16)
    past_score = (jnp.einsum("bhc,blc->bhl", q_abs, cache_lat, preferred_element_type=jnp.float32) + jnp.einsum("bhr,blr->bhl", q_rope, cache_rope, preferred_element_type=jnp.float32)) * score_scale
    own_score = (jnp.einsum("bhc,bc->bh", q_abs, new_lat, preferred_element_type=jnp.float32) + jnp.einsum("bhr,br->bh", q_rope, new_rope, preferred_element_type=jnp.float32)) * score_scale
    key_pos = lax.broadcasted_iota(jnp.int32, (1, 1, cache_len), 2)
    past_score = jnp.where(key_pos < seq_lens[:, None, None], past_score, -jnp.inf)
    row_max = jnp.maximum(jnp.max(past_score, axis=-1), own_score)
    past_exp = jnp.exp(past_score - row_max[..., None])
    own_exp = jnp.exp(own_score - row_max)
    row_total = jnp.sum(past_exp, axis=-1) + own_exp
    past_prob = (past_exp / row_total[..., None]).astype(jnp.bfloat16)
    own_prob = (own_exp / row_total).astype(jnp.bfloat16)
    mixed_lat = (jnp.einsum("bhl,blc->bhc", past_prob, cache_lat, preferred_element_type=jnp.float32) + own_prob.astype(jnp.float32)[..., None] * new_lat.astype(jnp.float32)[:, None, :]).astype(jnp.bfloat16)
    out_heads = jnp.einsum("bhc,chv->bhv", mixed_lat, w_uv, preferred_element_type=jnp.float32).astype(jnp.bfloat16)
    attn_out = jnp.dot(out_heads.reshape(out_heads.shape[0], -1), w_o, preferred_element_type=jnp.float32)
    resid_rows = (hidden.astype(jnp.float32) + attn_out).astype(jnp.bfloat16)
    return resid_rows, new_lat, new_rope


MESH = pl.DeviceIdType.MESH


def mlp_kernel(m_ref, h_ref, wg_hbm, wu_hbm, wd_hbm, out_ref, wg, wu, wd, gath, keep, s1_send, s1_recv, s2_send, s2_recv,
               w_sems, ag_send, ag_recv, fw_send, fw_recv, p1_send, p1_recv, p2_send, p2_recv):
    rows = m_ref.shape[0]
    me = lax.axis_index("g")
    core = lax.rem(me, 2)
    chip_x = lax.rem(me // 2, 2)
    chip_y = me // 4
    sibling = me + 1 - 2 * core
    mine = pl.ds(pl.multiple_of(core * rows, rows), rows)
    theirs = pl.ds(pl.multiple_of((1 - core) * rows, rows), rows)

    def peer(rel):
        return me + (rel % 2) * (2 - 4 * chip_x) + (rel // 2) * (4 - 8 * chip_y)

    def gather_copy(rel):
        target = sibling if rel == 0 else peer(rel)
        return pltpu.make_async_remote_copy(m_ref, gath.at[rel, mine], ag_send.at[rel], ag_recv.at[rel], device_id={"g": target}, device_id_type=MESH)

    def forward_copy(rel):
        return pltpu.make_async_remote_copy(gath.at[rel, mine], gath.at[rel, mine], fw_send.at[rel], fw_recv.at[rel], device_id={"g": sibling}, device_id_type=MESH)

    def pair_copy(rel):
        return pltpu.make_async_remote_copy(s1_send.at[rel], s1_recv.at[rel], p1_send.at[rel], p1_recv.at[rel], device_id={"g": sibling}, device_id_type=MESH)

    def chip_copy(rel):
        return pltpu.make_async_remote_copy(s2_send.at[rel], s2_recv.at[rel], p2_send.at[rel], p2_recv.at[rel], device_id={"g": peer(rel)}, device_id_type=MESH)

    loads = [pltpu.make_async_copy(src, dst, w_sems.at[k]) for k, (src, dst) in enumerate(((wg_hbm, wg), (wu_hbm, wu), (wd_hbm, wd)))]
    for load in loads:
        load.start()

    barrier = pltpu.get_barrier_semaphore()
    for target in (sibling, peer(1), peer(2), peer(3)):
        pl.semaphore_signal(barrier, inc=1, device_id={"g": target}, device_id_type=MESH)
    pl.semaphore_wait(barrier, 4)

    for rel in (1, 2, 3, 0):
        gather_copy(rel).start()
    gath[0, mine] = m_ref[...]
    for rel in (1, 2):
        gather_copy(rel).wait_recv()
        forward_copy(rel).start()

    def finish_pair(rel):
        pair_copy(rel).wait_recv()
        keep[rel] = keep[rel] + s1_recv[rel]

        @pl.when(rel > 0)
        def _():
            s2_send[rel] = keep[rel].astype(jnp.bfloat16)
            chip_copy(rel).start()

    for load in loads:
        load.wait()

    def block(step, _):
        rel = lax.rem(step + 1, 4)

        @pl.when(step == 1)
        def _():
            gather_copy(3).wait_recv()
            forward_copy(3).start()

        @pl.when(step < 3)
        def _():
            forward_recv = pltpu.make_async_remote_copy(gath.at[rel, theirs], gath.at[rel, theirs], fw_send.at[rel], fw_recv.at[rel], device_id={"g": sibling}, device_id_type=MESH)
            forward_recv.wait_recv()

        @pl.when(step == 3)
        def _():
            pltpu.make_async_remote_copy(m_ref, gath.at[0, theirs], ag_send.at[0], ag_recv.at[0], device_id={"g": sibling}, device_id_type=MESH).wait_recv()

        block_rows = gath[rel]
        gate = jnp.dot(block_rows, wg[...], preferred_element_type=jnp.float32)
        up = jnp.dot(block_rows, wu[...], preferred_element_type=jnp.float32)
        act = (jax.nn.silu(gate) * up).astype(jnp.bfloat16)

        @pl.when(step > 0)
        def _():
            finish_pair(step)

        part = jnp.dot(act, wd[...], preferred_element_type=jnp.float32)
        low, high = part[:rows], part[rows:]
        is_low = core == 0
        keep[rel] = jnp.where(is_low, low, high)
        s1_send[rel] = jnp.where(is_low, high, low)
        pair_copy(rel).start()
        return 0

    lax.fori_loop(0, 4, block, 0)
    finish_pair(0)
    total = h_ref[...].astype(jnp.float32) + keep[0]
    for rel in (1, 2, 3):
        chip_copy(rel).wait_recv()
        total = total + s2_recv[rel].astype(jnp.float32)
    out_ref[...] = total.astype(jnp.bfloat16)
    for rel in range(4):
        gather_copy(rel).wait_send()
        pair_copy(rel).wait_send()
    for rel in (1, 2, 3):
        forward_copy(rel).wait_send()
        chip_copy(rel).wait_send()


def mlp_call(m, h, w_gate, w_up, w_down):
    rows, width = m.shape
    cols = w_gate.shape[1]
    vmem = pl.BlockSpec(memory_space=pltpu.VMEM)
    hbm = pl.BlockSpec(memory_space=pl.ANY)
    dma = pltpu.SemaphoreType.DMA
    return pl.pallas_call(
        mlp_kernel,
        out_shape=jax.ShapeDtypeStruct((rows, width), jnp.bfloat16),
        in_specs=[vmem, vmem, hbm, hbm, hbm],
        out_specs=vmem,
        scratch_shapes=[
            pltpu.VMEM((width, cols), jnp.bfloat16),
            pltpu.VMEM((width, cols), jnp.bfloat16),
            pltpu.VMEM((cols, width), jnp.bfloat16),
            pltpu.VMEM((4, 2 * rows, width), jnp.bfloat16),
            pltpu.VMEM((4, rows, width), jnp.float32),
            pltpu.VMEM((4, rows, width), jnp.float32),
            pltpu.VMEM((4, rows, width), jnp.float32),
            pltpu.VMEM((4, rows, width), jnp.bfloat16),
            pltpu.VMEM((4, rows, width), jnp.bfloat16),
            dma((3,)), dma((4,)), dma((4,)), dma((4,)), dma((4,)), dma((4,)), dma((4,)), dma((4,)), dma((4,)),
        ],
        compiler_params=pltpu.CompilerParams(collective_id=0, has_side_effects=True, vmem_limit_bytes=48 * 1024 * 1024),
        name="mlp_exchange",
    )(m, h, w_gate, w_up, w_down)


def solution(mesh):
    row_spec = P(("rep", "g"))
    full_spec = P()
    in_specs = (row_spec, row_spec, row_spec, row_spec, full_spec, full_spec, full_spec, full_spec, full_spec, full_spec, full_spec, full_spec, full_spec, full_spec, full_spec, P(None, "g"), P(None, "g"), P("g", None))

    def local_step(hidden, cache_lat, cache_rope, seq_lens, gain_attn, w_dq, gain_q, w_uq, w_qr, w_dkv, gain_kv, w_uk, w_uv, w_o, gain_mlp, w_gate, w_up, w_down):
        resid_rows, new_lat, new_rope = attention_rows(hidden, cache_lat, cache_rope, seq_lens, gain_attn, w_dq, gain_q, w_uq, w_qr, w_dkv, gain_kv, w_uk, w_uv, w_o)
        mlp_in = rms_norm(resid_rows.astype(jnp.float32), gain_mlp).astype(jnp.bfloat16)
        out_hidden = mlp_call(mlp_in, resid_rows, w_gate, w_up, w_down)
        return out_hidden, new_lat, new_rope

    return jax.shard_map(local_step, mesh=mesh, in_specs=in_specs, out_specs=(row_spec, row_spec, row_spec), check_vma=False)
```

```python
import jax
import jax.numpy as jnp
from jax import lax
from jax.experimental import pallas as pl
from jax.experimental.pallas import tpu as pltpu
from jax.sharding import PartitionSpec as P


HEADS = 20
HEAD_PAD = 24
RING = 12
GROUP = 4


def attn_kernel(lens_ref, hid_ref, ga_ref, gq_ref, gkv_ref, gm_ref, lat_hbm, rope_hbm, wdq_hbm, wdkv_hbm, wqr_hbm, wuq_hbm, wuk_hbm, wuv_hbm, wo_hbm,
                resid_ref, mlp_ref, newlat_ref, newrope_ref,
                wdq, wdkv, wqr, wuq, wuk, wuv, wo, lat_buf, rope_buf, q_scr, qr_scr, o_scr, nl_scr, nr_scr, heads_scr,
                w_sems, o_sems, lat_sems, rope_sems):
    rows = hid_ref.shape[0]
    kv_dim = lat_buf.shape[2]
    rope_dim = rope_buf.shape[1]
    cache_len = lat_buf.shape[1]
    nope_dim = wuk.shape[1]
    v_dim = wuv.shape[2]
    half = rope_dim // 2
    f32, bf16 = jnp.float32, jnp.bfloat16
    nt = (((1,), (1,)), ((), ()))

    early = [pltpu.make_async_copy(src, dst, w_sems.at[k]) for k, (src, dst) in enumerate(((wdq_hbm, wdq), (wdkv_hbm, wdkv), (wqr_hbm, wqr), (wuq_hbm, wuq), (wuk_hbm, wuk)))]
    for copy in early:
        copy.start()

    def lat_copy(row, slot):
        count = pl.multiple_of(((lens_ref[row] + 15) // 16) * 16, 16)
        return pltpu.make_async_copy(lat_hbm.at[row, pl.ds(0, count)], lat_buf.at[slot, pl.ds(0, count)], lat_sems.at[slot])

    def rope_copy(row, slot):
        return pltpu.make_async_copy(rope_hbm.at[row], rope_buf.at[slot], rope_sems.at[slot])

    def start_row(row, slot):
        lat_copy(row, slot).start()
        rope_copy(row, slot).start()

    def uv_copy(head):
        return pltpu.make_async_copy(wuv_hbm.at[head], wuv.at[head], o_sems.at[0])

    wo_rows = wo.shape[0] // rows

    def wo_copy(part):
        span = pl.ds(pl.multiple_of(part * wo_rows, 32), wo_rows)
        return pltpu.make_async_copy(wo_hbm.at[span], wo.at[span], o_sems.at[1])

    def clear_and_start(slot, _):
        lat_buf[slot, pl.ds(256, cache_len - 256)] = jnp.zeros((cache_len - 256, kv_dim), bf16)
        start_row(slot, slot)
        return 0

    lax.fori_loop(0, RING, clear_and_start, 0)

    def norm(values, gain_ref):
        mean_sq = jnp.mean(values * values, axis=-1, keepdims=True)
        return values * lax.rsqrt(mean_sq + 1e-6) * gain_ref[...].astype(f32)

    row_id = lax.broadcasted_iota(jnp.int32, (rows, 128), 0)
    position = jnp.zeros((rows, 128), jnp.int32)
    for row in range(rows):
        position = jnp.where(row_id == row, lens_ref[row], position)
    lane = lax.broadcasted_iota(jnp.int32, (rows, 128), 1)
    freq_id = lane & (half - 1)
    inv_freq = jnp.exp(freq_id.astype(f32) * (-jnp.log(jnp.float32(10000.0)) / half))
    angle = position.astype(f32) * inv_freq
    first_half = (lane & half) == 0
    cos_part = jnp.cos(angle)
    sin_part = jnp.where(first_half, -jnp.sin(angle), jnp.sin(angle))

    def rotate(values):
        swapped = jnp.where(first_half, pltpu.roll(values, 128 - half, 1), pltpu.roll(values, half, 1))
        return values * cos_part + swapped * sin_part

    hidden = hid_ref[...].astype(f32)
    normed = norm(hidden, ga_ref).astype(bf16)
    q_scr[...] = jnp.zeros_like(q_scr)
    qr_scr[...] = jnp.zeros_like(qr_scr)

    early[0].wait()
    q_in = norm(jnp.dot(normed, wdq[...], preferred_element_type=f32), gq_ref).astype(bf16)
    early[1].wait()
    kv_raw = lax.dot_general(normed, wdkv[...], nt, preferred_element_type=f32)
    new_lat = norm(kv_raw[:, :kv_dim], gkv_ref).astype(bf16)
    newlat_ref[...] = new_lat
    nl_scr[...] = new_lat.astype(f32)
    kv_rope = jnp.concatenate([kv_raw[:, kv_dim:], jnp.zeros((rows, 128 - rope_dim), f32)], axis=1)
    new_rope = rotate(kv_rope).astype(bf16)
    newrope_ref[...] = new_rope[:, :rope_dim]
    low_lanes = lane < rope_dim
    nr_scr[...] = jnp.where(low_lanes, new_rope.astype(f32), 0.0)

    early[2].wait()
    for pair in range(HEADS // 2):
        raw = lax.dot_general(q_in, wqr[pl.ds(pair * 128, 128)], nt, preferred_element_type=f32)
        turned = rotate(raw).astype(bf16).astype(f32)
        qr_scr[pl.ds(2 * pair, rows, stride=HEAD_PAD), :] = turned
        qr_scr[pl.ds(2 * pair + 1, rows, stride=HEAD_PAD), :] = pltpu.roll(turned, rope_dim, 1)

    early[3].wait()
    early[4].wait()
    for quad in range(HEADS // 4):
        q_nope = lax.dot_general(q_in, wuq[pl.ds(quad * 4 * nope_dim, 4 * nope_dim)], nt, preferred_element_type=f32)
        for sub in range(4):
            head = quad * 4 + sub
            one = q_nope[:, sub * nope_dim:(sub + 1) * nope_dim].astype(bf16)
            q_abs = jnp.dot(one, wuk[head], preferred_element_type=f32).astype(bf16).astype(f32)
            for col in range(kv_dim // 128):
                q_scr[col, pl.ds(head, rows, stride=HEAD_PAD), :] = q_abs[:, col * 128:(col + 1) * 128]

    scale = (nope_dim + rope_dim) ** -0.5
    key_pos = lax.broadcasted_iota(jnp.int32, (HEAD_PAD, cache_len), 1)

    def attend(row, slot):
        head_rows = pl.ds(pl.multiple_of(row * HEAD_PAD, 8), HEAD_PAD)
        q_cols = [q_scr[col, head_rows, :] for col in range(kv_dim // 128)]
        q_lat = jnp.concatenate(q_cols, axis=1)
        q_rope = qr_scr[head_rows, :]
        lat = lat_buf[slot]
        own_lat = nl_scr[pl.ds(row, 1), :]
        score = lax.dot_general(q_lat.astype(bf16), lat, nt, preferred_element_type=f32)
        score = score + jnp.dot(q_rope[:, :rope_dim].astype(bf16), rope_buf[slot], preferred_element_type=f32)
        score = jnp.where(key_pos < lens_ref[row], score * scale, -jnp.inf)
        own = jnp.sum(q_lat * own_lat, axis=-1, keepdims=True) + jnp.sum(q_rope * nr_scr[pl.ds(row, 1), :], axis=-1, keepdims=True)
        own = own * scale
        top = jnp.maximum(jnp.max(score, axis=-1, keepdims=True), own)
        weight = jnp.exp(score - top)
        own_weight = jnp.exp(own - top)
        total = jnp.sum(weight, axis=-1, keepdims=True) + own_weight
        prob = (weight / total).astype(bf16)
        own_prob = (own_weight / total).astype(bf16).astype(f32)
        mixed = jnp.dot(prob, lat, preferred_element_type=f32) + own_prob * own_lat
        mixed = mixed.astype(bf16).astype(f32)
        for col in range(kv_dim // 128):
            o_scr[col, head_rows, :] = mixed[:, col * 128:(col + 1) * 128]

    def group_step(group, _):
        base = group * GROUP
        for sub in range(GROUP):
            part = base + sub
            wo_copy(part).start()

            @pl.when(part < HEADS)
            def _():
                uv_copy(part).start()
        slots = [lax.rem(base, RING) + sub for sub in range(GROUP)]
        for sub in range(GROUP):
            lat_copy(base + sub, slots[sub]).wait()
            rope_copy(base + sub, slots[sub]).wait()
        for sub in range(GROUP):
            attend(base + sub, slots[sub])

        @pl.when(base + RING < rows)
        def _():
            for sub in range(GROUP):
                start_row(base + RING + sub, slots[sub])
        return 0

    lax.fori_loop(0, rows // GROUP, group_step, 0)

    pltpu.make_async_copy(wuv_hbm, wuv, o_sems.at[0]).wait()
    for head in range(HEADS):
        cols = [o_scr[col, pl.ds(head, rows, stride=HEAD_PAD), :] for col in range(kv_dim // 128)]
        mixed = jnp.concatenate(cols, axis=1).astype(bf16)
        heads_scr[:, head * v_dim:(head + 1) * v_dim] = jnp.dot(mixed, wuv[head], preferred_element_type=f32).astype(bf16)
    pltpu.make_async_copy(wo_hbm, wo, o_sems.at[1]).wait()
    attn_out = jnp.dot(heads_scr[...], wo[...], preferred_element_type=f32)
    resid = (hid_ref[...].astype(f32) + attn_out).astype(bf16)
    resid_ref[...] = resid
    mlp_ref[...] = norm(resid.astype(f32), gm_ref).astype(bf16)


def attn_call(hidden, cache_lat, cache_rope, seq_lens, gain_attn, w_dq, gain_q, w_uq, w_qr, w_dkv, gain_kv, w_uk, w_uv, w_o, gain_mlp):
    rows, width = hidden.shape
    cache_len, kv_dim = cache_lat.shape[1:]
    rope_dim = cache_rope.shape[2]
    q_dim, heads, nope_dim = w_uq.shape
    v_dim = w_uv.shape[2]
    bf16, f32 = jnp.bfloat16, jnp.float32
    vmem = pl.BlockSpec(memory_space=pltpu.VMEM)
    smem = pl.BlockSpec(memory_space=pltpu.SMEM)
    hbm = pl.BlockSpec(memory_space=pl.ANY)
    dma = pltpu.SemaphoreType.DMA
    rope_keys = jnp.swapaxes(cache_rope, 1, 2)
    dkv_t = w_dkv.T
    qr_t = jnp.transpose(w_qr, (1, 2, 0)).reshape(heads * rope_dim, q_dim)
    uq_t = jnp.transpose(w_uq, (1, 2, 0)).reshape(heads * nope_dim, q_dim)
    uk_t = jnp.transpose(w_uk, (1, 2, 0))
    uv_t = jnp.swapaxes(w_uv, 0, 1)
    return pl.pallas_call(
        attn_kernel,
        out_shape=(
            jax.ShapeDtypeStruct((rows, width), bf16),
            jax.ShapeDtypeStruct((rows, width), bf16),
            jax.ShapeDtypeStruct((rows, kv_dim), bf16),
            jax.ShapeDtypeStruct((rows, rope_dim), bf16),
        ),
        in_specs=[smem, vmem, vmem, vmem, vmem, vmem] + [hbm] * 9,
        out_specs=(vmem, vmem, vmem, vmem),
        scratch_shapes=[
            pltpu.VMEM(w_dq.shape, bf16),
            pltpu.VMEM(dkv_t.shape, bf16),
            pltpu.VMEM(qr_t.shape, bf16),
            pltpu.VMEM(uq_t.shape, bf16),
            pltpu.VMEM(uk_t.shape, bf16),
            pltpu.VMEM(uv_t.shape, bf16),
            pltpu.VMEM(w_o.shape, bf16),
            pltpu.VMEM((RING, cache_len, kv_dim), bf16),
            pltpu.VMEM((RING, rope_dim, cache_len), bf16),
            pltpu.VMEM((kv_dim // 128, rows * HEAD_PAD, 128), f32),
            pltpu.VMEM((rows * HEAD_PAD, 128), f32),
            pltpu.VMEM((kv_dim // 128, rows * HEAD_PAD, 128), f32),
            pltpu.VMEM((rows, kv_dim), f32),
            pltpu.VMEM((rows, 128), f32),
            pltpu.VMEM((rows, heads * v_dim), bf16),
            dma((5,)), dma((2,)), dma((RING,)), dma((RING,)),
        ],
        compiler_params=pltpu.CompilerParams(vmem_limit_bytes=67043328),
        name="attention",
    )(seq_lens, hidden, gain_attn, gain_q, gain_kv, gain_mlp, cache_lat, rope_keys, w_dq, dkv_t, qr_t, uq_t, uk_t, uv_t, w_o)


MESH = pl.DeviceIdType.MESH


def mlp_kernel(m_ref, h_ref, wg_hbm, wu_hbm, wd_hbm, out_ref, wg, wu, wd, gath, keep, s1_send, s1_recv, s2_send, s2_recv,
               w_sems, ag_send, ag_recv, fw_send, fw_recv, p1_send, p1_recv, p2_send, p2_recv):
    rows = m_ref.shape[0]
    me = lax.axis_index("g")
    core = lax.rem(me, 2)
    chip_x = lax.rem(me // 2, 2)
    chip_y = me // 4
    sibling = me + 1 - 2 * core
    mine = pl.ds(pl.multiple_of(core * rows, rows), rows)
    theirs = pl.ds(pl.multiple_of((1 - core) * rows, rows), rows)

    def peer(rel):
        return me + (rel % 2) * (2 - 4 * chip_x) + (rel // 2) * (4 - 8 * chip_y)

    def gather_copy(rel):
        target = sibling if rel == 0 else peer(rel)
        return pltpu.make_async_remote_copy(m_ref, gath.at[rel, mine], ag_send.at[rel], ag_recv.at[rel], device_id={"g": target}, device_id_type=MESH)

    def forward_copy(rel):
        return pltpu.make_async_remote_copy(gath.at[rel, mine], gath.at[rel, mine], fw_send.at[rel], fw_recv.at[rel], device_id={"g": sibling}, device_id_type=MESH)

    def pair_copy(rel):
        return pltpu.make_async_remote_copy(s1_send.at[rel], s1_recv.at[rel], p1_send.at[rel], p1_recv.at[rel], device_id={"g": sibling}, device_id_type=MESH)

    def chip_copy(rel):
        return pltpu.make_async_remote_copy(s2_send.at[rel], s2_recv.at[rel], p2_send.at[rel], p2_recv.at[rel], device_id={"g": peer(rel)}, device_id_type=MESH)

    loads = [pltpu.make_async_copy(src, dst, w_sems.at[k]) for k, (src, dst) in enumerate(((wg_hbm, wg), (wu_hbm, wu), (wd_hbm, wd)))]
    for load in loads:
        load.start()

    barrier = pltpu.get_barrier_semaphore()
    for target in (sibling, peer(1), peer(2), peer(3)):
        pl.semaphore_signal(barrier, inc=1, device_id={"g": target}, device_id_type=MESH)
    pl.semaphore_wait(barrier, 4)

    for rel in (1, 2, 3, 0):
        gather_copy(rel).start()
    gath[0, mine] = m_ref[...]
    for rel in (1, 2):
        gather_copy(rel).wait_recv()
        forward_copy(rel).start()

    def finish_pair(rel):
        pair_copy(rel).wait_recv()
        keep[rel] = keep[rel] + s1_recv[rel]

        @pl.when(rel > 0)
        def _():
            s2_send[rel] = keep[rel].astype(jnp.bfloat16)
            chip_copy(rel).start()

    for load in loads:
        load.wait()

    def block(step, _):
        rel = lax.rem(step + 1, 4)

        @pl.when(step == 1)
        def _():
            gather_copy(3).wait_recv()
            forward_copy(3).start()

        @pl.when(step < 3)
        def _():
            forward_recv = pltpu.make_async_remote_copy(gath.at[rel, theirs], gath.at[rel, theirs], fw_send.at[rel], fw_recv.at[rel], device_id={"g": sibling}, device_id_type=MESH)
            forward_recv.wait_recv()

        @pl.when(step == 3)
        def _():
            pltpu.make_async_remote_copy(m_ref, gath.at[0, theirs], ag_send.at[0], ag_recv.at[0], device_id={"g": sibling}, device_id_type=MESH).wait_recv()

        block_rows = gath[rel]
        gate = jnp.dot(block_rows, wg[...], preferred_element_type=jnp.float32)
        up = jnp.dot(block_rows, wu[...], preferred_element_type=jnp.float32)
        act = (jax.nn.silu(gate) * up).astype(jnp.bfloat16)

        @pl.when(step > 0)
        def _():
            finish_pair(step)

        part = jnp.dot(act, wd[...], preferred_element_type=jnp.float32)
        low, high = part[:rows], part[rows:]
        is_low = core == 0
        keep[rel] = jnp.where(is_low, low, high)
        s1_send[rel] = jnp.where(is_low, high, low)
        pair_copy(rel).start()
        return 0

    lax.fori_loop(0, 4, block, 0)
    finish_pair(0)
    total = h_ref[...].astype(jnp.float32) + keep[0]
    for rel in (1, 2, 3):
        chip_copy(rel).wait_recv()
        total = total + s2_recv[rel].astype(jnp.float32)
    out_ref[...] = total.astype(jnp.bfloat16)
    for rel in range(4):
        gather_copy(rel).wait_send()
        pair_copy(rel).wait_send()
    for rel in (1, 2, 3):
        forward_copy(rel).wait_send()
        chip_copy(rel).wait_send()


def mlp_call(m, h, w_gate, w_up, w_down):
    rows, width = m.shape
    cols = w_gate.shape[1]
    vmem = pl.BlockSpec(memory_space=pltpu.VMEM)
    hbm = pl.BlockSpec(memory_space=pl.ANY)
    dma = pltpu.SemaphoreType.DMA
    return pl.pallas_call(
        mlp_kernel,
        out_shape=jax.ShapeDtypeStruct((rows, width), jnp.bfloat16),
        in_specs=[vmem, vmem, hbm, hbm, hbm],
        out_specs=vmem,
        scratch_shapes=[
            pltpu.VMEM((width, cols), jnp.bfloat16),
            pltpu.VMEM((width, cols), jnp.bfloat16),
            pltpu.VMEM((cols, width), jnp.bfloat16),
            pltpu.VMEM((4, 2 * rows, width), jnp.bfloat16),
            pltpu.VMEM((4, rows, width), jnp.float32),
            pltpu.VMEM((4, rows, width), jnp.float32),
            pltpu.VMEM((4, rows, width), jnp.float32),
            pltpu.VMEM((4, rows, width), jnp.bfloat16),
            pltpu.VMEM((4, rows, width), jnp.bfloat16),
            dma((3,)), dma((4,)), dma((4,)), dma((4,)), dma((4,)), dma((4,)), dma((4,)), dma((4,)), dma((4,)),
        ],
        compiler_params=pltpu.CompilerParams(collective_id=0, has_side_effects=True, vmem_limit_bytes=48 * 1024 * 1024),
        name="mlp_exchange",
    )(m, h, w_gate, w_up, w_down)


def solution(mesh):
    row_spec = P(("rep", "g"))
    full_spec = P()
    in_specs = (row_spec, row_spec, row_spec, row_spec, full_spec, full_spec, full_spec, full_spec, full_spec, full_spec, full_spec, full_spec, full_spec, full_spec, full_spec, P(None, "g"), P(None, "g"), P("g", None))

    def local_step(hidden, cache_lat, cache_rope, seq_lens, gain_attn, w_dq, gain_q, w_uq, w_qr, w_dkv, gain_kv, w_uk, w_uv, w_o, gain_mlp, w_gate, w_up, w_down):
        resid_rows, mlp_in, new_lat, new_rope = attn_call(hidden, cache_lat, cache_rope, seq_lens, gain_attn, w_dq, gain_q, w_uq, w_qr, w_dkv, gain_kv, w_uk, w_uv, w_o, gain_mlp)
        out_hidden = mlp_call(mlp_in, resid_rows, w_gate, w_up, w_down)
        return out_hidden, new_lat, new_rope

    return jax.shard_map(local_step, mesh=mesh, in_specs=in_specs, out_specs=(row_spec, row_spec, row_spec), check_vma=False)
```

```python
import functools

import jax
import jax.numpy as jnp
from jax import lax
from jax.experimental import pallas as pl
from jax.experimental.pallas import tpu as pltpu
from jax.sharding import PartitionSpec as P


HEADS = 20
HEAD_PAD = 24
RING = 12
GROUP = 4
WO_PARTS = 20
WO_EARLY = 6
WO_STEP = 2


def attn_kernel(lens_ref, hid_ref, ga_ref, gq_ref, gkv_ref, gm_ref, lat_hbm, rope_hbm, wdq_hbm, wdkv_hbm, wqr_hbm, wuq_hbm, wuk_hbm, wuv_hbm, wo_hbm,
                resid_ref, mlp_ref, newlat_ref, newrope_ref,
                wdq, wdkv, wqr, wuq, wuk, wuv, wo, lat_buf, rope_buf, q_scr, qr_scr, o_scr, nl_scr, nr_scr, heads_scr, s_scr,
                order, fill, w_sems, o_sems, lat_sems, rope_sems):
    rows = hid_ref.shape[0]
    kv_dim = lat_buf.shape[2]
    rope_dim = rope_buf.shape[1]
    cache_len = lat_buf.shape[1]
    nope_dim = wuk.shape[1]
    v_dim = wuv.shape[2]
    half = rope_dim // 2
    groups = rows // GROUP
    f32, bf16 = jnp.float32, jnp.bfloat16
    nt = (((1,), (1,)), ((), ()))

    early = [pltpu.make_async_copy(src, dst, w_sems.at[k]) for k, (src, dst) in enumerate(((wdq_hbm, wdq), (wdkv_hbm, wdkv), (wqr_hbm, wqr), (wuq_hbm, wuq), (wuk_hbm, wuk)))]
    for copy in early:
        copy.start()

    def bucket(row):
        return (lens_ref[row] + 127) // 128

    for k in range(9):
        fill[k] = 0

    def count(row, _):
        k = bucket(row)
        fill[k] = fill[k] + 1
        return 0

    lax.fori_loop(0, rows, count, 0)
    running = jnp.int32(0)
    for k in range(9):
        size = fill[k]
        fill[k] = running
        running = running + size

    def place(row, _):
        k = bucket(row)
        order[fill[k]] = row
        fill[k] = fill[k] + 1
        return 0

    lax.fori_loop(0, rows, place, 0)

    def lat_copy(row, slot):
        count16 = pl.multiple_of(((lens_ref[row] + 15) // 16) * 16, 16)
        return pltpu.make_async_copy(lat_hbm.at[row, pl.ds(0, count16)], lat_buf.at[slot, pl.ds(0, count16)], lat_sems.at[slot])

    def rope_copy(row, slot):
        return pltpu.make_async_copy(rope_hbm.at[row], rope_buf.at[slot], rope_sems.at[slot])

    def start_place(place_id, slot):
        row = order[place_id]
        lat_copy(row, slot).start()
        rope_copy(row, slot).start()

    wo_rows = wo.shape[0] // WO_PARTS

    def wo_copy(part):
        span = pl.ds(pl.multiple_of(part * wo_rows, 32), wo_rows)
        return pltpu.make_async_copy(wo_hbm.at[span], wo.at[span], o_sems.at[1])

    def clear_and_start(slot, _):
        lat_buf[slot, pl.ds(256, cache_len - 256)] = jnp.zeros((cache_len - 256, kv_dim), bf16)
        start_place(slot, slot)
        return 0

    lax.fori_loop(0, RING, clear_and_start, 0)
    uv_copy = pltpu.make_async_copy(wuv_hbm, wuv, o_sems.at[0])
    uv_copy.start()
    for part in range(WO_EARLY):
        wo_copy(part).start()

    def norm(values, gain_ref):
        mean_sq = jnp.mean(values * values, axis=-1, keepdims=True)
        return values * lax.rsqrt(mean_sq + 1e-6) * gain_ref[...].astype(f32)

    row_id = lax.broadcasted_iota(jnp.int32, (rows, 128), 0)
    position = jnp.zeros((rows, 128), jnp.int32)
    for row in range(rows):
        position = jnp.where(row_id == row, lens_ref[row], position)
    lane = lax.broadcasted_iota(jnp.int32, (rows, 128), 1)
    freq_id = lane & (half - 1)
    inv_freq = jnp.exp(freq_id.astype(f32) * (-jnp.log(jnp.float32(10000.0)) / half))
    angle = position.astype(f32) * inv_freq
    first_half = (lane & half) == 0
    cos_part = jnp.cos(angle)
    sin_part = jnp.where(first_half, -jnp.sin(angle), jnp.sin(angle))

    def rotate(values):
        swapped = jnp.where(first_half, pltpu.roll(values, 128 - half, 1), pltpu.roll(values, half, 1))
        return values * cos_part + swapped * sin_part

    hidden = hid_ref[...].astype(f32)
    normed = norm(hidden, ga_ref).astype(bf16)
    q_scr[...] = jnp.zeros_like(q_scr)
    qr_scr[...] = jnp.zeros_like(qr_scr)

    early[0].wait()
    q_raw = jnp.dot(normed, wdq[...], preferred_element_type=f32)
    early[1].wait()
    kv_raw = lax.dot_general(normed, wdkv[...], nt, preferred_element_type=f32)
    q_in = norm(q_raw, gq_ref).astype(bf16)
    early[2].wait()
    rope_raw = lax.dot_general(q_in, wqr[...], nt, preferred_element_type=f32)
    new_lat = norm(kv_raw[:, :kv_dim], gkv_ref).astype(bf16)
    newlat_ref[...] = new_lat
    nl_scr[...] = new_lat.astype(f32)
    kv_rope = jnp.concatenate([kv_raw[:, kv_dim:], jnp.zeros((rows, 128 - rope_dim), f32)], axis=1)
    new_rope = rotate(kv_rope).astype(bf16)
    newrope_ref[...] = new_rope[:, :rope_dim]
    nr_scr[...] = jnp.where(lane < rope_dim, new_rope.astype(f32), 0.0)

    def nope_quad(quad):
        return lax.dot_general(q_in, wuq[pl.ds(quad * 4 * nope_dim, 4 * nope_dim)], nt, preferred_element_type=f32)

    def absorb_quad(quad, q_nope):
        for sub in range(4):
            head = quad * 4 + sub
            one = q_nope[:, sub * nope_dim:(sub + 1) * nope_dim].astype(bf16)
            q_abs = jnp.dot(one, wuk[head], preferred_element_type=f32).astype(bf16).astype(f32)
            for col in range(kv_dim // 128):
                q_scr[col, pl.ds(head, rows, stride=HEAD_PAD), :] = q_abs[:, col * 128:(col + 1) * 128]

    early[3].wait()
    quads = HEADS // 4
    ahead = nope_quad(0)
    for pair in range(HEADS // 2):
        turned = rotate(rope_raw[:, pair * 128:(pair + 1) * 128]).astype(bf16).astype(f32)
        qr_scr[pl.ds(2 * pair, rows, stride=HEAD_PAD), :] = turned
        qr_scr[pl.ds(2 * pair + 1, rows, stride=HEAD_PAD), :] = pltpu.roll(turned, rope_dim, 1)
    for quad in range(quads):
        now = ahead
        if quad + 1 < quads:
            ahead = nope_quad(quad + 1)
        if quad == 0:
            early[4].wait()
        absorb_quad(quad, now)

    scale = (nope_dim + rope_dim) ** -0.5

    def head_rows(row):
        return pl.ds(pl.multiple_of(row * HEAD_PAD, 8), HEAD_PAD)

    def query(row):
        return jnp.concatenate([q_scr[col, head_rows(row), :] for col in range(kv_dim // 128)], axis=1)

    def score_part(row, slot, span):
        lat = lat_buf[slot, pl.ds(0, span)]
        score = lax.dot_general(query(row).astype(bf16), lat, nt, preferred_element_type=f32)
        q_rope = qr_scr[head_rows(row), :][:, :rope_dim].astype(bf16)
        return score + jnp.dot(q_rope, rope_buf[slot, :, pl.ds(0, span)], preferred_element_type=f32)

    def soft_part(row, score):
        key_pos = lax.broadcasted_iota(jnp.int32, score.shape, 1)
        score = jnp.where(key_pos < lens_ref[row], score * scale, -jnp.inf)
        q_rope = qr_scr[head_rows(row), :]
        own = jnp.sum(query(row) * nl_scr[pl.ds(row, 1), :], axis=-1, keepdims=True) + jnp.sum(q_rope * nr_scr[pl.ds(row, 1), :], axis=-1, keepdims=True)
        own = own * scale
        top = jnp.maximum(jnp.max(score, axis=-1, keepdims=True), own)
        weight = jnp.exp(score - top)
        own_weight = jnp.exp(own - top)
        total = jnp.sum(weight, axis=-1, keepdims=True) + own_weight
        return (weight / total).astype(bf16), (own_weight / total).astype(bf16).astype(f32)

    def mix_part(row, slot, prob, own_prob, span):
        mixed = jnp.dot(prob, lat_buf[slot, pl.ds(0, span)], preferred_element_type=f32) + own_prob * nl_scr[pl.ds(row, 1), :]
        mixed = mixed.astype(bf16).astype(f32)
        for col in range(kv_dim // 128):
            o_scr[col, head_rows(row), :] = mixed[:, col * 128:(col + 1) * 128]

    def members(group):
        return [(order[group * GROUP + sub], lax.rem(group * GROUP, RING) + sub) for sub in range(GROUP)]

    def wait_members(items):
        for row, slot in items:
            lat_copy(row, slot).wait()
            rope_copy(row, slot).wait()

    def group_blocks(group):
        return (lens_ref[order[group * GROUP + GROUP - 1]] + 255) // 256

    def by_span(blocks, run):
        for size, test in ((2, blocks <= 2), (3, blocks == 3), (4, blocks == 4)):
            pl.when(test)(functools.partial(run, size * cache_len // 4))

    first = members(0)
    wait_members(first)

    def first_scores(span):
        for sub, (row, slot) in enumerate(first):
            s_scr[sub, :, pl.ds(0, span)] = score_part(row, slot, span)

    by_span(group_blocks(0), first_scores)

    def group_step(group, _):
        now = members(group)
        later = members(group + 1)
        wait_members(later)

        def run(span):
            pending = None
            for sub in range(GROUP):
                fresh = score_part(*later[sub], span)
                probs = soft_part(now[sub][0], s_scr[sub, :, pl.ds(0, span)])
                s_scr[sub, :, pl.ds(0, span)] = fresh
                if pending is not None:
                    mix_part(*pending, span)
                pending = (*now[sub], *probs)
            mix_part(*pending, span)

        by_span(group_blocks(group + 1), run)

        @pl.when(group < groups - RING // GROUP)
        def _():
            for sub in range(GROUP):
                start_place(group * GROUP + RING + sub, now[sub][1])

        for extra in range(WO_STEP):
            wo_copy(WO_EARLY + group * WO_STEP + extra).start()
        return 0

    lax.fori_loop(0, groups - 1, group_step, 0)
    last = members(groups - 1)
    pending = None
    for sub in range(GROUP):
        probs = soft_part(last[sub][0], s_scr[sub])
        if pending is not None:
            mix_part(*pending, cache_len)
        pending = (*last[sub], *probs)
    mix_part(*pending, cache_len)

    uv_copy.wait()
    for head in range(HEADS):
        cols = [o_scr[col, pl.ds(head, rows, stride=HEAD_PAD), :] for col in range(kv_dim // 128)]
        mixed = jnp.concatenate(cols, axis=1).astype(bf16)
        heads_scr[:, head * v_dim:(head + 1) * v_dim] = jnp.dot(mixed, wuv[head], preferred_element_type=f32).astype(bf16)
    pltpu.make_async_copy(wo_hbm, wo, o_sems.at[1]).wait()
    attn_out = jnp.dot(heads_scr[...], wo[...], preferred_element_type=f32)
    resid = (hid_ref[...].astype(f32) + attn_out).astype(bf16)
    resid_ref[...] = resid
    mlp_ref[...] = norm(resid.astype(f32), gm_ref).astype(bf16)


def attn_call(hidden, cache_lat, cache_rope, seq_lens, gain_attn, w_dq, gain_q, w_uq, w_qr, w_dkv, gain_kv, w_uk, w_uv, w_o, gain_mlp):
    rows, width = hidden.shape
    cache_len, kv_dim = cache_lat.shape[1:]
    rope_dim = cache_rope.shape[2]
    q_dim, heads, nope_dim = w_uq.shape
    v_dim = w_uv.shape[2]
    bf16, f32 = jnp.bfloat16, jnp.float32
    vmem = pl.BlockSpec(memory_space=pltpu.VMEM)
    smem = pl.BlockSpec(memory_space=pltpu.SMEM)
    hbm = pl.BlockSpec(memory_space=pl.ANY)
    dma = pltpu.SemaphoreType.DMA
    rope_keys = jnp.swapaxes(cache_rope, 1, 2)
    dkv_t = w_dkv.T
    qr_t = jnp.transpose(w_qr, (1, 2, 0)).reshape(heads * rope_dim, q_dim)
    uq_t = jnp.transpose(w_uq, (1, 2, 0)).reshape(heads * nope_dim, q_dim)
    uk_t = jnp.transpose(w_uk, (1, 2, 0))
    uv_t = jnp.swapaxes(w_uv, 0, 1)
    return pl.pallas_call(
        attn_kernel,
        out_shape=(
            jax.ShapeDtypeStruct((rows, width), bf16),
            jax.ShapeDtypeStruct((rows, width), bf16),
            jax.ShapeDtypeStruct((rows, kv_dim), bf16),
            jax.ShapeDtypeStruct((rows, rope_dim), bf16),
        ),
        in_specs=[smem, vmem, vmem, vmem, vmem, vmem] + [hbm] * 9,
        out_specs=(vmem, vmem, vmem, vmem),
        scratch_shapes=[
            pltpu.VMEM(w_dq.shape, bf16),
            pltpu.VMEM(dkv_t.shape, bf16),
            pltpu.VMEM(qr_t.shape, bf16),
            pltpu.VMEM(uq_t.shape, bf16),
            pltpu.VMEM(uk_t.shape, bf16),
            pltpu.VMEM(uv_t.shape, bf16),
            pltpu.VMEM(w_o.shape, bf16),
            pltpu.VMEM((RING, cache_len, kv_dim), bf16),
            pltpu.VMEM((RING, rope_dim, cache_len), bf16),
            pltpu.VMEM((kv_dim // 128, rows * HEAD_PAD, 128), f32),
            pltpu.VMEM((rows * HEAD_PAD, 128), f32),
            pltpu.VMEM((kv_dim // 128, rows * HEAD_PAD, 128), f32),
            pltpu.VMEM((rows, kv_dim), f32),
            pltpu.VMEM((rows, 128), f32),
            pltpu.VMEM((rows, heads * v_dim), bf16),
            pltpu.VMEM((GROUP, HEAD_PAD, cache_len), f32),
            pltpu.SMEM((rows,), jnp.int32),
            pltpu.SMEM((9,), jnp.int32),
            dma((5,)), dma((2,)), dma((RING,)), dma((RING,)),
        ],
        compiler_params=pltpu.CompilerParams(vmem_limit_bytes=67043328),
        name="attention",
    )(seq_lens, hidden, gain_attn, gain_q, gain_kv, gain_mlp, cache_lat, rope_keys, w_dq, dkv_t, qr_t, uq_t, uk_t, uv_t, w_o)


MESH = pl.DeviceIdType.MESH


def mlp_kernel(m_ref, h_ref, wg_hbm, wu_hbm, wd_hbm, out_ref, wg, wu, wd, gath, keep, s1_send, s1_recv, s2_send, s2_recv,
               w_sems, ag_send, ag_recv, fw_send, fw_recv, p1_send, p1_recv, p2_send, p2_recv):
    rows = m_ref.shape[0]
    me = lax.axis_index("g")
    core = lax.rem(me, 2)
    chip_x = lax.rem(me // 2, 2)
    chip_y = me // 4
    sibling = me + 1 - 2 * core
    mine = pl.ds(pl.multiple_of(core * rows, rows), rows)
    theirs = pl.ds(pl.multiple_of((1 - core) * rows, rows), rows)

    def peer(rel):
        return me + (rel % 2) * (2 - 4 * chip_x) + (rel // 2) * (4 - 8 * chip_y)

    def gather_copy(rel):
        target = sibling if rel == 0 else peer(rel)
        return pltpu.make_async_remote_copy(m_ref, gath.at[rel, mine], ag_send.at[rel], ag_recv.at[rel], device_id={"g": target}, device_id_type=MESH)

    def forward_copy(rel):
        return pltpu.make_async_remote_copy(gath.at[rel, mine], gath.at[rel, mine], fw_send.at[rel], fw_recv.at[rel], device_id={"g": sibling}, device_id_type=MESH)

    def pair_copy(rel):
        return pltpu.make_async_remote_copy(s1_send.at[rel], s1_recv.at[rel], p1_send.at[rel], p1_recv.at[rel], device_id={"g": sibling}, device_id_type=MESH)

    def chip_copy(rel):
        return pltpu.make_async_remote_copy(s2_send.at[rel], s2_recv.at[rel], p2_send.at[rel], p2_recv.at[rel], device_id={"g": peer(rel)}, device_id_type=MESH)

    loads = [pltpu.make_async_copy(src, dst, w_sems.at[k]) for k, (src, dst) in enumerate(((wg_hbm, wg), (wu_hbm, wu), (wd_hbm, wd)))]
    for load in loads:
        load.start()

    barrier = pltpu.get_barrier_semaphore()
    for target in (sibling, peer(1), peer(2), peer(3)):
        pl.semaphore_signal(barrier, inc=1, device_id={"g": target}, device_id_type=MESH)
    pl.semaphore_wait(barrier, 4)

    for rel in (1, 2, 3, 0):
        gather_copy(rel).start()
    gath[0, mine] = m_ref[...]
    for rel in (1, 2):
        gather_copy(rel).wait_recv()
        forward_copy(rel).start()

    def finish_pair(rel):
        pair_copy(rel).wait_recv()
        keep[rel] = keep[rel] + s1_recv[rel]

        @pl.when(rel > 0)
        def _():
            s2_send[rel] = keep[rel].astype(jnp.bfloat16)
            chip_copy(rel).start()

    for load in loads:
        load.wait()

    def block(step, _):
        rel = lax.rem(step + 1, 4)

        @pl.when(step == 1)
        def _():
            gather_copy(3).wait_recv()
            forward_copy(3).start()

        @pl.when(step < 3)
        def _():
            forward_recv = pltpu.make_async_remote_copy(gath.at[rel, theirs], gath.at[rel, theirs], fw_send.at[rel], fw_recv.at[rel], device_id={"g": sibling}, device_id_type=MESH)
            forward_recv.wait_recv()

        @pl.when(step == 3)
        def _():
            pltpu.make_async_remote_copy(m_ref, gath.at[0, theirs], ag_send.at[0], ag_recv.at[0], device_id={"g": sibling}, device_id_type=MESH).wait_recv()

        block_rows = gath[rel]
        gate = jnp.dot(block_rows, wg[...], preferred_element_type=jnp.float32)
        up = jnp.dot(block_rows, wu[...], preferred_element_type=jnp.float32)
        act = (jax.nn.silu(gate) * up).astype(jnp.bfloat16)

        @pl.when(step > 0)
        def _():
            finish_pair(step)

        part = jnp.dot(act, wd[...], preferred_element_type=jnp.float32)
        low, high = part[:rows], part[rows:]
        is_low = core == 0
        keep[rel] = jnp.where(is_low, low, high)
        s1_send[rel] = jnp.where(is_low, high, low)
        pair_copy(rel).start()
        return 0

    lax.fori_loop(0, 4, block, 0)
    finish_pair(0)
    total = h_ref[...].astype(jnp.float32) + keep[0]
    for rel in (1, 2, 3):
        chip_copy(rel).wait_recv()
        total = total + s2_recv[rel].astype(jnp.float32)
    out_ref[...] = total.astype(jnp.bfloat16)
    for rel in range(4):
        gather_copy(rel).wait_send()
        pair_copy(rel).wait_send()
    for rel in (1, 2, 3):
        forward_copy(rel).wait_send()
        chip_copy(rel).wait_send()


def mlp_call(m, h, w_gate, w_up, w_down):
    rows, width = m.shape
    cols = w_gate.shape[1]
    vmem = pl.BlockSpec(memory_space=pltpu.VMEM)
    hbm = pl.BlockSpec(memory_space=pl.ANY)
    dma = pltpu.SemaphoreType.DMA
    return pl.pallas_call(
        mlp_kernel,
        out_shape=jax.ShapeDtypeStruct((rows, width), jnp.bfloat16),
        in_specs=[vmem, vmem, hbm, hbm, hbm],
        out_specs=vmem,
        scratch_shapes=[
            pltpu.VMEM((width, cols), jnp.bfloat16),
            pltpu.VMEM((width, cols), jnp.bfloat16),
            pltpu.VMEM((cols, width), jnp.bfloat16),
            pltpu.VMEM((4, 2 * rows, width), jnp.bfloat16),
            pltpu.VMEM((4, rows, width), jnp.float32),
            pltpu.VMEM((4, rows, width), jnp.float32),
            pltpu.VMEM((4, rows, width), jnp.float32),
            pltpu.VMEM((4, rows, width), jnp.bfloat16),
            pltpu.VMEM((4, rows, width), jnp.bfloat16),
            dma((3,)), dma((4,)), dma((4,)), dma((4,)), dma((4,)), dma((4,)), dma((4,)), dma((4,)), dma((4,)),
        ],
        compiler_params=pltpu.CompilerParams(collective_id=0, has_side_effects=True, vmem_limit_bytes=67043328),
        name="mlp_exchange",
    )(m, h, w_gate, w_up, w_down)


def solution(mesh):
    row_spec = P(("rep", "g"))
    full_spec = P()
    in_specs = (row_spec, row_spec, row_spec, row_spec, full_spec, full_spec, full_spec, full_spec, full_spec, full_spec, full_spec, full_spec, full_spec, full_spec, full_spec, P(None, "g"), P(None, "g"), P("g", None))

    def local_step(hidden, cache_lat, cache_rope, seq_lens, gain_attn, w_dq, gain_q, w_uq, w_qr, w_dkv, gain_kv, w_uk, w_uv, w_o, gain_mlp, w_gate, w_up, w_down):
        resid_rows, mlp_in, new_lat, new_rope = attn_call(hidden, cache_lat, cache_rope, seq_lens, gain_attn, w_dq, gain_q, w_uq, w_qr, w_dkv, gain_kv, w_uk, w_uv, w_o, gain_mlp)
        out_hidden = mlp_call(mlp_in, resid_rows, w_gate, w_up, w_down)
        return out_hidden, new_lat, new_rope

    return jax.shard_map(local_step, mesh=mesh, in_specs=in_specs, out_specs=(row_spec, row_spec, row_spec), check_vma=False)
```

```python
import functools

import jax
import jax.numpy as jnp
from jax import lax
from jax.experimental import pallas as pl
from jax.experimental.pallas import tpu as pltpu
from jax.sharding import PartitionSpec as P


HEADS = 20
HEAD_PAD = 24
RING = 16
GROUP = 4
WO_PARTS = 20
WO_STEP = 3


def attn_kernel(lens_ref, hid_ref, ga_ref, gq_ref, gkv_ref, lat_hbm, rope_hbm, wdq_hbm, wdkv_hbm, wqr_hbm, wuq_hbm, wuk_hbm, wuv_hbm, wo_hbm,
                newlat_ref, newrope_ref, o_scr, hid_out, wuv, wo,
                wdq, wdkv, wuk, lat_buf, rope_buf, q_scr, qr_scr, nl_scr, nr_scr, s_scr,
                order, fill, w_sems, o_sems, lat_sems, rope_sems):
    rows = hid_ref.shape[0]
    kv_dim = lat_buf.shape[2]
    rope_dim = rope_buf.shape[1]
    cache_len = lat_buf.shape[1]
    nope_dim = wuk.shape[1]
    q_dim = wdq.shape[1]
    half = rope_dim // 2
    groups = rows // GROUP
    f32, bf16 = jnp.float32, jnp.bfloat16
    nt = (((1,), (1,)), ((), ()))

    wuq = wo.at[pl.ds(0, HEADS * nope_dim), pl.ds(0, q_dim)]
    wqr = wo.at[pl.ds(0, HEADS * rope_dim), pl.ds(q_dim, q_dim)]
    early = [pltpu.make_async_copy(src, dst, w_sems.at[k]) for k, (src, dst) in enumerate(((wdq_hbm, wdq), (wdkv_hbm, wdkv), (wqr_hbm, wqr), (wuq_hbm, wuq), (wuk_hbm, wuk)))]
    for copy in early:
        copy.start()

    def bucket(row):
        return 8 - (lens_ref[row] + 127) // 128

    for k in range(9):
        fill[k] = 0

    def count(row, _):
        k = bucket(row)
        fill[k] = fill[k] + 1
        return 0

    lax.fori_loop(0, rows, count, 0)
    running = jnp.int32(0)
    for k in range(9):
        size = fill[k]
        fill[k] = running
        running = running + size

    def place(row, _):
        k = bucket(row)
        order[fill[k]] = row
        fill[k] = fill[k] + 1
        return 0

    lax.fori_loop(0, rows, place, 0)

    def lat_copy(row, slot):
        count16 = pl.multiple_of(((lens_ref[row] + 15) // 16) * 16, 16)
        return pltpu.make_async_copy(lat_hbm.at[row, pl.ds(0, count16)], lat_buf.at[slot, pl.ds(0, count16)], lat_sems.at[slot])

    def rope_copy(row, slot):
        return pltpu.make_async_copy(rope_hbm.at[row], rope_buf.at[slot], rope_sems.at[slot])

    def start_place(place_id, slot):
        row = order[place_id]
        lat_copy(row, slot).start()
        rope_copy(row, slot).start()

    wo_rows = wo.shape[0] // WO_PARTS

    def wo_copy(part):
        span = pl.ds(pl.multiple_of(part * wo_rows, 32), wo_rows)
        return pltpu.make_async_copy(wo_hbm.at[span], wo.at[span], o_sems.at[1])

    def clear_and_start(slot, _):
        lat_buf[slot, pl.ds(256, cache_len - 256)] = jnp.zeros((cache_len - 256, kv_dim), bf16)
        start_place(slot, slot)
        return 0

    lax.fori_loop(0, RING, clear_and_start, 0)
    uv_copy = pltpu.make_async_copy(wuv_hbm, wuv, o_sems.at[0])

    def norm(values, gain_ref):
        mean_sq = jnp.mean(values * values, axis=-1, keepdims=True)
        return values * lax.rsqrt(mean_sq + 1e-6) * gain_ref[...].astype(f32)

    row_id = lax.broadcasted_iota(jnp.int32, (rows, 128), 0)
    position = jnp.zeros((rows, 128), jnp.int32)
    for row in range(rows):
        position = jnp.where(row_id == row, lens_ref[row], position)
    lane = lax.broadcasted_iota(jnp.int32, (rows, 128), 1)
    freq_id = lane & (half - 1)
    inv_freq = jnp.exp(freq_id.astype(f32) * (-jnp.log(jnp.float32(10000.0)) / half))
    angle = position.astype(f32) * inv_freq
    first_half = (lane & half) == 0
    cos_part = jnp.cos(angle)
    sin_part = jnp.where(first_half, -jnp.sin(angle), jnp.sin(angle))

    def rotate(values):
        swapped = jnp.where(first_half, pltpu.roll(values, 128 - half, 1), pltpu.roll(values, half, 1))
        return values * cos_part + swapped * sin_part

    hid_out[...] = hid_ref[...]
    hidden = hid_ref[...].astype(f32)
    normed = norm(hidden, ga_ref).astype(bf16)
    q_scr[...] = jnp.zeros_like(q_scr)
    qr_scr[...] = jnp.zeros_like(qr_scr)

    early[0].wait()
    q_raw = jnp.dot(normed, wdq[...], preferred_element_type=f32)
    early[1].wait()
    kv_raw = lax.dot_general(normed, wdkv[...], nt, preferred_element_type=f32)
    q_in = norm(q_raw, gq_ref).astype(bf16)
    early[2].wait()
    rope_raw = lax.dot_general(q_in, wo[pl.ds(0, HEADS * rope_dim), pl.ds(q_dim, q_dim)], nt, preferred_element_type=f32)
    new_lat = norm(kv_raw[:, :kv_dim], gkv_ref).astype(bf16)
    newlat_ref[...] = new_lat
    nl_scr[...] = new_lat.astype(f32)
    kv_rope = jnp.concatenate([kv_raw[:, kv_dim:], jnp.zeros((rows, 128 - rope_dim), f32)], axis=1)
    new_rope = rotate(kv_rope).astype(bf16)
    newrope_ref[...] = new_rope[:, :rope_dim]
    nr_scr[...] = jnp.where(lane < rope_dim, new_rope.astype(f32), 0.0)

    def nope_quad(quad):
        return lax.dot_general(q_in, wo[pl.ds(quad * 4 * nope_dim, 4 * nope_dim), pl.ds(0, q_dim)], nt, preferred_element_type=f32)

    def absorb_quad(quad, q_nope):
        for sub in range(4):
            head = quad * 4 + sub
            one = q_nope[:, sub * nope_dim:(sub + 1) * nope_dim].astype(bf16)
            q_abs = jnp.dot(one, wuk[head], preferred_element_type=f32).astype(bf16).astype(f32)
            for col in range(kv_dim // 128):
                q_scr[col, pl.ds(head, rows, stride=HEAD_PAD), :] = q_abs[:, col * 128:(col + 1) * 128]

    early[3].wait()
    quads = HEADS // 4
    ahead = nope_quad(0)
    for pair in range(HEADS // 2):
        turned = rotate(rope_raw[:, pair * 128:(pair + 1) * 128]).astype(bf16).astype(f32)
        qr_scr[pl.ds(2 * pair, rows, stride=HEAD_PAD), :] = turned
        qr_scr[pl.ds(2 * pair + 1, rows, stride=HEAD_PAD), :] = pltpu.roll(turned, rope_dim, 1)
    for quad in range(quads):
        now = ahead
        if quad + 1 < quads:
            ahead = nope_quad(quad + 1)
        if quad == 0:
            early[4].wait()
        absorb_quad(quad, now)

    scale = (nope_dim + rope_dim) ** -0.5

    def head_rows(row):
        return pl.ds(pl.multiple_of(row * HEAD_PAD, 8), HEAD_PAD)

    def query(row):
        return jnp.concatenate([q_scr[col, head_rows(row), :] for col in range(kv_dim // 128)], axis=1)

    def score_part(row, slot, span):
        lat = lat_buf[slot, pl.ds(0, span)]
        score = lax.dot_general(query(row).astype(bf16), lat, nt, preferred_element_type=f32)
        q_rope = qr_scr[head_rows(row), :][:, :rope_dim].astype(bf16)
        return score + jnp.dot(q_rope, rope_buf[slot, :, pl.ds(0, span)], preferred_element_type=f32)

    def soft_part(row, score):
        key_pos = lax.broadcasted_iota(jnp.int32, score.shape, 1)
        score = jnp.where(key_pos < lens_ref[row], score * scale, -jnp.inf)
        q_rope = qr_scr[head_rows(row), :]
        own = jnp.sum(query(row) * nl_scr[pl.ds(row, 1), :], axis=-1, keepdims=True) + jnp.sum(q_rope * nr_scr[pl.ds(row, 1), :], axis=-1, keepdims=True)
        own = own * scale
        top = jnp.maximum(jnp.max(score, axis=-1, keepdims=True), own)
        weight = jnp.exp(score - top)
        own_weight = jnp.exp(own - top)
        total = jnp.sum(weight, axis=-1, keepdims=True) + own_weight
        return (weight / total).astype(bf16), (own_weight / total).astype(bf16).astype(f32)

    def mix_part(row, slot, prob, own_prob, span):
        mixed = jnp.dot(prob, lat_buf[slot, pl.ds(0, span)], preferred_element_type=f32) + own_prob * nl_scr[pl.ds(row, 1), :]
        mixed = mixed.astype(bf16).astype(f32)
        for col in range(kv_dim // 128):
            o_scr[col, head_rows(row), :] = mixed[:, col * 128:(col + 1) * 128]

    def members(group):
        return [(order[group * GROUP + sub], lax.rem(group * GROUP, RING) + sub) for sub in range(GROUP)]

    def wait_members(items):
        for row, slot in items:
            lat_copy(row, slot).wait()
            rope_copy(row, slot).wait()

    def group_blocks(group):
        return (lens_ref[order[group * GROUP]] + 255) // 256

    def by_span(blocks, run):
        for size, test in ((2, blocks <= 2), (3, blocks == 3), (4, blocks == 4)):
            pl.when(test)(functools.partial(run, size * cache_len // 4))

    first = members(0)
    wait_members(first)

    def first_scores(span):
        for sub, (row, slot) in enumerate(first):
            s_scr[sub, :, pl.ds(0, span)] = score_part(row, slot, span)

    by_span(group_blocks(0), first_scores)

    def group_step(group, _):
        now = members(group)
        later = members(group + 1)
        wait_members(later)

        def run(span):
            pending = None
            for sub in range(GROUP):
                fresh = score_part(*later[sub], span)
                probs = soft_part(now[sub][0], s_scr[sub, :, pl.ds(0, span)])
                s_scr[sub, :, pl.ds(0, span)] = fresh
                if pending is not None:
                    mix_part(*pending, span)
                pending = (*now[sub], *probs)
            mix_part(*pending, span)

        by_span(group_blocks(group), run)

        @pl.when(group < groups - RING // GROUP)
        def _():
            for sub in range(GROUP):
                start_place(group * GROUP + RING + sub, now[sub][1])

        @pl.when(group == 0)
        def _():
            uv_copy.start()

        for extra in range(WO_STEP):
            part = group * WO_STEP + extra
            pl.when(part < WO_PARTS)(lambda part=part: wo_copy(part).start())
        return 0

    lax.fori_loop(0, groups - 1, group_step, 0)
    last = members(groups - 1)

    def last_mix(span):
        pending = None
        for sub in range(GROUP):
            probs = soft_part(last[sub][0], s_scr[sub, :, pl.ds(0, span)])
            if pending is not None:
                mix_part(*pending, span)
            pending = (*last[sub], *probs)
        mix_part(*pending, span)

    by_span(group_blocks(groups - 1), last_mix)
    uv_copy.wait()
    pltpu.make_async_copy(wo_hbm, wo, o_sems.at[1]).wait()


def attn_call(hidden, cache_lat, cache_rope, seq_lens, gain_attn, w_dq, gain_q, w_uq, w_qr, w_dkv, gain_kv, w_uk, w_uv, w_o):
    rows, width = hidden.shape
    cache_len, kv_dim = cache_lat.shape[1:]
    rope_dim = cache_rope.shape[2]
    q_dim, heads, nope_dim = w_uq.shape
    bf16, f32 = jnp.bfloat16, jnp.float32
    vmem = pl.BlockSpec(memory_space=pltpu.VMEM)
    smem = pl.BlockSpec(memory_space=pltpu.SMEM)
    hbm = pl.BlockSpec(memory_space=pltpu.HBM)
    dma = pltpu.SemaphoreType.DMA
    rope_keys = jnp.swapaxes(cache_rope, 1, 2)
    dkv_t = w_dkv.T
    qr_t = jnp.transpose(w_qr, (1, 2, 0)).reshape(heads * rope_dim, q_dim)
    uq_t = jnp.transpose(w_uq, (1, 2, 0)).reshape(heads * nope_dim, q_dim)
    uk_t = jnp.transpose(w_uk, (1, 2, 0))
    uv_t = jnp.swapaxes(w_uv, 0, 1)
    handed = (
        pltpu.VMEM((kv_dim // 128, rows * HEAD_PAD, 128), f32),
        pltpu.VMEM(hidden.shape, bf16),
        pltpu.VMEM(uv_t.shape, bf16),
        pltpu.VMEM(w_o.shape, bf16),
    )
    return pl.pallas_call(
        attn_kernel,
        out_shape=(jax.ShapeDtypeStruct((rows, kv_dim), bf16), jax.ShapeDtypeStruct((rows, rope_dim), bf16)) + handed,
        in_specs=[smem, vmem, vmem, vmem, vmem] + [hbm] * 9,
        out_specs=(vmem,) * 6,
        scratch_shapes=[
            pltpu.VMEM(w_dq.shape, bf16),
            pltpu.VMEM(dkv_t.shape, bf16),
            pltpu.VMEM(uk_t.shape, bf16),
            pltpu.VMEM((RING, cache_len, kv_dim), bf16),
            pltpu.VMEM((RING, rope_dim, cache_len), bf16),
            pltpu.VMEM((kv_dim // 128, rows * HEAD_PAD, 128), f32),
            pltpu.VMEM((rows * HEAD_PAD, 128), f32),
            pltpu.VMEM((rows, kv_dim), f32),
            pltpu.VMEM((rows, 128), f32),
            pltpu.VMEM((GROUP, HEAD_PAD, cache_len), f32),
            pltpu.SMEM((rows,), jnp.int32),
            pltpu.SMEM((9,), jnp.int32),
            dma((5,)), dma((2,)), dma((RING,)), dma((RING,)),
        ],
        compiler_params=pltpu.CompilerParams(vmem_limit_bytes=33 * 1024 * 1024),
        name="attention",
    )(seq_lens, hidden, gain_attn, gain_q, gain_kv, cache_lat, rope_keys, w_dq, dkv_t, qr_t, uq_t, uk_t, uv_t, w_o)


MESH = pl.DeviceIdType.MESH
CHUNKS = 4


def mlp_kernel(o_ref, hid_ref, wuv, wo, gm_ref, wg_hbm, wu_hbm, wd_hbm, out_ref,
               wg, wu, wd, heads_scr, h_scr, gath, m_scr, keep, s1_send, s1_recv, s2_send, s2_recv,
               w_sems, near_send, near_recv, far_send, far_recv, fw_send, fw_recv, p1_send, p1_recv, p2_send, p2_recv):
    rows, width = hid_ref.shape
    part_width = width // CHUNKS
    heads, kv_dim, v_dim = wuv.shape
    f32, bf16 = jnp.float32, jnp.bfloat16
    me = lax.axis_index("g")
    core = lax.rem(me, 2)
    chip_x = lax.rem(me // 2, 2)
    chip_y = me // 4
    is_low = core == 0
    sibling = me + 1 - 2 * core
    mine = pl.ds(pl.multiple_of(core * rows, rows), rows)
    theirs = pl.ds(pl.multiple_of((1 - core) * rows, rows), rows)

    def peer(rel):
        return me + (rel % 2) * (2 - 4 * chip_x) + (rel // 2) * (4 - 8 * chip_y)

    def remote(src, dst, send, recv, target):
        return pltpu.make_async_remote_copy(src, dst, send, recv, device_id={"g": target}, device_id_type=MESH)

    def near_copy(rel, part):
        return remote(h_scr.at[part], gath.at[rel, part, mine], near_send.at[rel, part], near_recv.at[rel, part], peer(rel))

    def far_copy(rel):
        return remote(h_scr, gath.at[rel, :, mine], far_send.at[rel], far_recv.at[rel], sibling if rel == 0 else peer(rel))

    def sibling_rows_arrived():
        remote(h_scr, gath.at[0, :, theirs], far_send.at[0], far_recv.at[0], sibling).wait_recv()

    def forward_copy(rel):
        return remote(gath.at[rel, :, mine], gath.at[rel, :, mine], fw_send.at[rel], fw_recv.at[rel], sibling)

    def forward_arrived(rel):
        remote(gath.at[rel, :, theirs], gath.at[rel, :, theirs], fw_send.at[rel], fw_recv.at[rel], sibling).wait_recv()

    def pair_copy(rel):
        return remote(s1_send.at[rel], s1_recv.at[rel], p1_send.at[rel], p1_recv.at[rel], sibling)

    def chip_copy(rel):
        return remote(s2_send.at[rel], s2_recv.at[rel], p2_send.at[rel], p2_recv.at[rel], peer(rel))

    loads = [pltpu.make_async_copy(src, dst, w_sems.at[k]) for k, (src, dst) in enumerate(((wg_hbm, wg), (wu_hbm, wu), (wd_hbm, wd)))]
    for load in loads:
        load.start()
    barrier = pltpu.get_barrier_semaphore()
    for target in (sibling, peer(1), peer(2), peer(3)):
        pl.semaphore_signal(barrier, inc=1, device_id={"g": target}, device_id_type=MESH)

    for head in range(heads):
        cols = [o_ref[col, pl.ds(head, rows, stride=HEAD_PAD), :] for col in range(kv_dim // 128)]
        mixed = jnp.concatenate(cols, axis=1).astype(bf16)
        heads_scr[:, head * v_dim:(head + 1) * v_dim] = jnp.dot(mixed, wuv[head], preferred_element_type=f32).astype(bf16)

    def columns(part):
        return pl.ds(part * part_width, part_width)

    for part in range(CHUNKS):
        attn_out = jnp.dot(heads_scr[...], wo[:, columns(part)], preferred_element_type=f32)
        resid = (hid_ref[:, columns(part)].astype(f32) + attn_out).astype(bf16)
        h_scr[part] = resid
        gath[0, part, mine] = resid
        if part == 0:
            pl.semaphore_wait(barrier, 4)
        near_copy(1, part).start()
        near_copy(2, part).start()
    far_copy(3).start()
    far_copy(0).start()

    def normed_rows(rel, at):
        square = jnp.zeros((2 * rows, 1), f32)
        for part in range(CHUNKS):
            piece = gath[rel, part].astype(f32)
            square = square + jnp.sum(piece * piece, axis=-1, keepdims=True)
        factor = lax.rsqrt(square / width + 1e-6)
        for part in range(CHUNKS):
            piece = gath[rel, part].astype(f32) * factor * gm_ref[columns(part)].astype(f32)
            m_scr[pl.ds(at, 2 * rows), columns(part)] = piece.astype(bf16)

    def activation(count):
        block = m_scr[pl.ds(0, count)]
        gate = jnp.dot(block, wg[...], preferred_element_type=f32)
        up = jnp.dot(block, wu[...], preferred_element_type=f32)
        return (jax.nn.silu(gate) * up).astype(bf16)

    def contract(act, rels):
        part = jnp.dot(act, wd[...], preferred_element_type=f32)
        for index, rel in enumerate(rels):
            low = part[2 * index * rows:(2 * index + 1) * rows]
            high = part[(2 * index + 1) * rows:(2 * index + 2) * rows]
            s1_send[rel] = jnp.where(is_low, high, low)
            keep[rel] = jnp.where(is_low, low, high)
            pair_copy(rel).start()

    def send_sum(rel):
        pair_copy(rel).wait_recv()
        s2_send[rel] = (keep[rel] + s1_recv[rel]).astype(bf16)
        chip_copy(rel).start()

    sibling_rows_arrived()
    normed_rows(0, 0)
    loads[0].wait()
    loads[1].wait()
    act = activation(2 * rows)
    for rel in (1, 2):
        for part in range(CHUNKS):
            near_copy(rel, part).wait_recv()
        forward_copy(rel).start()
    loads[2].wait()
    contract(act, (0,))

    forward_arrived(1)
    normed_rows(1, 0)
    forward_arrived(2)
    normed_rows(2, 2 * rows)
    contract(activation(4 * rows), (1, 2))
    far_copy(3).wait_recv()
    forward_copy(3).start()
    send_sum(1)
    send_sum(2)

    forward_arrived(3)
    normed_rows(3, 0)
    contract(activation(2 * rows), (3,))
    pair_copy(0).wait_recv()
    send_sum(3)

    cols = [h_scr[part].astype(f32) for part in range(CHUNKS)]
    total = jnp.concatenate(cols, axis=1) + (keep[0] + s1_recv[0])
    for rel in (1, 2, 3):
        chip_copy(rel).wait_recv()
        total = total + s2_recv[rel].astype(f32)
    out_ref[...] = total.astype(bf16)
    for rel in (1, 2):
        for part in range(CHUNKS):
            near_copy(rel, part).wait_send()
    far_copy(3).wait_send()
    far_copy(0).wait_send()
    for rel in range(4):
        pair_copy(rel).wait_send()
    for rel in (1, 2, 3):
        forward_copy(rel).wait_send()
        chip_copy(rel).wait_send()


def mlp_call(o_lat, hidden, w_uv, w_o, gain_mlp, w_gate, w_up, w_down):
    rows, width = hidden.shape
    cols = w_gate.shape[1]
    bf16, f32 = jnp.bfloat16, jnp.float32
    vmem = pl.BlockSpec(memory_space=pltpu.VMEM)
    hbm = pl.BlockSpec(memory_space=pltpu.HBM)
    dma = pltpu.SemaphoreType.DMA
    part_width = width // CHUNKS
    held = [pltpu.with_memory_space_constraint(x, pltpu.VMEM) for x in (o_lat, hidden, w_uv, w_o)]
    streamed = [pltpu.with_memory_space_constraint(x, pltpu.HBM) for x in (w_gate, w_up, w_down)]
    return pl.pallas_call(
        mlp_kernel,
        out_shape=jax.ShapeDtypeStruct((rows, width), bf16),
        in_specs=[vmem, vmem, vmem, vmem, vmem, hbm, hbm, hbm],
        out_specs=vmem,
        scratch_shapes=[
            pltpu.VMEM((width, cols), bf16),
            pltpu.VMEM((width, cols), bf16),
            pltpu.VMEM((cols, width), bf16),
            pltpu.VMEM((rows, w_o.shape[0]), bf16),
            pltpu.VMEM((CHUNKS, rows, part_width), bf16),
            pltpu.VMEM((4, CHUNKS, 2 * rows, part_width), bf16),
            pltpu.VMEM((4 * rows, width), bf16),
            pltpu.VMEM((4, rows, width), f32),
            pltpu.VMEM((4, rows, width), f32),
            pltpu.VMEM((4, rows, width), f32),
            pltpu.VMEM((4, rows, width), bf16),
            pltpu.VMEM((4, rows, width), bf16),
            dma((3,)), dma((4, CHUNKS)), dma((4, CHUNKS)), dma((4,)), dma((4,)), dma((4,)), dma((4,)), dma((4,)), dma((4,)), dma((4,)), dma((4,)),
        ],
        compiler_params=pltpu.CompilerParams(collective_id=0, has_side_effects=True, vmem_limit_bytes=33 * 1024 * 1024),
        name="mlp_exchange",
    )(*held, gain_mlp, *streamed)


def solution(mesh):
    row_spec = P(("rep", "g"))
    full_spec = P()
    in_specs = (row_spec, row_spec, row_spec, row_spec, full_spec, full_spec, full_spec, full_spec, full_spec, full_spec, full_spec, full_spec, full_spec, full_spec, full_spec, P(None, "g"), P(None, "g"), P("g", None))

    def local_step(hidden, cache_lat, cache_rope, seq_lens, gain_attn, w_dq, gain_q, w_uq, w_qr, w_dkv, gain_kv, w_uk, w_uv, w_o, gain_mlp, w_gate, w_up, w_down):
        new_lat, new_rope, o_lat, hid_rows, uv_held, wo_held = attn_call(hidden, cache_lat, cache_rope, seq_lens, gain_attn, w_dq, gain_q, w_uq, w_qr, w_dkv, gain_kv, w_uk, w_uv, w_o)
        out_hidden = mlp_call(o_lat, hid_rows, uv_held, wo_held, gain_mlp, w_gate, w_up, w_down)
        return out_hidden, new_lat, new_rope

    return jax.shard_map(local_step, mesh=mesh, in_specs=in_specs, out_specs=(row_spec, row_spec, row_spec), check_vma=False)
```

```python
import functools

import jax
import jax.numpy as jnp
from jax import lax
from jax.experimental import pallas as pl
from jax.experimental.pallas import tpu as pltpu
from jax.sharding import PartitionSpec as P


HEADS = 20
HEAD_PAD = 24
RING = 16
GROUP = 4
WO_PARTS = 20
WO_STEP = 3


def attn_kernel(lens_hbm, hid_hbm, ga_hbm, gq_hbm, gkv_hbm, lat_hbm, rope_hbm, wdq_hbm, wdkv_hbm, wqr_hbm, wuq_hbm, wuk_hbm, wuv_hbm, wo_hbm,
                newlat_hbm, newrope_hbm, o_scr, hid_ref, wuv, wo,
                wdq, wdkv, wuk, lat_buf, rope_buf, q_scr, qr_scr, nl_scr, nr_scr, s_scr,
                ga_ref, gq_ref, gkv_ref, newlat_ref, newrope_ref, lens_ref, order, fill, w_sems, o_sems, in_sems, new_sems, lat_sems, rope_sems):
    rows = hid_ref.shape[0]
    kv_dim = lat_buf.shape[2]
    rope_dim = rope_buf.shape[1]
    cache_len = lat_buf.shape[1]
    nope_dim = wuk.shape[1]
    q_dim = wdq.shape[1]
    half = rope_dim // 2
    groups = rows // GROUP
    f32, bf16 = jnp.float32, jnp.bfloat16
    nt = (((1,), (1,)), ((), ()))

    wuq = wo.at[pl.ds(0, HEADS * nope_dim), pl.ds(0, q_dim)]
    wqr = wo.at[pl.ds(0, HEADS * rope_dim), pl.ds(q_dim, q_dim)]
    early = [pltpu.make_async_copy(src, dst, w_sems.at[k]) for k, (src, dst) in enumerate(((wdq_hbm, wdq), (wdkv_hbm, wdkv), (wqr_hbm, wqr), (wuq_hbm, wuq), (wuk_hbm, wuk)))]
    small = [pltpu.make_async_copy(src, dst, in_sems.at[k]) for k, (src, dst) in enumerate(((lens_hbm, lens_ref), (hid_hbm, hid_ref), (ga_hbm, ga_ref), (gq_hbm, gq_ref), (gkv_hbm, gkv_ref)))]
    for copy in small + early:
        copy.start()
    small[0].wait()

    def bucket(row):
        return 8 - ((lens_ref[row] + 127) >> 7)

    for k in range(9):
        fill[k] = 0

    def count(row, _):
        k = bucket(row)
        fill[k] = fill[k] + 1
        return 0

    lax.fori_loop(0, rows, count, 0)
    running = jnp.int32(0)
    for k in range(9):
        size = fill[k]
        fill[k] = running
        running = running + size

    def place(row, _):
        k = bucket(row)
        order[fill[k]] = row
        fill[k] = fill[k] + 1
        return 0

    lax.fori_loop(0, rows, place, 0)

    def lat_copy(place_id, slot):
        row = order[place_id]
        span = jnp.maximum((lens_ref[order[(place_id // GROUP) * GROUP]] + 255) >> 8, 2) << 8
        count = jnp.where(place_id < RING, span, ((lens_ref[row] + 15) >> 4) << 4)
        count = pl.multiple_of(count, 16)
        return pltpu.make_async_copy(lat_hbm.at[row, pl.ds(0, count)], lat_buf.at[slot, pl.ds(0, count)], lat_sems.at[slot])

    def rope_copy(row, slot):
        return pltpu.make_async_copy(rope_hbm.at[row], rope_buf.at[slot], rope_sems.at[slot])

    def start_place(place_id, slot):
        lat_copy(place_id, slot).start()
        rope_copy(order[place_id], slot).start()

    wo_rows = wo.shape[0] // WO_PARTS

    def wo_copy(part):
        span = pl.ds(pl.multiple_of(part * wo_rows, 32), wo_rows)
        return pltpu.make_async_copy(wo_hbm.at[span], wo.at[span], o_sems.at[1])

    def fill_ring(slot, _):
        start_place(slot, slot)
        return 0

    lax.fori_loop(0, RING, fill_ring, 0)
    uv_copy = pltpu.make_async_copy(wuv_hbm, wuv, o_sems.at[0])

    def norm(values, gain_ref):
        mean_sq = jnp.mean(values * values, axis=-1, keepdims=True)
        return values * lax.rsqrt(mean_sq + 1e-6) * gain_ref[...].astype(f32)

    row_id = lax.broadcasted_iota(jnp.int32, (rows, 128), 0)
    position = jnp.zeros((rows, 128), jnp.int32)
    for row in range(rows):
        position = jnp.where(row_id == row, lens_ref[row], position)
    lane = lax.broadcasted_iota(jnp.int32, (rows, 128), 1)
    freq_id = lane & (half - 1)
    inv_freq = jnp.exp(freq_id.astype(f32) * (-jnp.log(jnp.float32(10000.0)) / half))
    angle = position.astype(f32) * inv_freq
    first_half = (lane & half) == 0
    cos_part = jnp.cos(angle)
    sin_part = jnp.where(first_half, -jnp.sin(angle), jnp.sin(angle))

    def rotate(values):
        swapped = jnp.where(first_half, pltpu.roll(values, 128 - half, 1), pltpu.roll(values, half, 1))
        return values * cos_part + swapped * sin_part

    small[1].wait()
    small[2].wait()
    hidden = hid_ref[...].astype(f32)
    normed = norm(hidden, ga_ref).astype(bf16)
    q_scr[...] = jnp.zeros_like(q_scr)
    qr_scr[...] = jnp.zeros_like(qr_scr)

    small[3].wait()
    small[4].wait()
    early[0].wait()
    q_raw = jnp.dot(normed, wdq[...], preferred_element_type=f32)
    early[1].wait()
    kv_raw = lax.dot_general(normed, wdkv[...], nt, preferred_element_type=f32)
    q_in = norm(q_raw, gq_ref).astype(bf16)
    early[2].wait()
    rope_raw = lax.dot_general(q_in, wo[pl.ds(0, HEADS * rope_dim), pl.ds(q_dim, q_dim)], nt, preferred_element_type=f32)
    new_lat = norm(kv_raw[:, :kv_dim], gkv_ref).astype(bf16)
    newlat_ref[...] = new_lat
    nl_scr[...] = new_lat.astype(f32)
    kv_rope = jnp.concatenate([kv_raw[:, kv_dim:], jnp.zeros((rows, 128 - rope_dim), f32)], axis=1)
    new_rope = rotate(kv_rope).astype(bf16)
    newrope_ref[...] = new_rope[:, :rope_dim]
    outgoing = [pltpu.make_async_copy(newlat_ref, newlat_hbm, new_sems.at[0]), pltpu.make_async_copy(newrope_ref, newrope_hbm, new_sems.at[1])]
    nr_scr[...] = jnp.where(lane < rope_dim, new_rope.astype(f32), 0.0)

    def nope_quad(quad):
        return lax.dot_general(q_in, wo[pl.ds(quad * 4 * nope_dim, 4 * nope_dim), pl.ds(0, q_dim)], nt, preferred_element_type=f32)

    def absorb_quad(quad, q_nope):
        for sub in range(4):
            head = quad * 4 + sub
            one = q_nope[:, sub * nope_dim:(sub + 1) * nope_dim].astype(bf16)
            q_abs = jnp.dot(one, wuk[head], preferred_element_type=f32).astype(bf16).astype(f32)
            for col in range(kv_dim // 128):
                q_scr[col, pl.ds(head, rows, stride=HEAD_PAD), :] = q_abs[:, col * 128:(col + 1) * 128]

    early[3].wait()
    quads = HEADS // 4
    ahead = nope_quad(0)
    for pair in range(HEADS // 2):
        turned = rotate(rope_raw[:, pair * 128:(pair + 1) * 128]).astype(bf16).astype(f32)
        qr_scr[pl.ds(2 * pair, rows, stride=HEAD_PAD), :] = turned
        qr_scr[pl.ds(2 * pair + 1, rows, stride=HEAD_PAD), :] = pltpu.roll(turned, rope_dim, 1)
    for quad in range(quads):
        now = ahead
        if quad + 1 < quads:
            ahead = nope_quad(quad + 1)
        if quad == 0:
            early[4].wait()
        absorb_quad(quad, now)

    for copy in outgoing:
        copy.start()
    scale = (nope_dim + rope_dim) ** -0.5

    def head_rows(row):
        return pl.ds(pl.multiple_of(row * HEAD_PAD, 8), HEAD_PAD)

    def query(row):
        return jnp.concatenate([q_scr[col, head_rows(row), :] for col in range(kv_dim // 128)], axis=1)

    def score_part(row, slot, span):
        lat = lat_buf[slot, pl.ds(0, span)]
        score = lax.dot_general(query(row).astype(bf16), lat, nt, preferred_element_type=f32)
        q_rope = qr_scr[head_rows(row), :][:, :rope_dim].astype(bf16)
        return score + jnp.dot(q_rope, rope_buf[slot, :, pl.ds(0, span)], preferred_element_type=f32)

    def soft_part(row, score):
        key_pos = lax.broadcasted_iota(jnp.int32, score.shape, 1)
        score = jnp.where(key_pos < lens_ref[row], score * scale, -jnp.inf)
        q_rope = qr_scr[head_rows(row), :]
        own = jnp.sum(query(row) * nl_scr[pl.ds(row, 1), :], axis=-1, keepdims=True) + jnp.sum(q_rope * nr_scr[pl.ds(row, 1), :], axis=-1, keepdims=True)
        own = own * scale
        top = jnp.maximum(jnp.max(score, axis=-1, keepdims=True), own)
        weight = jnp.exp(score - top)
        own_weight = jnp.exp(own - top)
        total = jnp.sum(weight, axis=-1, keepdims=True) + own_weight
        return (weight / total).astype(bf16), (own_weight / total).astype(bf16).astype(f32)

    def mix_part(row, slot, prob, own_prob, span):
        mixed = jnp.dot(prob, lat_buf[slot, pl.ds(0, span)], preferred_element_type=f32) + own_prob * nl_scr[pl.ds(row, 1), :]
        mixed = mixed.astype(bf16).astype(f32)
        for col in range(kv_dim // 128):
            o_scr[col, head_rows(row), :] = mixed[:, col * 128:(col + 1) * 128]

    def members(group):
        return [(order[group * GROUP + sub], lax.rem(group * GROUP, RING) + sub) for sub in range(GROUP)]

    def wait_members(group):
        for sub, (row, slot) in enumerate(members(group)):
            lat_copy(group * GROUP + sub, slot).wait()
            rope_copy(row, slot).wait()

    def group_blocks(group):
        return (lens_ref[order[group * GROUP]] + 255) >> 8

    def by_span(blocks, run):
        for size, test in ((2, blocks <= 2), (3, blocks == 3), (4, blocks == 4)):
            pl.when(test)(functools.partial(run, size * cache_len // 4))

    first = members(0)
    wait_members(0)

    def first_scores(span):
        for sub, (row, slot) in enumerate(first):
            s_scr[sub, :, pl.ds(0, span)] = score_part(row, slot, span)

    by_span(group_blocks(0), first_scores)

    def group_step(group, _):
        now = members(group)
        later = members(group + 1)
        wait_members(group + 1)

        def run(span):
            pending = None
            for sub in range(GROUP):
                fresh = score_part(*later[sub], span)
                probs = soft_part(now[sub][0], s_scr[sub, :, pl.ds(0, span)])
                s_scr[sub, :, pl.ds(0, span)] = fresh
                if pending is not None:
                    mix_part(*pending, span)
                pending = (*now[sub], *probs)
            mix_part(*pending, span)

        by_span(group_blocks(group), run)

        @pl.when(group < groups - RING // GROUP)
        def _():
            for sub in range(GROUP):
                start_place(group * GROUP + RING + sub, now[sub][1])

        @pl.when(group == 0)
        def _():
            uv_copy.start()

        for extra in range(WO_STEP):
            part = group * WO_STEP + extra
            pl.when(part < WO_PARTS)(lambda part=part: wo_copy(part).start())
        return 0

    lax.fori_loop(0, groups - 1, group_step, 0)
    last = members(groups - 1)

    def last_mix(span):
        pending = None
        for sub in range(GROUP):
            probs = soft_part(last[sub][0], s_scr[sub, :, pl.ds(0, span)])
            if pending is not None:
                mix_part(*pending, span)
            pending = (*last[sub], *probs)
        mix_part(*pending, span)

    by_span(group_blocks(groups - 1), last_mix)
    uv_copy.wait()
    pltpu.make_async_copy(wo_hbm, wo, o_sems.at[1]).wait()
    for copy in outgoing:
        copy.wait()


def attn_call(hidden, cache_lat, cache_rope, seq_lens, gain_attn, w_dq, gain_q, w_uq, w_qr, w_dkv, gain_kv, w_uk, w_uv, w_o):
    rows, width = hidden.shape
    cache_len, kv_dim = cache_lat.shape[1:]
    rope_dim = cache_rope.shape[2]
    q_dim, heads, nope_dim = w_uq.shape
    bf16, f32 = jnp.bfloat16, jnp.float32
    vmem = pl.BlockSpec(memory_space=pltpu.VMEM)
    hbm = pl.BlockSpec(memory_space=pltpu.HBM)
    dma = pltpu.SemaphoreType.DMA
    rope_keys = jnp.swapaxes(cache_rope, 1, 2)
    dkv_t = w_dkv.T
    qr_t = jnp.transpose(w_qr, (1, 2, 0)).reshape(heads * rope_dim, q_dim)
    uq_t = jnp.transpose(w_uq, (1, 2, 0)).reshape(heads * nope_dim, q_dim)
    uk_t = jnp.transpose(w_uk, (1, 2, 0))
    uv_t = jnp.swapaxes(w_uv, 0, 1)
    handed = (
        pltpu.VMEM((kv_dim // 128, rows * HEAD_PAD, 128), f32),
        pltpu.VMEM(hidden.shape, bf16),
        pltpu.VMEM(uv_t.shape, bf16),
        pltpu.VMEM(w_o.shape, bf16),
    )
    return pl.pallas_call(
        attn_kernel,
        out_shape=(jax.ShapeDtypeStruct((rows, kv_dim), bf16), jax.ShapeDtypeStruct((rows, rope_dim), bf16)) + handed,
        in_specs=[hbm] * 14,
        out_specs=(hbm, hbm, vmem, vmem, vmem, vmem),
        scratch_shapes=[
            pltpu.VMEM(w_dq.shape, bf16),
            pltpu.VMEM(dkv_t.shape, bf16),
            pltpu.VMEM(uk_t.shape, bf16),
            pltpu.VMEM((RING, cache_len, kv_dim), bf16),
            pltpu.VMEM((RING, rope_dim, cache_len), bf16),
            pltpu.VMEM((kv_dim // 128, rows * HEAD_PAD, 128), f32),
            pltpu.VMEM((rows * HEAD_PAD, 128), f32),
            pltpu.VMEM((rows, kv_dim), f32),
            pltpu.VMEM((rows, 128), f32),
            pltpu.VMEM((GROUP, HEAD_PAD, cache_len), f32),
            pltpu.VMEM(gain_attn.shape, bf16),
            pltpu.VMEM(gain_q.shape, bf16),
            pltpu.VMEM(gain_kv.shape, bf16),
            pltpu.VMEM((rows, kv_dim), bf16),
            pltpu.VMEM((rows, rope_dim), bf16),
            pltpu.SMEM((rows,), jnp.int32),
            pltpu.SMEM((rows,), jnp.int32),
            pltpu.SMEM((9,), jnp.int32),
            dma((5,)), dma((2,)), dma((5,)), dma((2,)), dma((RING,)), dma((RING,)),
        ],
        compiler_params=pltpu.CompilerParams(vmem_limit_bytes=33 * 1024 * 1024),
        name="attention",
    )(seq_lens, hidden, gain_attn, gain_q, gain_kv, cache_lat, rope_keys, w_dq, dkv_t, qr_t, uq_t, uk_t, uv_t, w_o)


MESH = pl.DeviceIdType.MESH
CHUNKS = 4


def mlp_kernel(o_ref, hid_ref, wuv, wo, gm_hbm, wg_hbm, wu_hbm, wd_hbm, out_ref,
               gm_ref, wg, wu, wd, heads_scr, h_scr, gath, m_scr, keep, s1_send, s1_recv, s2_send, s2_recv,
               w_sems, near_send, near_recv, far_send, far_recv, fw_send, fw_recv, p1_send, p1_recv, p2_send, p2_recv):
    rows, width = hid_ref.shape
    part_width = width // CHUNKS
    heads, kv_dim, v_dim = wuv.shape
    f32, bf16 = jnp.float32, jnp.bfloat16
    me = lax.axis_index("g")
    core = lax.rem(me, 2)
    chip_x = lax.rem(me // 2, 2)
    chip_y = me // 4
    is_low = core == 0
    sibling = me + 1 - 2 * core
    mine = pl.ds(pl.multiple_of(core * rows, rows), rows)
    theirs = pl.ds(pl.multiple_of((1 - core) * rows, rows), rows)

    def peer(rel):
        return me + (rel % 2) * (2 - 4 * chip_x) + (rel // 2) * (4 - 8 * chip_y)

    def remote(src, dst, send, recv, target):
        return pltpu.make_async_remote_copy(src, dst, send, recv, device_id={"g": target}, device_id_type=MESH)

    def near_copy(rel, part):
        return remote(h_scr.at[part], gath.at[rel, part, mine], near_send.at[rel, part], near_recv.at[rel, part], peer(rel))

    def far_copy(rel):
        return remote(h_scr, gath.at[rel, :, mine], far_send.at[rel], far_recv.at[rel], sibling if rel == 0 else peer(rel))

    def sibling_rows_arrived():
        remote(h_scr, gath.at[0, :, theirs], far_send.at[0], far_recv.at[0], sibling).wait_recv()

    def forward_copy(rel):
        return remote(gath.at[rel, :, mine], gath.at[rel, :, mine], fw_send.at[rel], fw_recv.at[rel], sibling)

    def forward_arrived(rel):
        remote(gath.at[rel, :, theirs], gath.at[rel, :, theirs], fw_send.at[rel], fw_recv.at[rel], sibling).wait_recv()

    def pair_copy(rel):
        return remote(s1_send.at[rel], s1_recv.at[rel], p1_send.at[rel], p1_recv.at[rel], sibling)

    def chip_copy(rel):
        return remote(s2_send.at[rel], s2_recv.at[rel], p2_send.at[rel], p2_recv.at[rel], peer(rel))

    loads = [pltpu.make_async_copy(src, dst, w_sems.at[k]) for k, (src, dst) in enumerate(((wg_hbm, wg), (wu_hbm, wu), (wd_hbm, wd), (gm_hbm, gm_ref)))]
    for load in loads:
        load.start()
    barrier = pltpu.get_barrier_semaphore()
    for target in (sibling, peer(1), peer(2), peer(3)):
        pl.semaphore_signal(barrier, inc=1, device_id={"g": target}, device_id_type=MESH)

    for head in range(heads):
        cols = [o_ref[col, pl.ds(head, rows, stride=HEAD_PAD), :] for col in range(kv_dim // 128)]
        mixed = jnp.concatenate(cols, axis=1).astype(bf16)
        heads_scr[:, head * v_dim:(head + 1) * v_dim] = jnp.dot(mixed, wuv[head], preferred_element_type=f32).astype(bf16)

    def columns(part):
        return pl.ds(part * part_width, part_width)

    for part in range(CHUNKS):
        attn_out = jnp.dot(heads_scr[...], wo[:, columns(part)], preferred_element_type=f32)
        resid = (hid_ref[:, columns(part)].astype(f32) + attn_out).astype(bf16)
        h_scr[part] = resid
        gath[0, part, mine] = resid
        if part == 0:
            pl.semaphore_wait(barrier, 4)
        near_copy(1, part).start()
        near_copy(2, part).start()
    far_copy(3).start()
    far_copy(0).start()

    def normed_rows(rel, at):
        square = jnp.zeros((2 * rows, 1), f32)
        for part in range(CHUNKS):
            piece = gath[rel, part].astype(f32)
            square = square + jnp.sum(piece * piece, axis=-1, keepdims=True)
        factor = lax.rsqrt(square / width + 1e-6)
        for part in range(CHUNKS):
            piece = gath[rel, part].astype(f32) * factor * gm_ref[columns(part)].astype(f32)
            m_scr[pl.ds(at, 2 * rows), columns(part)] = piece.astype(bf16)

    def activation(count):
        block = m_scr[pl.ds(0, count)]
        gate = jnp.dot(block, wg[...], preferred_element_type=f32)
        up = jnp.dot(block, wu[...], preferred_element_type=f32)
        return (jax.nn.silu(gate) * up).astype(bf16)

    def contract(act, rels):
        part = jnp.dot(act, wd[...], preferred_element_type=f32)
        for index, rel in enumerate(rels):
            low = part[2 * index * rows:(2 * index + 1) * rows]
            high = part[(2 * index + 1) * rows:(2 * index + 2) * rows]
            s1_send[rel] = jnp.where(is_low, high, low)
            keep[rel] = jnp.where(is_low, low, high)
            pair_copy(rel).start()

    def send_sum(rel):
        pair_copy(rel).wait_recv()
        s2_send[rel] = (keep[rel] + s1_recv[rel]).astype(bf16)
        chip_copy(rel).start()

    for rel in (1, 2):
        for part in range(CHUNKS):
            near_copy(rel, part).wait_recv()
        forward_copy(rel).start()
    for load in loads:
        load.wait()
    forward_arrived(1)
    normed_rows(1, 0)
    forward_arrived(2)
    normed_rows(2, 2 * rows)
    contract(activation(4 * rows), (1, 2))
    far_copy(3).wait_recv()
    forward_copy(3).start()
    sibling_rows_arrived()
    normed_rows(0, 2 * rows)
    send_sum(1)
    send_sum(2)

    forward_arrived(3)
    normed_rows(3, 0)
    contract(activation(4 * rows), (3, 0))
    send_sum(3)
    pair_copy(0).wait_recv()

    cols = [h_scr[part].astype(f32) for part in range(CHUNKS)]
    total = jnp.concatenate(cols, axis=1) + (keep[0] + s1_recv[0])
    for rel in (1, 2, 3):
        chip_copy(rel).wait_recv()
        total = total + s2_recv[rel].astype(f32)
    out_ref[...] = total.astype(bf16)
    for rel in (1, 2):
        for part in range(CHUNKS):
            near_copy(rel, part).wait_send()
    far_copy(3).wait_send()
    far_copy(0).wait_send()
    for rel in range(4):
        pair_copy(rel).wait_send()
    for rel in (1, 2, 3):
        forward_copy(rel).wait_send()
        chip_copy(rel).wait_send()


def mlp_call(o_lat, hidden, w_uv, w_o, gain_mlp, w_gate, w_up, w_down):
    rows, width = hidden.shape
    cols = w_gate.shape[1]
    bf16, f32 = jnp.bfloat16, jnp.float32
    vmem = pl.BlockSpec(memory_space=pltpu.VMEM)
    hbm = pl.BlockSpec(memory_space=pltpu.HBM)
    dma = pltpu.SemaphoreType.DMA
    part_width = width // CHUNKS
    held = [pltpu.with_memory_space_constraint(x, pltpu.VMEM) for x in (o_lat, hidden, w_uv, w_o)]
    streamed = [pltpu.with_memory_space_constraint(x, pltpu.HBM) for x in (w_gate, w_up, w_down)]
    return pl.pallas_call(
        mlp_kernel,
        out_shape=pltpu.VMEM((rows, width), bf16),
        in_specs=[vmem, vmem, vmem, vmem, hbm, hbm, hbm, hbm],
        out_specs=vmem,
        scratch_shapes=[
            pltpu.VMEM(gain_mlp.shape, bf16),
            pltpu.VMEM((width, cols), bf16),
            pltpu.VMEM((width, cols), bf16),
            pltpu.VMEM((cols, width), bf16),
            pltpu.VMEM((rows, w_o.shape[0]), bf16),
            pltpu.VMEM((CHUNKS, rows, part_width), bf16),
            pltpu.VMEM((4, CHUNKS, 2 * rows, part_width), bf16),
            pltpu.VMEM((4 * rows, width), bf16),
            pltpu.VMEM((4, rows, width), f32),
            pltpu.VMEM((4, rows, width), f32),
            pltpu.VMEM((4, rows, width), f32),
            pltpu.VMEM((4, rows, width), bf16),
            pltpu.VMEM((4, rows, width), bf16),
            dma((4,)), dma((4, CHUNKS)), dma((4, CHUNKS)), dma((4,)), dma((4,)), dma((4,)), dma((4,)), dma((4,)), dma((4,)), dma((4,)), dma((4,)),
        ],
        compiler_params=pltpu.CompilerParams(collective_id=0, has_side_effects=True, vmem_limit_bytes=33 * 1024 * 1024),
        name="mlp_exchange",
    )(*held, gain_mlp, *streamed)


def solution(mesh):
    row_spec = P(("rep", "g"))
    full_spec = P()
    in_specs = (row_spec, row_spec, row_spec, row_spec, full_spec, full_spec, full_spec, full_spec, full_spec, full_spec, full_spec, full_spec, full_spec, full_spec, full_spec, P(None, "g"), P(None, "g"), P("g", None))

    def local_step(hidden, cache_lat, cache_rope, seq_lens, gain_attn, w_dq, gain_q, w_uq, w_qr, w_dkv, gain_kv, w_uk, w_uv, w_o, gain_mlp, w_gate, w_up, w_down):
        new_lat, new_rope, o_lat, hid_rows, uv_held, wo_held = attn_call(hidden, cache_lat, cache_rope, seq_lens, gain_attn, w_dq, gain_q, w_uq, w_qr, w_dkv, gain_kv, w_uk, w_uv, w_o)
        out_hidden = mlp_call(o_lat, hid_rows, uv_held, wo_held, gain_mlp, w_gate, w_up, w_down)
        return out_hidden, new_lat, new_rope

    return jax.shard_map(local_step, mesh=mesh, in_specs=in_specs, out_specs=(row_spec, row_spec, row_spec), check_vma=False)
```

```python
import functools

import jax
import jax.numpy as jnp
from jax import lax
from jax.experimental import pallas as pl
from jax.experimental.pallas import tpu as pltpu
from jax.sharding import PartitionSpec as P


HEADS = 20
HEAD_PAD = 24
RING = 24
GROUP = 4
VMEM_LIMIT = 43 * 1024 * 1024
WO_PARTS = 16
WO_STEP = 3


def attn_kernel(lens_hbm, hid_hbm, ga_hbm, gq_hbm, gkv_hbm, lat_hbm, rope_hbm, wdq_hbm, wdkv_hbm, wqr_hbm, wuq_hbm, wuk_hbm, wuv_hbm, wo_hbm,
                newlat_hbm, newrope_hbm, o_scr, hid_ref, wuv, wo,
                wdq, wdkv, wuk, lat_buf, rope_buf, q_scr, qr_scr, nl_scr, nr_scr, s_scr,
                ga_ref, gq_ref, gkv_ref, newlat_ref, newrope_ref, lens_ref, order, fill, w_sems, o_sems, in_sems, new_sems, lat_sems, rope_sems):
    rows = hid_ref.shape[0]
    kv_dim = lat_buf.shape[2]
    rope_dim = rope_buf.shape[1]
    cache_len = lat_buf.shape[1]
    nope_dim = wuk.shape[1]
    q_dim = wdq.shape[1]
    half = rope_dim // 2
    groups = rows // GROUP
    f32, bf16 = jnp.float32, jnp.bfloat16
    nt = (((1,), (1,)), ((), ()))

    wuq = wo.at[pl.ds(0, HEADS * nope_dim), pl.ds(0, q_dim)]
    wqr = wo.at[pl.ds(HEADS * nope_dim, HEADS * rope_dim), pl.ds(0, q_dim)]
    early = [pltpu.make_async_copy(src, dst, w_sems.at[k]) for k, (src, dst) in enumerate(((wdq_hbm, wdq), (wdkv_hbm, wdkv), (wqr_hbm, wqr), (wuq_hbm, wuq), (wuk_hbm, wuk)))]
    small = [pltpu.make_async_copy(src, dst, in_sems.at[k]) for k, (src, dst) in enumerate(((lens_hbm, lens_ref), (hid_hbm, hid_ref), (ga_hbm, ga_ref), (gq_hbm, gq_ref), (gkv_hbm, gkv_ref)))]
    for copy in small + early:
        copy.start()
    small[0].wait()

    def bucket(row):
        return 8 - ((lens_ref[row] + 127) >> 7)

    for k in range(9):
        fill[k] = 0

    def count(row, _):
        k = bucket(row)
        fill[k] = fill[k] + 1
        return 0

    lax.fori_loop(0, rows, count, 0)
    running = jnp.int32(0)
    for k in range(9):
        size = fill[k]
        fill[k] = running
        running = running + size

    def place(row, _):
        k = bucket(row)
        order[fill[k]] = row
        fill[k] = fill[k] + 1
        return 0

    lax.fori_loop(0, rows, place, 0)

    def lat_copy(place_id, slot):
        row = order[place_id]
        span = jnp.maximum((lens_ref[order[(place_id // GROUP) * GROUP]] + 255) >> 8, 2) << 8
        count = jnp.where(place_id < RING, span, ((lens_ref[row] + 15) >> 4) << 4)
        count = pl.multiple_of(count, 16)
        return pltpu.make_async_copy(lat_hbm.at[row, pl.ds(0, count)], lat_buf.at[slot, pl.ds(0, count)], lat_sems.at[slot])

    def rope_copy(row, slot):
        return pltpu.make_async_copy(rope_hbm.at[row], rope_buf.at[slot], rope_sems.at[slot])

    def start_place(place_id, slot):
        lat_copy(place_id, slot).start()
        rope_copy(order[place_id], slot).start()

    wo_rows = wo.shape[0] // WO_PARTS

    def wo_copy(part):
        span = pl.ds(pl.multiple_of(part * wo_rows, 32), wo_rows)
        return pltpu.make_async_copy(wo_hbm.at[span, pl.ds(0, wo.shape[1])], wo.at[span], o_sems.at[1])

    def fill_ring(slot, _):
        start_place(slot, slot)
        return 0

    lax.fori_loop(0, RING, fill_ring, 0)
    uv_copy = pltpu.make_async_copy(wuv_hbm, wuv, o_sems.at[0])

    def norm(values, gain_ref):
        mean_sq = jnp.mean(values * values, axis=-1, keepdims=True)
        return values * lax.rsqrt(mean_sq + 1e-6) * gain_ref[...].astype(f32)

    row_id = lax.broadcasted_iota(jnp.int32, (rows, 128), 0)
    position = jnp.zeros((rows, 128), jnp.int32)
    for row in range(rows):
        position = jnp.where(row_id == row, lens_ref[row], position)
    lane = lax.broadcasted_iota(jnp.int32, (rows, 128), 1)
    freq_id = lane & (half - 1)
    inv_freq = jnp.exp(freq_id.astype(f32) * (-jnp.log(jnp.float32(10000.0)) / half))
    angle = position.astype(f32) * inv_freq
    first_half = (lane & half) == 0
    cos_part = jnp.cos(angle)
    sin_part = jnp.where(first_half, -jnp.sin(angle), jnp.sin(angle))

    def rotate(values):
        swapped = jnp.where(first_half, pltpu.roll(values, 128 - half, 1), pltpu.roll(values, half, 1))
        return values * cos_part + swapped * sin_part

    small[1].wait()
    small[2].wait()
    hidden = hid_ref[...].astype(f32)
    normed = norm(hidden, ga_ref).astype(bf16)
    q_scr[...] = jnp.zeros_like(q_scr)
    qr_scr[...] = jnp.zeros_like(qr_scr)

    small[3].wait()
    small[4].wait()
    early[0].wait()
    q_raw = jnp.dot(normed, wdq[...], preferred_element_type=f32)
    early[1].wait()
    kv_raw = lax.dot_general(normed, wdkv[...], nt, preferred_element_type=f32)
    q_in = norm(q_raw, gq_ref).astype(bf16)
    early[2].wait()
    rope_raw = lax.dot_general(q_in, wo[pl.ds(HEADS * nope_dim, HEADS * rope_dim), pl.ds(0, q_dim)], nt, preferred_element_type=f32)
    new_lat = norm(kv_raw[:, :kv_dim], gkv_ref).astype(bf16)
    newlat_ref[...] = new_lat
    nl_scr[...] = new_lat.astype(f32)
    kv_rope = jnp.concatenate([kv_raw[:, kv_dim:], jnp.zeros((rows, 128 - rope_dim), f32)], axis=1)
    new_rope = rotate(kv_rope).astype(bf16)
    newrope_ref[...] = new_rope[:, :rope_dim]
    outgoing = [pltpu.make_async_copy(newlat_ref, newlat_hbm, new_sems.at[0]), pltpu.make_async_copy(newrope_ref, newrope_hbm, new_sems.at[1])]
    nr_scr[...] = jnp.where(lane < rope_dim, new_rope.astype(f32), 0.0)

    def nope_quad(quad):
        return lax.dot_general(q_in, wo[pl.ds(quad * 4 * nope_dim, 4 * nope_dim), pl.ds(0, q_dim)], nt, preferred_element_type=f32)

    def absorb_quad(quad, q_nope):
        for sub in range(4):
            head = quad * 4 + sub
            one = q_nope[:, sub * nope_dim:(sub + 1) * nope_dim].astype(bf16)
            q_abs = jnp.dot(one, wuk[head], preferred_element_type=f32).astype(bf16).astype(f32)
            for col in range(kv_dim // 128):
                q_scr[col, pl.ds(head, rows, stride=HEAD_PAD), :] = q_abs[:, col * 128:(col + 1) * 128]

    early[3].wait()
    quads = HEADS // 4
    ahead = nope_quad(0)
    for pair in range(HEADS // 2):
        turned = rotate(rope_raw[:, pair * 128:(pair + 1) * 128]).astype(bf16).astype(f32)
        qr_scr[pl.ds(2 * pair, rows, stride=HEAD_PAD), :] = turned
        qr_scr[pl.ds(2 * pair + 1, rows, stride=HEAD_PAD), :] = pltpu.roll(turned, rope_dim, 1)
    for quad in range(quads):
        now = ahead
        if quad + 1 < quads:
            ahead = nope_quad(quad + 1)
        if quad == 0:
            early[4].wait()
        absorb_quad(quad, now)

    for copy in outgoing:
        copy.start()
    scale = (nope_dim + rope_dim) ** -0.5

    def head_rows(row):
        return pl.ds(pl.multiple_of(row * HEAD_PAD, 8), HEAD_PAD)

    def query(row):
        return jnp.concatenate([q_scr[col, head_rows(row), :] for col in range(kv_dim // 128)], axis=1)

    def score_part(row, slot, span):
        lat = lat_buf[slot, pl.ds(0, span)]
        score = lax.dot_general(query(row).astype(bf16), lat, nt, preferred_element_type=f32)
        q_rope = qr_scr[head_rows(row), :][:, :rope_dim].astype(bf16)
        return score + jnp.dot(q_rope, rope_buf[slot, :, pl.ds(0, span)], preferred_element_type=f32)

    def soft_part(row, score):
        key_pos = lax.broadcasted_iota(jnp.int32, score.shape, 1)
        score = jnp.where(key_pos < lens_ref[row], score * scale, -jnp.inf)
        q_rope = qr_scr[head_rows(row), :]
        own = jnp.sum(query(row) * nl_scr[pl.ds(row, 1), :], axis=-1, keepdims=True) + jnp.sum(q_rope * nr_scr[pl.ds(row, 1), :], axis=-1, keepdims=True)
        own = own * scale
        top = jnp.maximum(jnp.max(score, axis=-1, keepdims=True), own)
        weight = jnp.exp(score - top)
        own_weight = jnp.exp(own - top)
        total = jnp.sum(weight, axis=-1, keepdims=True) + own_weight
        return (weight / total).astype(bf16), (own_weight / total).astype(bf16).astype(f32)

    def mix_part(row, slot, prob, own_prob, span):
        mixed = jnp.dot(prob, lat_buf[slot, pl.ds(0, span)], preferred_element_type=f32) + own_prob * nl_scr[pl.ds(row, 1), :]
        mixed = mixed.astype(bf16).astype(f32)
        for col in range(kv_dim // 128):
            o_scr[col, head_rows(row), :] = mixed[:, col * 128:(col + 1) * 128]

    def members(group):
        return [(order[group * GROUP + sub], lax.rem(group * GROUP, RING) + sub) for sub in range(GROUP)]

    def wait_members(group):
        for sub, (row, slot) in enumerate(members(group)):
            lat_copy(group * GROUP + sub, slot).wait()
            rope_copy(row, slot).wait()

    def group_blocks(group):
        return (lens_ref[order[group * GROUP]] + 255) >> 8

    def by_span(blocks, run):
        for size, test in ((2, blocks <= 2), (3, blocks == 3), (4, blocks == 4)):
            pl.when(test)(functools.partial(run, size * cache_len // 4))

    first = members(0)
    wait_members(0)

    def first_scores(span):
        for sub, (row, slot) in enumerate(first):
            s_scr[sub, :, pl.ds(0, span)] = score_part(row, slot, span)

    by_span(group_blocks(0), first_scores)

    def group_step(group, _):
        now = members(group)
        later = members(group + 1)
        wait_members(group + 1)

        def run(span):
            pending = None
            for sub in range(GROUP):
                fresh = score_part(*later[sub], span)
                probs = soft_part(now[sub][0], s_scr[sub, :, pl.ds(0, span)])
                s_scr[sub, :, pl.ds(0, span)] = fresh
                if pending is not None:
                    mix_part(*pending, span)
                pending = (*now[sub], *probs)
            mix_part(*pending, span)

        by_span(group_blocks(group), run)

        @pl.when(group < groups - RING // GROUP)
        def _():
            for sub in range(GROUP):
                start_place(group * GROUP + RING + sub, now[sub][1])

        @pl.when(group == 0)
        def _():
            uv_copy.start()

        for extra in range(WO_STEP):
            part = group * WO_STEP + extra
            pl.when(part < WO_PARTS)(lambda part=part: wo_copy(part).start())
        return 0

    lax.fori_loop(0, groups - 1, group_step, 0)
    last = members(groups - 1)

    def last_mix(span):
        pending = None
        for sub in range(GROUP):
            probs = soft_part(last[sub][0], s_scr[sub, :, pl.ds(0, span)])
            if pending is not None:
                mix_part(*pending, span)
            pending = (*last[sub], *probs)
        mix_part(*pending, span)

    by_span(group_blocks(groups - 1), last_mix)
    uv_copy.wait()
    pltpu.make_async_copy(wo_hbm.at[:, pl.ds(0, wo.shape[1])], wo, o_sems.at[1]).wait()
    for copy in outgoing:
        copy.wait()


def attn_call(hidden, cache_lat, cache_rope, seq_lens, gain_attn, w_dq, gain_q, w_uq, w_qr, w_dkv, gain_kv, w_uk, w_uv, w_o):
    rows, width = hidden.shape
    cache_len, kv_dim = cache_lat.shape[1:]
    rope_dim = cache_rope.shape[2]
    q_dim, heads, nope_dim = w_uq.shape
    bf16, f32 = jnp.bfloat16, jnp.float32
    vmem = pl.BlockSpec(memory_space=pltpu.VMEM)
    hbm = pl.BlockSpec(memory_space=pltpu.HBM)
    dma = pltpu.SemaphoreType.DMA
    rope_keys = jnp.swapaxes(cache_rope, 1, 2)
    dkv_t = w_dkv.T
    qr_t = jnp.transpose(w_qr, (1, 2, 0)).reshape(heads * rope_dim, q_dim)
    uq_t = jnp.transpose(w_uq, (1, 2, 0)).reshape(heads * nope_dim, q_dim)
    uk_t = jnp.transpose(w_uk, (1, 2, 0))
    uv_t = jnp.swapaxes(w_uv, 0, 1)
    handed = (
        pltpu.VMEM((kv_dim // 128, rows * HEAD_PAD, 128), f32),
        pltpu.VMEM(hidden.shape, bf16),
        pltpu.VMEM(uv_t.shape, bf16),
        pltpu.VMEM((w_o.shape[0], width // 2), bf16),
    )
    return pl.pallas_call(
        attn_kernel,
        out_shape=(jax.ShapeDtypeStruct((rows, kv_dim), bf16), jax.ShapeDtypeStruct((rows, rope_dim), bf16)) + handed,
        in_specs=[hbm] * 14,
        out_specs=(hbm, hbm, vmem, vmem, vmem, vmem),
        scratch_shapes=[
            pltpu.VMEM(w_dq.shape, bf16),
            pltpu.VMEM(dkv_t.shape, bf16),
            pltpu.VMEM(uk_t.shape, bf16),
            pltpu.VMEM((RING, cache_len, kv_dim), bf16),
            pltpu.VMEM((RING, rope_dim, cache_len), bf16),
            pltpu.VMEM((kv_dim // 128, rows * HEAD_PAD, 128), f32),
            pltpu.VMEM((rows * HEAD_PAD, 128), f32),
            pltpu.VMEM((rows, kv_dim), f32),
            pltpu.VMEM((rows, 128), f32),
            pltpu.VMEM((GROUP, HEAD_PAD, cache_len), f32),
            pltpu.VMEM(gain_attn.shape, bf16),
            pltpu.VMEM(gain_q.shape, bf16),
            pltpu.VMEM(gain_kv.shape, bf16),
            pltpu.VMEM((rows, kv_dim), bf16),
            pltpu.VMEM((rows, rope_dim), bf16),
            pltpu.SMEM((rows,), jnp.int32),
            pltpu.SMEM((rows,), jnp.int32),
            pltpu.SMEM((9,), jnp.int32),
            dma((5,)), dma((2,)), dma((5,)), dma((2,)), dma((RING,)), dma((RING,)),
        ],
        compiler_params=pltpu.CompilerParams(vmem_limit_bytes=VMEM_LIMIT),
        name="attention",
    )(seq_lens, hidden, gain_attn, gain_q, gain_kv, cache_lat, rope_keys, w_dq, dkv_t, qr_t, uq_t, uk_t, uv_t, w_o)


MESH = pl.DeviceIdType.MESH
CHUNKS = 4


def mlp_kernel(o_ref, hid_ref, wuv, wo_low, gm_hbm, wo_hbm, wg_hbm, wu_hbm, wd_hbm, out_ref,
               gm_ref, wo_high, wg, wu, wd, heads_scr, h_scr, gath, m_scr, keep, s1_send, s1_recv, s2_send, s2_recv,
               w_sems, wo_sems, near_send, near_recv, far_send, far_recv, fw_send, fw_recv, p1_send, p1_recv, p2_send, p2_recv):
    rows, width = hid_ref.shape
    part_width = width // CHUNKS
    heads, kv_dim, v_dim = wuv.shape
    f32, bf16 = jnp.float32, jnp.bfloat16
    me = lax.axis_index("g")
    core = lax.rem(me, 2)
    chip_x = lax.rem(me // 2, 2)
    chip_y = me // 4
    is_low = core == 0
    sibling = me + 1 - 2 * core
    mine = pl.ds(pl.multiple_of(core * rows, rows), rows)
    theirs = pl.ds(pl.multiple_of((1 - core) * rows, rows), rows)

    def peer(rel):
        return me + (rel % 2) * (2 - 4 * chip_x) + (rel // 2) * (4 - 8 * chip_y)

    def remote(src, dst, send, recv, target):
        return pltpu.make_async_remote_copy(src, dst, send, recv, device_id={"g": target}, device_id_type=MESH)

    def near_copy(rel, part):
        return remote(h_scr.at[part], gath.at[rel, part, mine], near_send.at[rel, part], near_recv.at[rel, part], peer(rel))

    def far_copy(rel):
        return remote(h_scr, gath.at[rel, :, mine], far_send.at[rel], far_recv.at[rel], sibling)

    def sibling_rows_arrived():
        remote(h_scr, gath.at[0, :, theirs], far_send.at[0], far_recv.at[0], sibling).wait_recv()

    def forward_copy(rel):
        return remote(gath.at[rel, :, mine], gath.at[rel, :, mine], fw_send.at[rel], fw_recv.at[rel], sibling)

    def forward_arrived(rel):
        remote(gath.at[rel, :, theirs], gath.at[rel, :, theirs], fw_send.at[rel], fw_recv.at[rel], sibling).wait_recv()

    def pair_copy(rel):
        return remote(s1_send.at[rel], s1_recv.at[rel], p1_send.at[rel], p1_recv.at[rel], sibling)

    def chip_copy(rel):
        return remote(s2_send.at[rel], s2_recv.at[rel], p2_send.at[rel], p2_recv.at[rel], peer(rel))

    half_width = wo_low.shape[1]
    late = [pltpu.make_async_copy(wo_hbm.at[:, pl.ds(half_width + k * part_width, part_width)], wo_high.at[k], wo_sems.at[k]) for k in range(2)]
    loads = [pltpu.make_async_copy(src, dst, w_sems.at[k]) for k, (src, dst) in enumerate(((wg_hbm, wg), (wu_hbm, wu), (wd_hbm, wd), (gm_hbm, gm_ref)))]
    for load in late + loads:
        load.start()
    barrier = pltpu.get_barrier_semaphore()
    for target in (sibling, peer(1), peer(2), peer(3)):
        pl.semaphore_signal(barrier, inc=1, device_id={"g": target}, device_id_type=MESH)

    for head in range(heads):
        cols = [o_ref[col, pl.ds(head, rows, stride=HEAD_PAD), :] for col in range(kv_dim // 128)]
        mixed = jnp.concatenate(cols, axis=1).astype(bf16)
        heads_scr[:, head * v_dim:(head + 1) * v_dim] = jnp.dot(mixed, wuv[head], preferred_element_type=f32).astype(bf16)

    def columns(part):
        return pl.ds(part * part_width, part_width)

    for part in range(CHUNKS):
        if part < 2:
            weights = wo_low[:, columns(part)]
        else:
            late[part - 2].wait()
            weights = wo_high[part - 2]
        attn_out = jnp.dot(heads_scr[...], weights, preferred_element_type=f32)
        resid = (hid_ref[:, columns(part)].astype(f32) + attn_out).astype(bf16)
        h_scr[part] = resid
        gath[0, part, mine] = resid
        if part == 0:
            pl.semaphore_wait(barrier, 4)
        near_copy(1, part).start()
        near_copy(2, part).start()
        if part > 0:
            near_copy(3, part - 1).start()
    near_copy(3, CHUNKS - 1).start()
    far_copy(0).start()

    def normed_rows(rel, at):
        square = jnp.zeros((2 * rows, 1), f32)
        for part in range(CHUNKS):
            piece = gath[rel, part].astype(f32)
            square = square + jnp.sum(piece * piece, axis=-1, keepdims=True)
        factor = lax.rsqrt(square / width + 1e-6)
        for part in range(CHUNKS):
            piece = gath[rel, part].astype(f32) * factor * gm_ref[columns(part)].astype(f32)
            m_scr[pl.ds(at, 2 * rows), columns(part)] = piece.astype(bf16)

    def activation(count):
        block = m_scr[pl.ds(0, count)]
        gate = jnp.dot(block, wg[...], preferred_element_type=f32)
        up = jnp.dot(block, wu[...], preferred_element_type=f32)
        return (jax.nn.silu(gate) * up).astype(bf16)

    def contract(act, rels):
        part = jnp.dot(act, wd[...], preferred_element_type=f32)
        for index, rel in enumerate(rels):
            low = part[2 * index * rows:(2 * index + 1) * rows]
            high = part[(2 * index + 1) * rows:(2 * index + 2) * rows]
            s1_send[rel] = jnp.where(is_low, high, low)
            keep[rel] = jnp.where(is_low, low, high)
            pair_copy(rel).start()

    def send_sum(rel):
        pair_copy(rel).wait_recv()
        s2_send[rel] = (keep[rel] + s1_recv[rel]).astype(bf16)
        chip_copy(rel).start()

    for rel in (1, 2):
        for part in range(CHUNKS):
            near_copy(rel, part).wait_recv()
        forward_copy(rel).start()
    for load in loads:
        load.wait()
    forward_arrived(1)
    normed_rows(1, 0)
    forward_arrived(2)
    normed_rows(2, 2 * rows)
    contract(activation(4 * rows), (1, 2))
    for part in range(CHUNKS):
        near_copy(3, part).wait_recv()
    forward_copy(3).start()
    sibling_rows_arrived()
    normed_rows(0, 2 * rows)

    forward_arrived(3)
    normed_rows(3, 0)
    act = activation(4 * rows)
    send_sum(1)
    send_sum(2)
    contract(act, (3, 0))
    send_sum(3)
    pair_copy(0).wait_recv()

    cols = [h_scr[part].astype(f32) for part in range(CHUNKS)]
    total = jnp.concatenate(cols, axis=1) + (keep[0] + s1_recv[0])
    for rel in (1, 2, 3):
        chip_copy(rel).wait_recv()
        total = total + s2_recv[rel].astype(f32)
    out_ref[...] = total.astype(bf16)
    for rel in (1, 2, 3):
        for part in range(CHUNKS):
            near_copy(rel, part).wait_send()
    far_copy(0).wait_send()
    for rel in range(4):
        pair_copy(rel).wait_send()
    for rel in (1, 2, 3):
        forward_copy(rel).wait_send()
        chip_copy(rel).wait_send()


def mlp_call(o_lat, hidden, w_uv, wo_low, gain_mlp, w_o, w_gate, w_up, w_down):
    rows, width = hidden.shape
    cols = w_gate.shape[1]
    bf16, f32 = jnp.bfloat16, jnp.float32
    vmem = pl.BlockSpec(memory_space=pltpu.VMEM)
    hbm = pl.BlockSpec(memory_space=pltpu.HBM)
    dma = pltpu.SemaphoreType.DMA
    part_width = width // CHUNKS
    held = [pltpu.with_memory_space_constraint(x, pltpu.VMEM) for x in (o_lat, hidden, w_uv, wo_low)]
    streamed = [pltpu.with_memory_space_constraint(x, pltpu.HBM) for x in (w_o, w_gate, w_up, w_down)]
    return pl.pallas_call(
        mlp_kernel,
        out_shape=pltpu.VMEM((rows, width), bf16),
        in_specs=[vmem, vmem, vmem, vmem, hbm, hbm, hbm, hbm, hbm],
        out_specs=vmem,
        scratch_shapes=[
            pltpu.VMEM(gain_mlp.shape, bf16),
            pltpu.VMEM((2, w_o.shape[0], part_width), bf16),
            pltpu.VMEM((width, cols), bf16),
            pltpu.VMEM((width, cols), bf16),
            pltpu.VMEM((cols, width), bf16),
            pltpu.VMEM((rows, w_o.shape[0]), bf16),
            pltpu.VMEM((CHUNKS, rows, part_width), bf16),
            pltpu.VMEM((4, CHUNKS, 2 * rows, part_width), bf16),
            pltpu.VMEM((4 * rows, width), bf16),
            pltpu.VMEM((4, rows, width), f32),
            pltpu.VMEM((4, rows, width), f32),
            pltpu.VMEM((4, rows, width), f32),
            pltpu.VMEM((4, rows, width), bf16),
            pltpu.VMEM((4, rows, width), bf16),
            dma((4,)), dma((2,)), dma((4, CHUNKS)), dma((4, CHUNKS)), dma((4,)), dma((4,)), dma((4,)), dma((4,)), dma((4,)), dma((4,)), dma((4,)), dma((4,)),
        ],
        compiler_params=pltpu.CompilerParams(collective_id=0, has_side_effects=True, vmem_limit_bytes=VMEM_LIMIT),
        name="mlp_exchange",
    )(*held, gain_mlp, *streamed)


def solution(mesh):
    row_spec = P(("rep", "g"))
    full_spec = P()
    in_specs = (row_spec, row_spec, row_spec, row_spec, full_spec, full_spec, full_spec, full_spec, full_spec, full_spec, full_spec, full_spec, full_spec, full_spec, full_spec, P(None, "g"), P(None, "g"), P("g", None))

    def local_step(hidden, cache_lat, cache_rope, seq_lens, gain_attn, w_dq, gain_q, w_uq, w_qr, w_dkv, gain_kv, w_uk, w_uv, w_o, gain_mlp, w_gate, w_up, w_down):
        new_lat, new_rope, o_lat, hid_rows, uv_held, wo_held = attn_call(hidden, cache_lat, cache_rope, seq_lens, gain_attn, w_dq, gain_q, w_uq, w_qr, w_dkv, gain_kv, w_uk, w_uv, w_o)
        out_hidden = mlp_call(o_lat, hid_rows, uv_held, wo_held, gain_mlp, w_o, w_gate, w_up, w_down)
        return out_hidden, new_lat, new_rope

    return jax.shard_map(local_step, mesh=mesh, in_specs=in_specs, out_specs=(row_spec, row_spec, row_spec), check_vma=False)
```

```python
import functools

import jax
import jax.numpy as jnp
from jax import lax
from jax.experimental import pallas as pl
from jax.experimental.pallas import tpu as pltpu
from jax.sharding import PartitionSpec as P


HEADS = 20
HEAD_PAD = 24
RING = 20
GROUP = 4
VMEM_LIMIT = 39 * 1024 * 1024
WO_PARTS = 16
WO_STEP = 3


def attn_kernel(lens_hbm, hid_hbm, ga_hbm, gq_hbm, gkv_hbm, lat_hbm, rope_hbm, wdq_hbm, wdkv_hbm, wqr_hbm, wuq_hbm, wuk_hbm, wuv_hbm, wo_hbm,
                newlat_hbm, newrope_hbm, o_scr, hid_ref, wuv, wo,
                wdq, wdkv, wuk, lat_buf, rope_buf, q_scr, qr_scr, nl_scr, nr_scr, s_scr,
                ga_ref, gq_ref, gkv_ref, newlat_ref, newrope_ref, lens_ref, order, fill, w_sems, o_sems, in_sems, new_sems, lat_sems, rope_sems):
    rows = hid_ref.shape[0]
    kv_dim = lat_buf.shape[2]
    rope_dim = rope_buf.shape[1]
    cache_len = lat_buf.shape[1]
    nope_dim = wuk.shape[1]
    q_dim = wdq.shape[1]
    half = rope_dim // 2
    groups = rows // GROUP
    f32, bf16 = jnp.float32, jnp.bfloat16
    nt = (((1,), (1,)), ((), ()))

    wqr = wo.at[pl.ds(HEADS * nope_dim, HEADS * rope_dim), pl.ds(0, q_dim)]
    cut = 8 * nope_dim
    uq_low = wo.at[pl.ds(0, cut), pl.ds(0, q_dim)]
    uq_high = wo.at[pl.ds(cut, HEADS * nope_dim - cut), pl.ds(0, q_dim)]
    pairs = ((wdq_hbm, wdq), (wdkv_hbm, wdkv), (wqr_hbm, wqr), (wuq_hbm.at[pl.ds(0, cut)], uq_low), (wuq_hbm.at[pl.ds(cut, HEADS * nope_dim - cut)], uq_high), (wuk_hbm, wuk))
    early = [pltpu.make_async_copy(src, dst, w_sems.at[k]) for k, (src, dst) in enumerate(pairs)]
    small = [pltpu.make_async_copy(src, dst, in_sems.at[k]) for k, (src, dst) in enumerate(((lens_hbm, lens_ref), (hid_hbm, hid_ref), (ga_hbm, ga_ref), (gq_hbm, gq_ref), (gkv_hbm, gkv_ref)))]
    for copy in small + early[:2]:
        copy.start()
    small[0].wait()

    def bucket(row):
        return 8 - ((lens_ref[row] + 127) >> 7)

    for k in range(9):
        fill[k] = 0

    def count(row, _):
        k = bucket(row)
        fill[k] = fill[k] + 1
        return 0

    lax.fori_loop(0, rows, count, 0)
    running = jnp.int32(0)
    for k in range(9):
        size = fill[k]
        fill[k] = running
        running = running + size

    def place(row, _):
        k = bucket(row)
        order[fill[k]] = row
        fill[k] = fill[k] + 1
        return 0

    lax.fori_loop(0, rows, place, 0)

    def lat_copy(place_id, slot):
        row = order[place_id]
        span = jnp.maximum((lens_ref[order[(place_id // GROUP) * GROUP]] + 255) >> 8, 2) << 8
        count = jnp.where(place_id < RING, span, ((lens_ref[row] + 15) >> 4) << 4)
        count = pl.multiple_of(count, 16)
        return pltpu.make_async_copy(lat_hbm.at[row, pl.ds(0, count)], lat_buf.at[slot, pl.ds(0, count)], lat_sems.at[slot])

    def rope_copy(row, slot):
        return pltpu.make_async_copy(rope_hbm.at[row], rope_buf.at[slot], rope_sems.at[slot])

    def start_place(place_id, slot):
        lat_copy(place_id, slot).start()
        rope_copy(order[place_id], slot).start()

    wo_rows = wo.shape[0] // WO_PARTS

    def wo_copy(part):
        span = pl.ds(pl.multiple_of(part * wo_rows, 32), wo_rows)
        return pltpu.make_async_copy(wo_hbm.at[span, pl.ds(0, wo.shape[1])], wo.at[span], o_sems.at[1])

    def start_group(group):
        for sub in range(GROUP):
            start_place(group * GROUP + sub, lax.rem(group * GROUP, RING) + sub)

    uv_copy = pltpu.make_async_copy(wuv_hbm, wuv, o_sems.at[0])

    def norm(values, gain_ref):
        mean_sq = jnp.mean(values * values, axis=-1, keepdims=True)
        return values * lax.rsqrt(mean_sq + 1e-6) * gain_ref[...].astype(f32)

    row_id = lax.broadcasted_iota(jnp.int32, (rows, 128), 0)
    position = jnp.zeros((rows, 128), jnp.int32)
    for row in range(rows):
        position = jnp.where(row_id == row, lens_ref[row], position)
    lane = lax.broadcasted_iota(jnp.int32, (rows, 128), 1)
    freq_id = lane & (half - 1)
    inv_freq = jnp.exp(freq_id.astype(f32) * (-jnp.log(jnp.float32(10000.0)) / half))
    angle = position.astype(f32) * inv_freq
    first_half = (lane & half) == 0
    cos_part = jnp.cos(angle)
    sin_part = jnp.where(first_half, -jnp.sin(angle), jnp.sin(angle))

    def rotate(values):
        swapped = jnp.where(first_half, pltpu.roll(values, 128 - half, 1), pltpu.roll(values, half, 1))
        return values * cos_part + swapped * sin_part

    small[1].wait()
    small[2].wait()
    hidden = hid_ref[...].astype(f32)
    normed = norm(hidden, ga_ref).astype(bf16)
    q_scr[...] = jnp.zeros_like(q_scr)
    qr_scr[...] = jnp.zeros_like(qr_scr)

    small[3].wait()
    small[4].wait()
    early[0].wait()
    early[2].start()
    early[3].start()
    q_raw = jnp.dot(normed, wdq[...], preferred_element_type=f32)
    early[1].wait()
    early[4].start()
    kv_raw = lax.dot_general(normed, wdkv[...], nt, preferred_element_type=f32)
    q_in = norm(q_raw, gq_ref).astype(bf16)
    early[2].wait()
    early[5].start()
    rope_raw = lax.dot_general(q_in, wo[pl.ds(HEADS * nope_dim, HEADS * rope_dim), pl.ds(0, q_dim)], nt, preferred_element_type=f32)
    new_lat = norm(kv_raw[:, :kv_dim], gkv_ref).astype(bf16)
    newlat_ref[...] = new_lat
    nl_scr[...] = new_lat.astype(f32)
    kv_rope = jnp.concatenate([kv_raw[:, kv_dim:], jnp.zeros((rows, 128 - rope_dim), f32)], axis=1)
    new_rope = rotate(kv_rope).astype(bf16)
    newrope_ref[...] = new_rope[:, :rope_dim]
    outgoing = [pltpu.make_async_copy(newlat_ref, newlat_hbm, new_sems.at[0]), pltpu.make_async_copy(newrope_ref, newrope_hbm, new_sems.at[1])]
    nr_scr[...] = jnp.where(lane < rope_dim, new_rope.astype(f32), 0.0)

    def nope_quad(quad):
        return lax.dot_general(q_in, wo[pl.ds(quad * 4 * nope_dim, 4 * nope_dim), pl.ds(0, q_dim)], nt, preferred_element_type=f32)

    def absorb_quad(quad, q_nope):
        for sub in range(4):
            head = quad * 4 + sub
            one = q_nope[:, sub * nope_dim:(sub + 1) * nope_dim].astype(bf16)
            q_abs = jnp.dot(one, wuk[head], preferred_element_type=f32).astype(bf16).astype(f32)
            for col in range(kv_dim // 128):
                q_scr[col, pl.ds(head, rows, stride=HEAD_PAD), :] = q_abs[:, col * 128:(col + 1) * 128]

    early[3].wait()
    start_group(0)
    quads = HEADS // 4
    ahead = nope_quad(0)
    for pair in range(HEADS // 2):
        turned = rotate(rope_raw[:, pair * 128:(pair + 1) * 128]).astype(bf16).astype(f32)
        qr_scr[pl.ds(2 * pair, rows, stride=HEAD_PAD), :] = turned
        qr_scr[pl.ds(2 * pair + 1, rows, stride=HEAD_PAD), :] = pltpu.roll(turned, rope_dim, 1)
    ahead2 = nope_quad(1)
    early[4].wait()
    start_group(1)
    pending_quads = [ahead, ahead2, nope_quad(2)]
    early[5].wait()
    start_group(2)
    for quad in range(quads):
        absorb_quad(quad, pending_quads[quad])
        if quad + 3 < quads:
            pending_quads.append(nope_quad(quad + 3))

    for copy in outgoing:
        copy.start()
    scale = (nope_dim + rope_dim) ** -0.5

    def head_rows(row):
        return pl.ds(pl.multiple_of(row * HEAD_PAD, 8), HEAD_PAD)

    def query(row):
        return jnp.concatenate([q_scr[col, head_rows(row), :] for col in range(kv_dim // 128)], axis=1)

    def score_part(row, slot, span):
        lat = lat_buf[slot, pl.ds(0, span)]
        score = lax.dot_general(query(row).astype(bf16), lat, nt, preferred_element_type=f32)
        q_rope = qr_scr[head_rows(row), :][:, :rope_dim].astype(bf16)
        return score + jnp.dot(q_rope, rope_buf[slot, :, pl.ds(0, span)], preferred_element_type=f32)

    def soft_part(row, score):
        key_pos = lax.broadcasted_iota(jnp.int32, score.shape, 1)
        score = jnp.where(key_pos < lens_ref[row], score * scale, -jnp.inf)
        q_rope = qr_scr[head_rows(row), :]
        own = jnp.sum(query(row) * nl_scr[pl.ds(row, 1), :], axis=-1, keepdims=True) + jnp.sum(q_rope * nr_scr[pl.ds(row, 1), :], axis=-1, keepdims=True)
        own = own * scale
        top = jnp.maximum(jnp.max(score, axis=-1, keepdims=True), own)
        weight = jnp.exp(score - top)
        own_weight = jnp.exp(own - top)
        total = jnp.sum(weight, axis=-1, keepdims=True) + own_weight
        return (weight / total).astype(bf16), (own_weight / total).astype(bf16).astype(f32)

    def mix_part(row, slot, prob, own_prob, span):
        mixed = jnp.dot(prob, lat_buf[slot, pl.ds(0, span)], preferred_element_type=f32) + own_prob * nl_scr[pl.ds(row, 1), :]
        mixed = mixed.astype(bf16).astype(f32)
        for col in range(kv_dim // 128):
            o_scr[col, head_rows(row), :] = mixed[:, col * 128:(col + 1) * 128]

    def members(group):
        return [(order[group * GROUP + sub], lax.rem(group * GROUP, RING) + sub) for sub in range(GROUP)]

    def wait_members(group):
        for sub, (row, slot) in enumerate(members(group)):
            lat_copy(group * GROUP + sub, slot).wait()
            rope_copy(row, slot).wait()

    def group_blocks(group):
        return (lens_ref[order[group * GROUP]] + 255) >> 8

    def by_span(blocks, run):
        for size, test in ((2, blocks <= 2), (3, blocks == 3), (4, blocks == 4)):
            pl.when(test)(functools.partial(run, size * cache_len // 4))

    first = members(0)
    wait_members(0)
    start_group(3)

    def first_scores(span):
        for sub, (row, slot) in enumerate(first):
            s_scr[sub, :, pl.ds(0, span)] = score_part(row, slot, span)

    by_span(group_blocks(0), first_scores)

    def group_step(group, _):
        now = members(group)
        later = members(group + 1)
        wait_members(group + 1)
        pl.when(group + 4 < groups)(lambda: start_group(group + 4))
        pl.when(group == 0)(uv_copy.start)
        for extra in range(WO_STEP):
            part = group * WO_STEP + extra
            pl.when(part < WO_PARTS)(lambda part=part: wo_copy(part).start())

        def run(span):
            pending = None
            for sub in range(GROUP):
                fresh = score_part(*later[sub], span)
                probs = soft_part(now[sub][0], s_scr[sub, :, pl.ds(0, span)])
                s_scr[sub, :, pl.ds(0, span)] = fresh
                if pending is not None:
                    mix_part(*pending, span)
                pending = (*now[sub], *probs)
            mix_part(*pending, span)

        by_span(group_blocks(group), run)

        return 0

    lax.fori_loop(0, groups - 1, group_step, 0)
    last = members(groups - 1)

    def last_mix(span):
        pending = None
        for sub in range(GROUP):
            probs = soft_part(last[sub][0], s_scr[sub, :, pl.ds(0, span)])
            if pending is not None:
                mix_part(*pending, span)
            pending = (*last[sub], *probs)
        mix_part(*pending, span)

    by_span(group_blocks(groups - 1), last_mix)
    uv_copy.wait()
    pltpu.make_async_copy(wo_hbm.at[:, pl.ds(0, wo.shape[1])], wo, o_sems.at[1]).wait()
    for copy in outgoing:
        copy.wait()


def attn_call(hidden, cache_lat, cache_rope, seq_lens, gain_attn, w_dq, gain_q, w_uq, w_qr, w_dkv, gain_kv, w_uk, w_uv, w_o):
    rows, width = hidden.shape
    cache_len, kv_dim = cache_lat.shape[1:]
    rope_dim = cache_rope.shape[2]
    q_dim, heads, nope_dim = w_uq.shape
    bf16, f32 = jnp.bfloat16, jnp.float32
    vmem = pl.BlockSpec(memory_space=pltpu.VMEM)
    hbm = pl.BlockSpec(memory_space=pltpu.HBM)
    dma = pltpu.SemaphoreType.DMA
    rope_keys = jnp.swapaxes(cache_rope, 1, 2)
    dkv_t = w_dkv.T
    qr_t = jnp.transpose(w_qr, (1, 2, 0)).reshape(heads * rope_dim, q_dim)
    uq_t = jnp.transpose(w_uq, (1, 2, 0)).reshape(heads * nope_dim, q_dim)
    uk_t = jnp.transpose(w_uk, (1, 2, 0))
    uv_t = jnp.swapaxes(w_uv, 0, 1)
    handed = (
        pltpu.VMEM((kv_dim // 128, rows * HEAD_PAD, 128), f32),
        pltpu.VMEM(hidden.shape, bf16),
        pltpu.VMEM(uv_t.shape, bf16),
        pltpu.VMEM((w_o.shape[0], width * 3 // 4), bf16),
    )
    return pl.pallas_call(
        attn_kernel,
        out_shape=(jax.ShapeDtypeStruct((rows, kv_dim), bf16), jax.ShapeDtypeStruct((rows, rope_dim), bf16)) + handed,
        in_specs=[hbm] * 14,
        out_specs=(hbm, hbm, vmem, vmem, vmem, vmem),
        scratch_shapes=[
            pltpu.VMEM(w_dq.shape, bf16),
            pltpu.VMEM(dkv_t.shape, bf16),
            pltpu.VMEM(uk_t.shape, bf16),
            pltpu.VMEM((RING, cache_len, kv_dim), bf16),
            pltpu.VMEM((RING, rope_dim, cache_len), bf16),
            pltpu.VMEM((kv_dim // 128, rows * HEAD_PAD, 128), f32),
            pltpu.VMEM((rows * HEAD_PAD, 128), f32),
            pltpu.VMEM((rows, kv_dim), f32),
            pltpu.VMEM((rows, 128), f32),
            pltpu.VMEM((GROUP, HEAD_PAD, cache_len), f32),
            pltpu.VMEM(gain_attn.shape, bf16),
            pltpu.VMEM(gain_q.shape, bf16),
            pltpu.VMEM(gain_kv.shape, bf16),
            pltpu.VMEM((rows, kv_dim), bf16),
            pltpu.VMEM((rows, rope_dim), bf16),
            pltpu.SMEM((rows,), jnp.int32),
            pltpu.SMEM((rows,), jnp.int32),
            pltpu.SMEM((9,), jnp.int32),
            dma((6,)), dma((2,)), dma((5,)), dma((2,)), dma((RING,)), dma((RING,)),
        ],
        compiler_params=pltpu.CompilerParams(vmem_limit_bytes=VMEM_LIMIT),
        name="attention",
    )(seq_lens, hidden, gain_attn, gain_q, gain_kv, cache_lat, rope_keys, w_dq, dkv_t, qr_t, uq_t, uk_t, uv_t, w_o)


MESH = pl.DeviceIdType.MESH
CHUNKS = 4


def mlp_kernel(o_ref, hid_ref, wuv, wo_low, gm_hbm, wo_hbm, wg_hbm, wu_hbm, wd_hbm, out_ref,
               gm_ref, wo_high, wg, wu, wd, heads_scr, h_scr, gath, m_scr, keep, s1_send, s1_recv, s2_send, s2_recv,
               w_sems, wo_sem, near_send, near_recv, far_send, far_recv, fw_send, fw_recv, p1_send, p1_recv, p2_send, p2_recv):
    rows, width = hid_ref.shape
    part_width = width // CHUNKS
    heads, kv_dim, v_dim = wuv.shape
    f32, bf16 = jnp.float32, jnp.bfloat16
    me = lax.axis_index("g")
    core = lax.rem(me, 2)
    chip_x = lax.rem(me // 2, 2)
    chip_y = me // 4
    is_low = core == 0
    sibling = me + 1 - 2 * core
    mine = pl.ds(pl.multiple_of(core * rows, rows), rows)
    theirs = pl.ds(pl.multiple_of((1 - core) * rows, rows), rows)

    def peer(rel):
        return me + (rel % 2) * (2 - 4 * chip_x) + (rel // 2) * (4 - 8 * chip_y)

    def remote(src, dst, send, recv, target):
        return pltpu.make_async_remote_copy(src, dst, send, recv, device_id={"g": target}, device_id_type=MESH)

    def near_copy(rel, part):
        return remote(h_scr.at[part], gath.at[rel, part, mine], near_send.at[rel, part], near_recv.at[rel, part], peer(rel))

    def far_copy(rel):
        return remote(h_scr, gath.at[rel, :, mine], far_send.at[rel], far_recv.at[rel], sibling)

    def sibling_rows_arrived():
        remote(h_scr, gath.at[0, :, theirs], far_send.at[0], far_recv.at[0], sibling).wait_recv()

    def forward_copy(rel):
        return remote(gath.at[rel, :, mine], gath.at[rel, :, mine], fw_send.at[rel], fw_recv.at[rel], sibling)

    def forward_arrived(rel):
        remote(gath.at[rel, :, theirs], gath.at[rel, :, theirs], fw_send.at[rel], fw_recv.at[rel], sibling).wait_recv()

    def pair_copy(rel):
        return remote(s1_send.at[rel], s1_recv.at[rel], p1_send.at[rel], p1_recv.at[rel], sibling)

    def chip_copy(rel):
        return remote(s2_send.at[rel], s2_recv.at[rel], p2_send.at[rel], p2_recv.at[rel], peer(rel))

    held_width = wo_low.shape[1]
    late = pltpu.make_async_copy(wo_hbm.at[:, pl.ds(held_width, part_width)], wo_high, wo_sem)
    loads = [pltpu.make_async_copy(src, dst, w_sems.at[k]) for k, (src, dst) in enumerate(((wg_hbm, wg), (wu_hbm, wu), (wd_hbm, wd), (gm_hbm, gm_ref)))]
    late.start()
    barrier = pltpu.get_barrier_semaphore()
    for target in (sibling, peer(1), peer(2), peer(3)):
        pl.semaphore_signal(barrier, inc=1, device_id={"g": target}, device_id_type=MESH)

    for head in range(heads):
        cols = [o_ref[col, pl.ds(head, rows, stride=HEAD_PAD), :] for col in range(kv_dim // 128)]
        mixed = jnp.concatenate(cols, axis=1).astype(bf16)
        heads_scr[:, head * v_dim:(head + 1) * v_dim] = jnp.dot(mixed, wuv[head], preferred_element_type=f32).astype(bf16)

    def columns(part):
        return pl.ds(part * part_width, part_width)

    for part in range(CHUNKS):
        if part < CHUNKS - 1:
            weights = wo_low[:, columns(part)]
        else:
            late.wait()
            weights = wo_high[...]
        attn_out = jnp.dot(heads_scr[...], weights, preferred_element_type=f32)
        resid = (hid_ref[:, columns(part)].astype(f32) + attn_out).astype(bf16)
        h_scr[part] = resid
        gath[0, part, mine] = resid
        if part == 0:
            for load in loads:
                load.start()
            pl.semaphore_wait(barrier, 4)
        near_copy(1, part).start()
        near_copy(2, part).start()
        if part > 0:
            near_copy(3, part - 1).start()
    near_copy(3, CHUNKS - 1).start()
    far_copy(0).start()

    def normed_rows(rel, at):
        square = jnp.zeros((2 * rows, 1), f32)
        for part in range(CHUNKS):
            piece = gath[rel, part].astype(f32)
            square = square + jnp.sum(piece * piece, axis=-1, keepdims=True)
        factor = lax.rsqrt(square / width + 1e-6)
        for part in range(CHUNKS):
            piece = gath[rel, part].astype(f32) * factor * gm_ref[columns(part)].astype(f32)
            m_scr[pl.ds(at, 2 * rows), columns(part)] = piece.astype(bf16)

    def activation(count):
        block = m_scr[pl.ds(0, count)]
        gate = jnp.dot(block, wg[...], preferred_element_type=f32)
        up = jnp.dot(block, wu[...], preferred_element_type=f32)
        return (jax.nn.silu(gate) * up).astype(bf16)

    def contract(act, rels):
        part = jnp.dot(act, wd[...], preferred_element_type=f32)
        for index, rel in enumerate(rels):
            low = part[2 * index * rows:(2 * index + 1) * rows]
            high = part[(2 * index + 1) * rows:(2 * index + 2) * rows]
            s1_send[rel] = jnp.where(is_low, high, low)
            keep[rel] = jnp.where(is_low, low, high)
            pair_copy(rel).start()

    def send_sum(rel):
        pair_copy(rel).wait_recv()
        s2_send[rel] = (keep[rel] + s1_recv[rel]).astype(bf16)
        chip_copy(rel).start()

    for rel in (1, 2):
        for part in range(CHUNKS):
            near_copy(rel, part).wait_recv()
        forward_copy(rel).start()
    for load in loads:
        load.wait()
    forward_arrived(1)
    normed_rows(1, 0)
    forward_arrived(2)
    normed_rows(2, 2 * rows)
    contract(activation(4 * rows), (1, 2))
    for part in range(CHUNKS):
        near_copy(3, part).wait_recv()
    forward_copy(3).start()
    sibling_rows_arrived()
    normed_rows(0, 2 * rows)

    forward_arrived(3)
    normed_rows(3, 0)
    act = activation(4 * rows)
    send_sum(1)
    send_sum(2)
    contract(act, (3, 0))
    send_sum(3)
    pair_copy(0).wait_recv()

    cols = [h_scr[part].astype(f32) for part in range(CHUNKS)]
    total = jnp.concatenate(cols, axis=1) + (keep[0] + s1_recv[0])
    for rel in (1, 2, 3):
        chip_copy(rel).wait_recv()
        total = total + s2_recv[rel].astype(f32)
    out_ref[...] = total.astype(bf16)
    for rel in (1, 2, 3):
        for part in range(CHUNKS):
            near_copy(rel, part).wait_send()
    far_copy(0).wait_send()
    for rel in range(4):
        pair_copy(rel).wait_send()
    for rel in (1, 2, 3):
        forward_copy(rel).wait_send()
        chip_copy(rel).wait_send()


def mlp_call(o_lat, hidden, w_uv, wo_low, gain_mlp, w_o, w_gate, w_up, w_down):
    rows, width = hidden.shape
    cols = w_gate.shape[1]
    bf16, f32 = jnp.bfloat16, jnp.float32
    vmem = pl.BlockSpec(memory_space=pltpu.VMEM)
    hbm = pl.BlockSpec(memory_space=pltpu.HBM)
    dma = pltpu.SemaphoreType.DMA
    part_width = width // CHUNKS
    held = [pltpu.with_memory_space_constraint(x, pltpu.VMEM) for x in (o_lat, hidden, w_uv, wo_low)]
    streamed = [pltpu.with_memory_space_constraint(x, pltpu.HBM) for x in (w_o, w_gate, w_up, w_down)]
    return pl.pallas_call(
        mlp_kernel,
        out_shape=pltpu.VMEM((rows, width), bf16),
        in_specs=[vmem, vmem, vmem, vmem, hbm, hbm, hbm, hbm, hbm],
        out_specs=vmem,
        scratch_shapes=[
            pltpu.VMEM(gain_mlp.shape, bf16),
            pltpu.VMEM((w_o.shape[0], part_width), bf16),
            pltpu.VMEM((width, cols), bf16),
            pltpu.VMEM((width, cols), bf16),
            pltpu.VMEM((cols, width), bf16),
            pltpu.VMEM((rows, w_o.shape[0]), bf16),
            pltpu.VMEM((CHUNKS, rows, part_width), bf16),
            pltpu.VMEM((4, CHUNKS, 2 * rows, part_width), bf16),
            pltpu.VMEM((4 * rows, width), bf16),
            pltpu.VMEM((4, rows, width), f32),
            pltpu.VMEM((4, rows, width), f32),
            pltpu.VMEM((4, rows, width), f32),
            pltpu.VMEM((4, rows, width), bf16),
            pltpu.VMEM((4, rows, width), bf16),
            dma((4,)), dma, dma((4, CHUNKS)), dma((4, CHUNKS)), dma((4,)), dma((4,)), dma((4,)), dma((4,)), dma((4,)), dma((4,)), dma((4,)), dma((4,)),
        ],
        compiler_params=pltpu.CompilerParams(collective_id=0, has_side_effects=True, vmem_limit_bytes=VMEM_LIMIT),
        name="mlp_exchange",
    )(*held, gain_mlp, *streamed)


def solution(mesh):
    row_spec = P(("rep", "g"))
    full_spec = P()
    in_specs = (row_spec, row_spec, row_spec, row_spec, full_spec, full_spec, full_spec, full_spec, full_spec, full_spec, full_spec, full_spec, full_spec, full_spec, full_spec, P(None, "g"), P(None, "g"), P("g", None))

    def local_step(hidden, cache_lat, cache_rope, seq_lens, gain_attn, w_dq, gain_q, w_uq, w_qr, w_dkv, gain_kv, w_uk, w_uv, w_o, gain_mlp, w_gate, w_up, w_down):
        new_lat, new_rope, o_lat, hid_rows, uv_held, wo_held = attn_call(hidden, cache_lat, cache_rope, seq_lens, gain_attn, w_dq, gain_q, w_uq, w_qr, w_dkv, gain_kv, w_uk, w_uv, w_o)
        out_hidden = mlp_call(o_lat, hid_rows, uv_held, wo_held, gain_mlp, w_o, w_gate, w_up, w_down)
        return out_hidden, new_lat, new_rope

    return jax.shard_map(local_step, mesh=mesh, in_specs=in_specs, out_specs=(row_spec, row_spec, row_spec), check_vma=False)
```

```python
import functools

import jax
import jax.numpy as jnp
from jax import lax
from jax.experimental import pallas as pl
from jax.experimental.pallas import tpu as pltpu
from jax.sharding import PartitionSpec as P


HEADS = 20
HEAD_PAD = 24
RING = 20
GROUP = 4
SPANS = (384, 512, 640, 768, 896, 1024)
VMEM_LIMIT = 39 * 1024 * 1024
WO_PARTS = 16
WO_STEP = 3


def attn_kernel(lens_hbm, hid_hbm, ga_hbm, gq_hbm, gkv_hbm, lat_hbm, rope_hbm, wdq_hbm, wdkv_hbm, wqr_hbm, wuq_hbm, wuk_hbm, wuv_hbm, wo_hbm,
                newlat_hbm, newrope_hbm, o_scr, hid_ref, wuv, wo,
                wdq, wdkv, wuk, lat_buf, rope_buf, q_scr, qr_scr, nl_scr, nr_scr, s_scr,
                ga_ref, gq_ref, gkv_ref, newlat_ref, newrope_ref, lens_ref, order, fill, w_sems, o_sems, in_sems, new_sems, lat_sems, rope_sems):
    rows = hid_ref.shape[0]
    kv_dim = lat_buf.shape[2]
    rope_dim = rope_buf.shape[1]
    cache_len = lat_buf.shape[1]
    nope_dim = wuk.shape[1]
    q_dim = wdq.shape[1]
    half = rope_dim // 2
    groups = rows // GROUP
    f32, bf16 = jnp.float32, jnp.bfloat16
    nt = (((1,), (1,)), ((), ()))

    wqr = wo.at[pl.ds(HEADS * nope_dim, HEADS * rope_dim), pl.ds(0, q_dim)]
    cut = 8 * nope_dim
    uq_low = wo.at[pl.ds(0, cut), pl.ds(0, q_dim)]
    uq_high = wo.at[pl.ds(cut, HEADS * nope_dim - cut), pl.ds(0, q_dim)]
    pairs = ((wdq_hbm, wdq), (wdkv_hbm, wdkv), (wqr_hbm, wqr), (wuq_hbm.at[pl.ds(0, cut)], uq_low), (wuq_hbm.at[pl.ds(cut, HEADS * nope_dim - cut)], uq_high), (wuk_hbm, wuk))
    early = [pltpu.make_async_copy(src, dst, w_sems.at[k]) for k, (src, dst) in enumerate(pairs)]
    small = [pltpu.make_async_copy(src, dst, in_sems.at[k]) for k, (src, dst) in enumerate(((lens_hbm, lens_ref), (hid_hbm, hid_ref), (ga_hbm, ga_ref), (gq_hbm, gq_ref), (gkv_hbm, gkv_ref)))]
    for copy in small + early[:2]:
        copy.start()
    small[0].wait()

    def bucket(row):
        return 8 - ((lens_ref[row] + 127) >> 7)

    for k in range(9):
        fill[k] = 0

    def count(row, _):
        k = bucket(row)
        fill[k] = fill[k] + 1
        return 0

    lax.fori_loop(0, rows, count, 0)
    running = jnp.int32(0)
    for k in range(9):
        size = fill[k]
        fill[k] = running
        running = running + size

    def place(row, _):
        k = bucket(row)
        order[fill[k]] = row
        fill[k] = fill[k] + 1
        return 0

    lax.fori_loop(0, rows, place, 0)

    def lat_copy(place_id, slot):
        row = order[place_id]
        span = jnp.maximum((lens_ref[order[(place_id // GROUP) * GROUP]] + 127) >> 7, SPANS[0] // 128) << 7
        count = jnp.where(place_id < RING, span, ((lens_ref[row] + 15) >> 4) << 4)
        count = pl.multiple_of(count, 16)
        return pltpu.make_async_copy(lat_hbm.at[row, pl.ds(0, count)], lat_buf.at[slot, pl.ds(0, count)], lat_sems.at[slot])

    def rope_copy(row, slot):
        return pltpu.make_async_copy(rope_hbm.at[row], rope_buf.at[slot], rope_sems.at[slot])

    def start_place(place_id, slot):
        lat_copy(place_id, slot).start()
        rope_copy(order[place_id], slot).start()

    wo_rows = wo.shape[0] // WO_PARTS

    def wo_copy(part):
        span = pl.ds(pl.multiple_of(part * wo_rows, 32), wo_rows)
        return pltpu.make_async_copy(wo_hbm.at[span, pl.ds(0, wo.shape[1])], wo.at[span], o_sems.at[1])

    def start_group(group):
        for sub in range(GROUP):
            start_place(group * GROUP + sub, lax.rem(group * GROUP, RING) + sub)

    uv_copy = pltpu.make_async_copy(wuv_hbm, wuv, o_sems.at[0])

    def norm(values, gain_ref):
        mean_sq = jnp.mean(values * values, axis=-1, keepdims=True)
        return values * lax.rsqrt(mean_sq + 1e-6) * gain_ref[...].astype(f32)

    row_id = lax.broadcasted_iota(jnp.int32, (rows, 128), 0)
    position = jnp.zeros((rows, 128), jnp.int32)
    for row in range(rows):
        position = jnp.where(row_id == row, lens_ref[row], position)
    lane = lax.broadcasted_iota(jnp.int32, (rows, 128), 1)
    freq_id = lane & (half - 1)
    inv_freq = jnp.exp(freq_id.astype(f32) * (-jnp.log(jnp.float32(10000.0)) / half))
    angle = position.astype(f32) * inv_freq
    first_half = (lane & half) == 0
    cos_part = jnp.cos(angle)
    sin_part = jnp.where(first_half, -jnp.sin(angle), jnp.sin(angle))

    def rotate(values):
        swapped = jnp.where(first_half, pltpu.roll(values, 128 - half, 1), pltpu.roll(values, half, 1))
        return values * cos_part + swapped * sin_part

    small[1].wait()
    small[2].wait()
    hidden = hid_ref[...].astype(f32)
    normed = norm(hidden, ga_ref).astype(bf16)
    q_scr[...] = jnp.zeros_like(q_scr)
    qr_scr[...] = jnp.zeros_like(qr_scr)

    small[3].wait()
    small[4].wait()
    early[0].wait()
    early[2].start()
    early[3].start()
    q_raw = jnp.dot(normed, wdq[...], preferred_element_type=f32)
    early[1].wait()
    early[4].start()
    kv_raw = lax.dot_general(normed, wdkv[...], nt, preferred_element_type=f32)
    q_in = norm(q_raw, gq_ref).astype(bf16)
    early[2].wait()
    early[5].start()
    rope_raw = lax.dot_general(q_in, wo[pl.ds(HEADS * nope_dim, HEADS * rope_dim), pl.ds(0, q_dim)], nt, preferred_element_type=f32)
    new_lat = norm(kv_raw[:, :kv_dim], gkv_ref).astype(bf16)
    newlat_ref[...] = new_lat
    nl_scr[...] = new_lat.astype(f32)
    kv_rope = jnp.concatenate([kv_raw[:, kv_dim:], jnp.zeros((rows, 128 - rope_dim), f32)], axis=1)
    new_rope = rotate(kv_rope).astype(bf16)
    newrope_ref[...] = new_rope[:, :rope_dim]
    outgoing = [pltpu.make_async_copy(newlat_ref, newlat_hbm, new_sems.at[0]), pltpu.make_async_copy(newrope_ref, newrope_hbm, new_sems.at[1])]
    nr_scr[...] = jnp.where(lane < rope_dim, new_rope.astype(f32), 0.0)

    def nope_quad(quad):
        return lax.dot_general(q_in, wo[pl.ds(quad * 4 * nope_dim, 4 * nope_dim), pl.ds(0, q_dim)], nt, preferred_element_type=f32)

    def absorb_quad(quad, q_nope):
        for sub in range(4):
            head = quad * 4 + sub
            one = q_nope[:, sub * nope_dim:(sub + 1) * nope_dim].astype(bf16)
            q_abs = jnp.dot(one, wuk[head], preferred_element_type=f32).astype(bf16).astype(f32)
            for col in range(kv_dim // 128):
                q_scr[col, pl.ds(head, rows, stride=HEAD_PAD), :] = q_abs[:, col * 128:(col + 1) * 128]

    early[3].wait()
    start_group(0)
    quads = HEADS // 4
    ahead = nope_quad(0)
    for pair in range(HEADS // 2):
        turned = rotate(rope_raw[:, pair * 128:(pair + 1) * 128]).astype(bf16).astype(f32)
        qr_scr[pl.ds(2 * pair, rows, stride=HEAD_PAD), :] = turned
        qr_scr[pl.ds(2 * pair + 1, rows, stride=HEAD_PAD), :] = pltpu.roll(turned, rope_dim, 1)
    ahead2 = nope_quad(1)
    early[4].wait()
    start_group(1)
    pending_quads = [ahead, ahead2, nope_quad(2)]
    early[5].wait()
    start_group(2)
    for quad in range(quads):
        absorb_quad(quad, pending_quads[quad])
        if quad + 3 < quads:
            pending_quads.append(nope_quad(quad + 3))

    for copy in outgoing:
        copy.start()
    scale = (nope_dim + rope_dim) ** -0.5

    def head_rows(row):
        return pl.ds(pl.multiple_of(row * HEAD_PAD, 8), HEAD_PAD)

    def query(row):
        return jnp.concatenate([q_scr[col, head_rows(row), :] for col in range(kv_dim // 128)], axis=1)

    def score_part(row, slot, span):
        lat = lat_buf[slot, pl.ds(0, span)]
        score = lax.dot_general(query(row).astype(bf16), lat, nt, preferred_element_type=f32)
        q_rope = qr_scr[head_rows(row), :][:, :rope_dim].astype(bf16)
        return score + jnp.dot(q_rope, rope_buf[slot, :, pl.ds(0, span)], preferred_element_type=f32)

    def soft_part(row, score):
        key_pos = lax.broadcasted_iota(jnp.int32, score.shape, 1)
        score = jnp.where(key_pos < lens_ref[row], score * scale, -jnp.inf)
        q_rope = qr_scr[head_rows(row), :]
        own = jnp.sum(query(row) * nl_scr[pl.ds(row, 1), :], axis=-1, keepdims=True) + jnp.sum(q_rope * nr_scr[pl.ds(row, 1), :], axis=-1, keepdims=True)
        own = own * scale
        top = jnp.maximum(jnp.max(score, axis=-1, keepdims=True), own)
        weight = jnp.exp(score - top)
        own_weight = jnp.exp(own - top)
        total = jnp.sum(weight, axis=-1, keepdims=True) + own_weight
        return (weight / total).astype(bf16), (own_weight / total).astype(bf16).astype(f32)

    def mix_part(row, slot, prob, own_prob, span):
        mixed = jnp.dot(prob, lat_buf[slot, pl.ds(0, span)], preferred_element_type=f32) + own_prob * nl_scr[pl.ds(row, 1), :]
        mixed = mixed.astype(bf16).astype(f32)
        for col in range(kv_dim // 128):
            o_scr[col, head_rows(row), :] = mixed[:, col * 128:(col + 1) * 128]

    def members(group):
        return [(order[group * GROUP + sub], lax.rem(group * GROUP, RING) + sub) for sub in range(GROUP)]

    def wait_members(group):
        for sub, (row, slot) in enumerate(members(group)):
            lat_copy(group * GROUP + sub, slot).wait()
            rope_copy(row, slot).wait()

    def group_blocks(group):
        return (lens_ref[order[group * GROUP]] + 127) >> 7

    def by_span(blocks, run, spans):
        for index, span in enumerate(spans):
            low = spans[index - 1] // 128 if index else 0
            pl.when((blocks > low) & (blocks <= span // 128))(functools.partial(run, span))

    first = members(0)
    wait_members(0)
    start_group(3)

    def first_scores(span):
        for sub, (row, slot) in enumerate(first):
            s_scr[sub, :, pl.ds(0, span)] = score_part(row, slot, span)

    by_span(group_blocks(0), first_scores, (512, 768, 1024))

    def group_step(group, _):
        now = members(group)
        later = members(group + 1)
        wait_members(group + 1)
        pl.when(group + 4 < groups)(lambda: start_group(group + 4))
        pl.when(group == 0)(uv_copy.start)
        for extra in range(WO_STEP):
            part = group * WO_STEP + extra
            pl.when(part < WO_PARTS)(lambda part=part: wo_copy(part).start())

        def run(span):
            pending = None
            for sub in range(GROUP):
                fresh = score_part(*later[sub], span)
                probs = soft_part(now[sub][0], s_scr[sub, :, pl.ds(0, span)])
                s_scr[sub, :, pl.ds(0, span)] = fresh
                if pending is not None:
                    mix_part(*pending, span)
                pending = (*now[sub], *probs)
            mix_part(*pending, span)

        by_span(group_blocks(group), run, SPANS)

        return 0

    lax.fori_loop(0, groups - 1, group_step, 0)
    last = members(groups - 1)

    def last_mix(span):
        pending = None
        for sub in range(GROUP):
            probs = soft_part(last[sub][0], s_scr[sub, :, pl.ds(0, span)])
            if pending is not None:
                mix_part(*pending, span)
            pending = (*last[sub], *probs)
        mix_part(*pending, span)

    by_span(group_blocks(groups - 1), last_mix, SPANS)
    uv_copy.wait()
    pltpu.make_async_copy(wo_hbm.at[:, pl.ds(0, wo.shape[1])], wo, o_sems.at[1]).wait()
    for copy in outgoing:
        copy.wait()


def attn_call(hidden, cache_lat, cache_rope, seq_lens, gain_attn, w_dq, gain_q, w_uq, w_qr, w_dkv, gain_kv, w_uk, w_uv, w_o):
    rows, width = hidden.shape
    cache_len, kv_dim = cache_lat.shape[1:]
    rope_dim = cache_rope.shape[2]
    q_dim, heads, nope_dim = w_uq.shape
    bf16, f32 = jnp.bfloat16, jnp.float32
    vmem = pl.BlockSpec(memory_space=pltpu.VMEM)
    hbm = pl.BlockSpec(memory_space=pltpu.HBM)
    dma = pltpu.SemaphoreType.DMA
    rope_keys = jnp.swapaxes(cache_rope, 1, 2)
    dkv_t = w_dkv.T
    qr_t = jnp.transpose(w_qr, (1, 2, 0)).reshape(heads * rope_dim, q_dim)
    uq_t = jnp.transpose(w_uq, (1, 2, 0)).reshape(heads * nope_dim, q_dim)
    uk_t = jnp.transpose(w_uk, (1, 2, 0))
    uv_t = jnp.swapaxes(w_uv, 0, 1)
    handed = (
        pltpu.VMEM((kv_dim // 128, rows * HEAD_PAD, 128), f32),
        pltpu.VMEM(hidden.shape, bf16),
        pltpu.VMEM(uv_t.shape, bf16),
        pltpu.VMEM((w_o.shape[0], width // 2), bf16),
    )
    return pl.pallas_call(
        attn_kernel,
        out_shape=(jax.ShapeDtypeStruct((rows, kv_dim), bf16), jax.ShapeDtypeStruct((rows, rope_dim), bf16)) + handed,
        in_specs=[hbm] * 14,
        out_specs=(hbm, hbm, vmem, vmem, vmem, vmem),
        scratch_shapes=[
            pltpu.VMEM(w_dq.shape, bf16),
            pltpu.VMEM(dkv_t.shape, bf16),
            pltpu.VMEM(uk_t.shape, bf16),
            pltpu.VMEM((RING, cache_len, kv_dim), bf16),
            pltpu.VMEM((RING, rope_dim, cache_len), bf16),
            pltpu.VMEM((kv_dim // 128, rows * HEAD_PAD, 128), f32),
            pltpu.VMEM((rows * HEAD_PAD, 128), f32),
            pltpu.VMEM((rows, kv_dim), f32),
            pltpu.VMEM((rows, 128), f32),
            pltpu.VMEM((GROUP, HEAD_PAD, cache_len), f32),
            pltpu.VMEM(gain_attn.shape, bf16),
            pltpu.VMEM(gain_q.shape, bf16),
            pltpu.VMEM(gain_kv.shape, bf16),
            pltpu.VMEM((rows, kv_dim), bf16),
            pltpu.VMEM((rows, rope_dim), bf16),
            pltpu.SMEM((rows,), jnp.int32),
            pltpu.SMEM((rows,), jnp.int32),
            pltpu.SMEM((9,), jnp.int32),
            dma((6,)), dma((2,)), dma((5,)), dma((2,)), dma((RING,)), dma((RING,)),
        ],
        compiler_params=pltpu.CompilerParams(vmem_limit_bytes=VMEM_LIMIT),
        name="attention",
    )(seq_lens, hidden, gain_attn, gain_q, gain_kv, cache_lat, rope_keys, w_dq, dkv_t, qr_t, uq_t, uk_t, uv_t, w_o)


MESH = pl.DeviceIdType.MESH
CHUNKS = 4


def mlp_kernel(o_ref, hid_ref, wuv, wo_low, gm_hbm, wo_hbm, wg_hbm, wu_hbm, wd_hbm, out_ref,
               gm_ref, wo_high, wg, wu, wd, heads_scr, h_scr, gath, m_scr, keep, s1_send, s1_recv, s2_send, s2_recv,
               w_sems, wo_sems, near_send, near_recv, far_send, far_recv, fw_send, fw_recv, p1_send, p1_recv, p2_send, p2_recv):
    rows, width = hid_ref.shape
    part_width = width // CHUNKS
    heads, kv_dim, v_dim = wuv.shape
    f32, bf16 = jnp.float32, jnp.bfloat16
    me = lax.axis_index("g")
    core = lax.rem(me, 2)
    chip_x = lax.rem(me // 2, 2)
    chip_y = me // 4
    is_low = core == 0
    sibling = me + 1 - 2 * core
    mine = pl.ds(pl.multiple_of(core * rows, rows), rows)
    theirs = pl.ds(pl.multiple_of((1 - core) * rows, rows), rows)

    def peer(rel):
        return me + (rel % 2) * (2 - 4 * chip_x) + (rel // 2) * (4 - 8 * chip_y)

    def remote(src, dst, send, recv, target):
        return pltpu.make_async_remote_copy(src, dst, send, recv, device_id={"g": target}, device_id_type=MESH)

    def near_copy(rel, part):
        return remote(h_scr.at[part], gath.at[rel, part, mine], near_send.at[rel, part], near_recv.at[rel, part], peer(rel))

    def far_copy(rel):
        return remote(h_scr, gath.at[rel, :, mine], far_send.at[rel], far_recv.at[rel], sibling)

    def sibling_rows_arrived():
        remote(h_scr, gath.at[0, :, theirs], far_send.at[0], far_recv.at[0], sibling).wait_recv()

    def forward_copy(rel):
        return remote(gath.at[rel, :, mine], gath.at[rel, :, mine], fw_send.at[rel], fw_recv.at[rel], sibling)

    def forward_arrived(rel):
        remote(gath.at[rel, :, theirs], gath.at[rel, :, theirs], fw_send.at[rel], fw_recv.at[rel], sibling).wait_recv()

    def pair_copy(rel, half):
        return remote(s1_send.at[rel, half], s1_recv.at[rel, half], p1_send.at[rel, half], p1_recv.at[rel, half], sibling)

    def chip_copy(rel, half):
        return remote(s2_send.at[rel, half], s2_recv.at[rel, half], p2_send.at[rel, half], p2_recv.at[rel, half], peer(rel))

    held_width = wo_low.shape[1]
    late = [pltpu.make_async_copy(wo_hbm.at[:, pl.ds(held_width + k * part_width, part_width)], wo_high.at[k], wo_sems.at[k]) for k in range(2)]
    loads = [pltpu.make_async_copy(src, dst, w_sems.at[k]) for k, (src, dst) in enumerate(((wg_hbm, wg), (wu_hbm, wu), (wd_hbm, wd), (gm_hbm, gm_ref)))]
    late[0].start()
    barrier = pltpu.get_barrier_semaphore()
    for target in (sibling, peer(1), peer(2), peer(3)):
        pl.semaphore_signal(barrier, inc=1, device_id={"g": target}, device_id_type=MESH)

    for head in range(heads):
        cols = [o_ref[col, pl.ds(head, rows, stride=HEAD_PAD), :] for col in range(kv_dim // 128)]
        mixed = jnp.concatenate(cols, axis=1).astype(bf16)
        heads_scr[:, head * v_dim:(head + 1) * v_dim] = jnp.dot(mixed, wuv[head], preferred_element_type=f32).astype(bf16)

    def columns(part):
        return pl.ds(part * part_width, part_width)

    for part in range(CHUNKS):
        if part < 2:
            weights = wo_low[:, columns(part)]
        else:
            late[part - 2].wait()
            weights = wo_high[part - 2]
        attn_out = jnp.dot(heads_scr[...], weights, preferred_element_type=f32)
        resid = (hid_ref[:, columns(part)].astype(f32) + attn_out).astype(bf16)
        h_scr[part] = resid
        gath[0, part, mine] = resid
        if part == 0:
            late[1].start()
            pl.semaphore_wait(barrier, 4)
        if part == 1:
            for load in loads:
                load.start()
        near_copy(1, part).start()
        near_copy(2, part).start()
        if part > 0:
            near_copy(3, part - 1).start()
    near_copy(3, CHUNKS - 1).start()
    far_copy(0).start()

    def normed_rows(rel, at):
        square = jnp.zeros((2 * rows, 1), f32)
        for part in range(CHUNKS):
            piece = gath[rel, part].astype(f32)
            square = square + jnp.sum(piece * piece, axis=-1, keepdims=True)
        factor = lax.rsqrt(square / width + 1e-6)
        for part in range(CHUNKS):
            piece = gath[rel, part].astype(f32) * factor * gm_ref[columns(part)].astype(f32)
            m_scr[pl.ds(at, 2 * rows), columns(part)] = piece.astype(bf16)

    def activation(count):
        block = m_scr[pl.ds(0, count)]
        gate = jnp.dot(block, wg[...], preferred_element_type=f32)
        up = jnp.dot(block, wu[...], preferred_element_type=f32)
        return (jax.nn.silu(gate) * up).astype(bf16)

    half_width = width // 2

    def contract(act, rels):
        for half in range(2):
            part = jnp.dot(act, wd[:, pl.ds(half * half_width, half_width)], preferred_element_type=f32)
            for index, rel in enumerate(rels):
                low = part[2 * index * rows:(2 * index + 1) * rows]
                high = part[(2 * index + 1) * rows:(2 * index + 2) * rows]
                s1_send[rel, half] = jnp.where(is_low, high, low)
                keep[rel, half] = jnp.where(is_low, low, high)
                pair_copy(rel, half).start()

    def send_sum(rel, half):
        pair_copy(rel, half).wait_recv()
        s2_send[rel, half] = (keep[rel, half] + s1_recv[rel, half]).astype(bf16)
        chip_copy(rel, half).start()

    for rel in (1, 2):
        for part in range(CHUNKS):
            near_copy(rel, part).wait_recv()
        forward_copy(rel).start()
    for load in loads:
        load.wait()
    forward_arrived(1)
    normed_rows(1, 0)
    forward_arrived(2)
    normed_rows(2, 2 * rows)
    contract(activation(4 * rows), (1, 2))
    for part in range(CHUNKS):
        near_copy(3, part).wait_recv()
    forward_copy(3).start()
    sibling_rows_arrived()
    normed_rows(0, 2 * rows)

    for half in range(2):
        send_sum(1, half)
        send_sum(2, half)

    forward_arrived(3)
    normed_rows(3, 0)
    contract(activation(4 * rows), (3, 0))
    send_sum(3, 0)
    send_sum(3, 1)
    totals = []
    for half in range(2):
        pair_copy(0, half).wait_recv()
        residual = jnp.concatenate([h_scr[2 * half].astype(f32), h_scr[2 * half + 1].astype(f32)], axis=1)
        totals.append(residual + (keep[0, half] + s1_recv[0, half]))
    for rel in (1, 2, 3):
        for half in range(2):
            chip_copy(rel, half).wait_recv()
            totals[half] = totals[half] + s2_recv[rel, half].astype(f32)
    for half in range(2):
        out_ref[:, half * half_width:(half + 1) * half_width] = totals[half].astype(bf16)
    for rel in (1, 2, 3):
        for part in range(CHUNKS):
            near_copy(rel, part).wait_send()
    far_copy(0).wait_send()
    for half in range(2):
        for rel in range(4):
            pair_copy(rel, half).wait_send()
        for rel in (1, 2, 3):
            chip_copy(rel, half).wait_send()
    for rel in (1, 2, 3):
        forward_copy(rel).wait_send()


def mlp_call(o_lat, hidden, w_uv, wo_low, gain_mlp, w_o, w_gate, w_up, w_down):
    rows, width = hidden.shape
    cols = w_gate.shape[1]
    bf16, f32 = jnp.bfloat16, jnp.float32
    vmem = pl.BlockSpec(memory_space=pltpu.VMEM)
    hbm = pl.BlockSpec(memory_space=pltpu.HBM)
    dma = pltpu.SemaphoreType.DMA
    part_width = width // CHUNKS
    held = [pltpu.with_memory_space_constraint(x, pltpu.VMEM) for x in (o_lat, hidden, w_uv, wo_low)]
    streamed = [pltpu.with_memory_space_constraint(x, pltpu.HBM) for x in (w_o, w_gate, w_up, w_down)]
    return pl.pallas_call(
        mlp_kernel,
        out_shape=pltpu.VMEM((rows, width), bf16),
        in_specs=[vmem, vmem, vmem, vmem, hbm, hbm, hbm, hbm, hbm],
        out_specs=vmem,
        scratch_shapes=[
            pltpu.VMEM(gain_mlp.shape, bf16),
            pltpu.VMEM((2, w_o.shape[0], part_width), bf16),
            pltpu.VMEM((width, cols), bf16),
            pltpu.VMEM((width, cols), bf16),
            pltpu.VMEM((cols, width), bf16),
            pltpu.VMEM((rows, w_o.shape[0]), bf16),
            pltpu.VMEM((CHUNKS, rows, part_width), bf16),
            pltpu.VMEM((4, CHUNKS, 2 * rows, part_width), bf16),
            pltpu.VMEM((4 * rows, width), bf16),
            pltpu.VMEM((4, 2, rows, width // 2), f32),
            pltpu.VMEM((4, 2, rows, width // 2), f32),
            pltpu.VMEM((4, 2, rows, width // 2), f32),
            pltpu.VMEM((4, 2, rows, width // 2), bf16),
            pltpu.VMEM((4, 2, rows, width // 2), bf16),
            dma((4,)), dma((2,)), dma((4, CHUNKS)), dma((4, CHUNKS)), dma((4,)), dma((4,)), dma((4,)), dma((4,)), dma((4, 2)), dma((4, 2)), dma((4, 2)), dma((4, 2)),
        ],
        compiler_params=pltpu.CompilerParams(collective_id=0, has_side_effects=True, vmem_limit_bytes=VMEM_LIMIT),
        name="mlp_exchange",
    )(*held, gain_mlp, *streamed)


def solution(mesh):
    row_spec = P(("rep", "g"))
    full_spec = P()
    in_specs = (row_spec, row_spec, row_spec, row_spec, full_spec, full_spec, full_spec, full_spec, full_spec, full_spec, full_spec, full_spec, full_spec, full_spec, full_spec, P(None, "g"), P(None, "g"), P("g", None))

    def local_step(hidden, cache_lat, cache_rope, seq_lens, gain_attn, w_dq, gain_q, w_uq, w_qr, w_dkv, gain_kv, w_uk, w_uv, w_o, gain_mlp, w_gate, w_up, w_down):
        new_lat, new_rope, o_lat, hid_rows, uv_held, wo_held = attn_call(hidden, cache_lat, cache_rope, seq_lens, gain_attn, w_dq, gain_q, w_uq, w_qr, w_dkv, gain_kv, w_uk, w_uv, w_o)
        out_hidden = mlp_call(o_lat, hid_rows, uv_held, wo_held, gain_mlp, w_o, w_gate, w_up, w_down)
        return out_hidden, new_lat, new_rope

    return jax.shard_map(local_step, mesh=mesh, in_specs=in_specs, out_specs=(row_spec, row_spec, row_spec), check_vma=False)
```

```python
import functools

import jax
import jax.numpy as jnp
from jax import lax
from jax.experimental import pallas as pl
from jax.experimental.pallas import tpu as pltpu
from jax.sharding import PartitionSpec as P


HEADS = 20
HEAD_PAD = 24
RING = 20
GROUP = 4
SPANS = (384, 512, 640, 768, 896, 1024)
VMEM_LIMIT = 39 * 1024 * 1024
WO_PARTS = 16
WO_STEP = 3


def attn_kernel(lens_hbm, hid_hbm, ga_hbm, gq_hbm, gkv_hbm, lat_hbm, rope_hbm, wdq_hbm, wdkv_hbm, wqr_hbm, wuq_hbm, wuk_hbm, wuv_hbm, wo_hbm,
                newlat_hbm, newrope_hbm, o_scr, hid_ref, wuv, wo,
                wdq, wdkv, wuk, lat_buf, rope_buf, q_scr, qr_scr, nl_scr, nr_scr, s_scr,
                ga_ref, gq_ref, gkv_ref, newlat_ref, newrope_ref, lens_ref, order, fill, w_sems, o_sems, in_sems, new_sems, lat_sems, rope_sems):
    rows = hid_ref.shape[0]
    kv_dim = lat_buf.shape[2]
    rope_dim = rope_buf.shape[1]
    cache_len = lat_buf.shape[1]
    nope_dim = wuk.shape[1]
    q_dim = wdq.shape[1]
    half = rope_dim // 2
    groups = rows // GROUP
    f32, bf16 = jnp.float32, jnp.bfloat16
    nt = (((1,), (1,)), ((), ()))

    wqr = wo.at[pl.ds(HEADS * nope_dim, HEADS * rope_dim), pl.ds(0, q_dim)]
    cut = 8 * nope_dim
    uq_low = wo.at[pl.ds(0, cut), pl.ds(0, q_dim)]
    uq_high = wo.at[pl.ds(cut, HEADS * nope_dim - cut), pl.ds(0, q_dim)]
    pairs = ((wdq_hbm, wdq), (wdkv_hbm, wdkv), (wqr_hbm, wqr), (wuq_hbm.at[pl.ds(0, cut)], uq_low), (wuq_hbm.at[pl.ds(cut, HEADS * nope_dim - cut)], uq_high), (wuk_hbm, wuk))
    early = [pltpu.make_async_copy(src, dst, w_sems.at[k]) for k, (src, dst) in enumerate(pairs)]
    small = [pltpu.make_async_copy(src, dst, in_sems.at[k]) for k, (src, dst) in enumerate(((lens_hbm, lens_ref), (hid_hbm, hid_ref), (ga_hbm, ga_ref), (gq_hbm, gq_ref), (gkv_hbm, gkv_ref)))]
    for copy in small + early[:2]:
        copy.start()
    small[0].wait()

    def bucket(row):
        return 8 - ((lens_ref[row] + 127) >> 7)

    for k in range(9):
        fill[k] = 0

    def count(row, _):
        k = bucket(row)
        fill[k] = fill[k] + 1
        return 0

    lax.fori_loop(0, rows, count, 0)
    running = jnp.int32(0)
    for k in range(9):
        size = fill[k]
        fill[k] = running
        running = running + size

    def place(row, _):
        k = bucket(row)
        order[fill[k]] = row
        fill[k] = fill[k] + 1
        return 0

    lax.fori_loop(0, rows, place, 0)

    def group_blocks(group):
        return (lens_ref[order[group * GROUP]] + 127) >> 7

    def group_copies(group):
        count = pl.multiple_of(jnp.maximum(group_blocks(group), SPANS[0] // 128) << 7, 128)
        base = lax.rem(group * GROUP, RING)
        copies = []
        for sub in range(GROUP):
            row, slot = order[group * GROUP + sub], base + sub
            copies.append(pltpu.make_async_copy(lat_hbm.at[row, pl.ds(0, count)], lat_buf.at[slot, pl.ds(0, count)], lat_sems.at[slot]))
            copies.append(pltpu.make_async_copy(rope_hbm.at[row], rope_buf.at[slot], rope_sems.at[slot]))
        return copies

    def start_group(group):
        for copy in group_copies(group):
            copy.start()

    wo_rows = wo.shape[0] // WO_PARTS

    def wo_copy(part):
        span = pl.ds(pl.multiple_of(part * wo_rows, 32), wo_rows)
        return pltpu.make_async_copy(wo_hbm.at[span, pl.ds(0, wo.shape[1])], wo.at[span], o_sems.at[1])

    uv_copy = pltpu.make_async_copy(wuv_hbm, wuv, o_sems.at[0])

    def norm(values, gain_ref):
        mean_sq = jnp.mean(values * values, axis=-1, keepdims=True)
        return values * lax.rsqrt(mean_sq + 1e-6) * gain_ref[...].astype(f32)

    row_id = lax.broadcasted_iota(jnp.int32, (rows, 128), 0)
    position = jnp.zeros((rows, 128), jnp.int32)
    for row in range(rows):
        position = jnp.where(row_id == row, lens_ref[row], position)
    lane = lax.broadcasted_iota(jnp.int32, (rows, 128), 1)
    freq_id = lane & (half - 1)
    inv_freq = jnp.exp(freq_id.astype(f32) * (-jnp.log(jnp.float32(10000.0)) / half))
    angle = position.astype(f32) * inv_freq
    first_half = (lane & half) == 0
    cos_part = jnp.cos(angle)
    sin_part = jnp.where(first_half, -jnp.sin(angle), jnp.sin(angle))

    def rotate(values):
        swapped = jnp.where(first_half, pltpu.roll(values, 128 - half, 1), pltpu.roll(values, half, 1))
        return values * cos_part + swapped * sin_part

    small[1].wait()
    small[2].wait()
    hidden = hid_ref[...].astype(f32)
    normed = norm(hidden, ga_ref).astype(bf16)
    q_scr[...] = jnp.zeros_like(q_scr)
    qr_scr[...] = jnp.zeros_like(qr_scr)

    small[3].wait()
    small[4].wait()
    early[2].start()
    early[3].start()
    early[0].wait()
    early[4].start()
    early[5].start()
    q_raw = jnp.dot(normed, wdq[...], preferred_element_type=f32)
    early[1].wait()
    start_group(0)
    kv_raw = lax.dot_general(normed, wdkv[...], nt, preferred_element_type=f32)
    q_in = norm(q_raw, gq_ref).astype(bf16)
    early[2].wait()
    rope_raw = lax.dot_general(q_in, wo[pl.ds(HEADS * nope_dim, HEADS * rope_dim), pl.ds(0, q_dim)], nt, preferred_element_type=f32)
    new_lat = norm(kv_raw[:, :kv_dim], gkv_ref).astype(bf16)
    newlat_ref[...] = new_lat
    nl_scr[...] = new_lat.astype(f32)
    kv_rope = jnp.concatenate([kv_raw[:, kv_dim:], jnp.zeros((rows, 128 - rope_dim), f32)], axis=1)
    new_rope = rotate(kv_rope).astype(bf16)
    newrope_ref[...] = new_rope[:, :rope_dim]
    outgoing = [pltpu.make_async_copy(newlat_ref, newlat_hbm, new_sems.at[0]), pltpu.make_async_copy(newrope_ref, newrope_hbm, new_sems.at[1])]
    nr_scr[...] = jnp.where(lane < rope_dim, new_rope.astype(f32), 0.0)

    def nope_quad(quad):
        return lax.dot_general(q_in, wo[pl.ds(quad * 4 * nope_dim, 4 * nope_dim), pl.ds(0, q_dim)], nt, preferred_element_type=f32)

    def absorb_quad(quad, q_nope):
        for sub in range(4):
            head = quad * 4 + sub
            one = q_nope[:, sub * nope_dim:(sub + 1) * nope_dim].astype(bf16)
            q_abs = jnp.dot(one, wuk[head], preferred_element_type=f32).astype(bf16).astype(f32)
            for col in range(kv_dim // 128):
                q_scr[col, pl.ds(head, rows, stride=HEAD_PAD), :] = q_abs[:, col * 128:(col + 1) * 128]

    early[3].wait()
    start_group(1)
    quads = HEADS // 4
    ahead = nope_quad(0)
    for pair in range(HEADS // 2):
        turned = rotate(rope_raw[:, pair * 128:(pair + 1) * 128]).astype(bf16).astype(f32)
        qr_scr[pl.ds(2 * pair, rows, stride=HEAD_PAD), :] = turned
        qr_scr[pl.ds(2 * pair + 1, rows, stride=HEAD_PAD), :] = pltpu.roll(turned, rope_dim, 1)
    ahead2 = nope_quad(1)
    early[4].wait()
    start_group(2)
    pending_quads = [ahead, ahead2, nope_quad(2)]
    early[5].wait()
    for quad in range(quads):
        absorb_quad(quad, pending_quads[quad])
        if quad + 3 < quads:
            pending_quads.append(nope_quad(quad + 3))

    for copy in outgoing:
        copy.start()
    scale = (nope_dim + rope_dim) ** -0.5

    def head_rows(row):
        return pl.ds(pl.multiple_of(row * HEAD_PAD, 8), HEAD_PAD)

    def query(row):
        return jnp.concatenate([q_scr[col, head_rows(row), :] for col in range(kv_dim // 128)], axis=1)

    def score_part(row, slot, span):
        lat = lat_buf[slot, pl.ds(0, span)]
        score = lax.dot_general(query(row).astype(bf16), lat, nt, preferred_element_type=f32)
        q_rope = qr_scr[head_rows(row), :][:, :rope_dim].astype(bf16)
        return score + jnp.dot(q_rope, rope_buf[slot, :, pl.ds(0, span)], preferred_element_type=f32)

    def soft_part(row, score):
        key_pos = lax.broadcasted_iota(jnp.int32, score.shape, 1)
        score = jnp.where(key_pos < lens_ref[row], score * scale, -jnp.inf)
        q_rope = qr_scr[head_rows(row), :]
        own = jnp.sum(query(row) * nl_scr[pl.ds(row, 1), :], axis=-1, keepdims=True) + jnp.sum(q_rope * nr_scr[pl.ds(row, 1), :], axis=-1, keepdims=True)
        own = own * scale
        top = jnp.maximum(jnp.max(score, axis=-1, keepdims=True), own)
        weight = jnp.exp(score - top)
        own_weight = jnp.exp(own - top)
        total = jnp.sum(weight, axis=-1, keepdims=True) + own_weight
        return (weight / total).astype(bf16), (own_weight / total).astype(bf16).astype(f32)

    def mix_part(row, slot, prob, own_prob, span):
        mixed = jnp.dot(prob, lat_buf[slot, pl.ds(0, span)], preferred_element_type=f32) + own_prob * nl_scr[pl.ds(row, 1), :]
        mixed = mixed.astype(bf16).astype(f32)
        for col in range(kv_dim // 128):
            o_scr[col, head_rows(row), :] = mixed[:, col * 128:(col + 1) * 128]

    def members(group):
        return [(order[group * GROUP + sub], lax.rem(group * GROUP, RING) + sub) for sub in range(GROUP)]

    def wait_members(group):
        for copy in group_copies(group):
            copy.wait()

    def by_span(blocks, run, spans):
        for index, span in enumerate(spans):
            low = spans[index - 1] // 128 if index else 0
            pl.when((blocks > low) & (blocks <= span // 128))(functools.partial(run, span))

    first = members(0)
    wait_members(0)
    start_group(3)

    def first_scores(span):
        for sub, (row, slot) in enumerate(first):
            s_scr[sub, :, pl.ds(0, span)] = score_part(row, slot, span)

    by_span(group_blocks(0), first_scores, (512, 768, 1024))

    def group_step(group, _):
        now = members(group)
        later = members(group + 1)
        wait_members(group + 1)
        pl.when(group + 4 < groups)(lambda: start_group(group + 4))
        pl.when(group == 0)(uv_copy.start)
        for extra in range(WO_STEP):
            part = group * WO_STEP + extra
            pl.when(part < WO_PARTS)(lambda part=part: wo_copy(part).start())

        def run(span):
            pending = None
            for sub in range(GROUP):
                fresh = score_part(*later[sub], span)
                probs = soft_part(now[sub][0], s_scr[sub, :, pl.ds(0, span)])
                s_scr[sub, :, pl.ds(0, span)] = fresh
                if pending is not None:
                    mix_part(*pending, span)
                pending = (*now[sub], *probs)
            mix_part(*pending, span)

        by_span(group_blocks(group), run, SPANS)

        return 0

    lax.fori_loop(0, groups - 1, group_step, 0)
    last = members(groups - 1)

    def last_mix(span):
        pending = None
        for sub in range(GROUP):
            probs = soft_part(last[sub][0], s_scr[sub, :, pl.ds(0, span)])
            if pending is not None:
                mix_part(*pending, span)
            pending = (*last[sub], *probs)
        mix_part(*pending, span)

    by_span(group_blocks(groups - 1), last_mix, SPANS)
    uv_copy.wait()
    pltpu.make_async_copy(wo_hbm.at[:, pl.ds(0, wo.shape[1])], wo, o_sems.at[1]).wait()
    for copy in outgoing:
        copy.wait()


def attn_call(hidden, cache_lat, cache_rope, seq_lens, gain_attn, w_dq, gain_q, w_uq, w_qr, w_dkv, gain_kv, w_uk, w_uv, w_o):
    rows, width = hidden.shape
    cache_len, kv_dim = cache_lat.shape[1:]
    rope_dim = cache_rope.shape[2]
    q_dim, heads, nope_dim = w_uq.shape
    bf16, f32 = jnp.bfloat16, jnp.float32
    vmem = pl.BlockSpec(memory_space=pltpu.VMEM)
    hbm = pl.BlockSpec(memory_space=pltpu.HBM)
    dma = pltpu.SemaphoreType.DMA
    rope_keys = jnp.swapaxes(cache_rope, 1, 2)
    dkv_t = w_dkv.T
    qr_t = jnp.transpose(w_qr, (1, 2, 0)).reshape(heads * rope_dim, q_dim)
    uq_t = jnp.transpose(w_uq, (1, 2, 0)).reshape(heads * nope_dim, q_dim)
    uk_t = jnp.transpose(w_uk, (1, 2, 0))
    uv_t = jnp.swapaxes(w_uv, 0, 1)
    handed = (
        pltpu.VMEM((kv_dim // 128, rows * HEAD_PAD, 128), f32),
        pltpu.VMEM(hidden.shape, bf16),
        pltpu.VMEM(uv_t.shape, bf16),
        pltpu.VMEM((w_o.shape[0], width // 2), bf16),
    )
    return pl.pallas_call(
        attn_kernel,
        out_shape=(jax.ShapeDtypeStruct((rows, kv_dim), bf16), jax.ShapeDtypeStruct((rows, rope_dim), bf16)) + handed,
        in_specs=[hbm] * 14,
        out_specs=(hbm, hbm, vmem, vmem, vmem, vmem),
        scratch_shapes=[
            pltpu.VMEM(w_dq.shape, bf16),
            pltpu.VMEM(dkv_t.shape, bf16),
            pltpu.VMEM(uk_t.shape, bf16),
            pltpu.VMEM((RING, cache_len, kv_dim), bf16),
            pltpu.VMEM((RING, rope_dim, cache_len), bf16),
            pltpu.VMEM((kv_dim // 128, rows * HEAD_PAD, 128), f32),
            pltpu.VMEM((rows * HEAD_PAD, 128), f32),
            pltpu.VMEM((rows, kv_dim), f32),
            pltpu.VMEM((rows, 128), f32),
            pltpu.VMEM((GROUP, HEAD_PAD, cache_len), f32),
            pltpu.VMEM(gain_attn.shape, bf16),
            pltpu.VMEM(gain_q.shape, bf16),
            pltpu.VMEM(gain_kv.shape, bf16),
            pltpu.VMEM((rows, kv_dim), bf16),
            pltpu.VMEM((rows, rope_dim), bf16),
            pltpu.SMEM((rows,), jnp.int32),
            pltpu.SMEM((rows,), jnp.int32),
            pltpu.SMEM((9,), jnp.int32),
            dma((6,)), dma((2,)), dma((5,)), dma((2,)), dma((RING,)), dma((RING,)),
        ],
        compiler_params=pltpu.CompilerParams(vmem_limit_bytes=VMEM_LIMIT),
        name="attention",
    )(seq_lens, hidden, gain_attn, gain_q, gain_kv, cache_lat, rope_keys, w_dq, dkv_t, qr_t, uq_t, uk_t, uv_t, w_o)


MESH = pl.DeviceIdType.MESH
CHUNKS = 4


def mlp_kernel(o_ref, hid_ref, wuv, wo_low, gm_hbm, wo_hbm, wg_hbm, wu_hbm, wd_hbm, out_ref,
               gm_ref, wo_high, wg, wu, wd, heads_scr, h_scr, gath, m_scr, keep, s1_send, s1_recv, s2_send, s2_recv,
               w_sems, wo_sems, near_send, near_recv, far_send, far_recv, fw_send, fw_recv, p1_send, p1_recv, p2_send, p2_recv):
    rows, width = hid_ref.shape
    part_width = width // CHUNKS
    heads, kv_dim, v_dim = wuv.shape
    f32, bf16 = jnp.float32, jnp.bfloat16
    me = lax.axis_index("g")
    core = lax.rem(me, 2)
    chip_x = lax.rem(me // 2, 2)
    chip_y = me // 4
    is_low = core == 0
    sibling = me + 1 - 2 * core
    mine = pl.ds(pl.multiple_of(core * rows, rows), rows)
    theirs = pl.ds(pl.multiple_of((1 - core) * rows, rows), rows)

    def peer(rel):
        return me + (rel % 2) * (2 - 4 * chip_x) + (rel // 2) * (4 - 8 * chip_y)

    def remote(src, dst, send, recv, target):
        return pltpu.make_async_remote_copy(src, dst, send, recv, device_id={"g": target}, device_id_type=MESH)

    def near_copy(rel, part):
        return remote(h_scr.at[part], gath.at[rel, part, mine], near_send.at[rel, part], near_recv.at[rel, part], peer(rel))

    def far_copy(rel):
        return remote(h_scr, gath.at[rel, :, mine], far_send.at[rel], far_recv.at[rel], sibling)

    def sibling_rows_arrived():
        remote(h_scr, gath.at[0, :, theirs], far_send.at[0], far_recv.at[0], sibling).wait_recv()

    def forward_copy(rel):
        return remote(gath.at[rel, :, mine], gath.at[rel, :, mine], fw_send.at[rel], fw_recv.at[rel], sibling)

    def forward_arrived(rel):
        remote(gath.at[rel, :, theirs], gath.at[rel, :, theirs], fw_send.at[rel], fw_recv.at[rel], sibling).wait_recv()

    def pair_copy(rel, half):
        return remote(s1_send.at[rel, half], s1_recv.at[rel, half], p1_send.at[rel, half], p1_recv.at[rel, half], sibling)

    def chip_copy(rel, half):
        return remote(s2_send.at[rel, half], s2_recv.at[rel, half], p2_send.at[rel, half], p2_recv.at[rel, half], peer(rel))

    held_width = wo_low.shape[1]
    late = [pltpu.make_async_copy(wo_hbm.at[:, pl.ds(held_width + k * part_width, part_width)], wo_high.at[k], wo_sems.at[k]) for k in range(2)]
    loads = [pltpu.make_async_copy(src, dst, w_sems.at[k]) for k, (src, dst) in enumerate(((wg_hbm, wg), (wu_hbm, wu), (wd_hbm, wd), (gm_hbm, gm_ref)))]
    late[0].start()
    barrier = pltpu.get_barrier_semaphore()
    for target in (sibling, peer(1), peer(2), peer(3)):
        pl.semaphore_signal(barrier, inc=1, device_id={"g": target}, device_id_type=MESH)

    for head in range(heads):
        cols = [o_ref[col, pl.ds(head, rows, stride=HEAD_PAD), :] for col in range(kv_dim // 128)]
        mixed = jnp.concatenate(cols, axis=1).astype(bf16)
        heads_scr[:, head * v_dim:(head + 1) * v_dim] = jnp.dot(mixed, wuv[head], preferred_element_type=f32).astype(bf16)

    def columns(part):
        return pl.ds(part * part_width, part_width)

    for part in range(CHUNKS):
        if part < 2:
            weights = wo_low[:, columns(part)]
        else:
            late[part - 2].wait()
            weights = wo_high[part - 2]
        attn_out = jnp.dot(heads_scr[...], weights, preferred_element_type=f32)
        resid = (hid_ref[:, columns(part)].astype(f32) + attn_out).astype(bf16)
        h_scr[part] = resid
        gath[0, part, mine] = resid
        if part == 0:
            late[1].start()
            pl.semaphore_wait(barrier, 4)
        if part == 1:
            for load in loads:
                load.start()
        near_copy(1, part).start()
        near_copy(2, part).start()
        if part > 0:
            near_copy(3, part - 1).start()
    near_copy(3, CHUNKS - 1).start()
    far_copy(0).start()

    def normed_rows(rel, at):
        square = jnp.zeros((2 * rows, 1), f32)
        for part in range(CHUNKS):
            piece = gath[rel, part].astype(f32)
            square = square + jnp.sum(piece * piece, axis=-1, keepdims=True)
        factor = lax.rsqrt(square / width + 1e-6)
        for part in range(CHUNKS):
            piece = gath[rel, part].astype(f32) * factor * gm_ref[columns(part)].astype(f32)
            m_scr[pl.ds(at, 2 * rows), columns(part)] = piece.astype(bf16)

    def activation(count, between=()):
        block = m_scr[pl.ds(0, count)]
        gate = jnp.dot(block, wg[...], preferred_element_type=f32)
        for rel, half in between:
            send_sum(rel, half)
        up = jnp.dot(block, wu[...], preferred_element_type=f32)
        return (jax.nn.silu(gate) * up).astype(bf16)

    half_width = width // 2

    def contract(act, rels):
        for half in range(2):
            part = jnp.dot(act, wd[:, pl.ds(half * half_width, half_width)], preferred_element_type=f32)
            for index, rel in enumerate(rels):
                low = part[2 * index * rows:(2 * index + 1) * rows]
                high = part[(2 * index + 1) * rows:(2 * index + 2) * rows]
                s1_send[rel, half] = jnp.where(is_low, high, low)
                keep[rel, half] = jnp.where(is_low, low, high)
                pair_copy(rel, half).start()

    def send_sum(rel, half):
        pair_copy(rel, half).wait_recv()
        s2_send[rel, half] = (keep[rel, half] + s1_recv[rel, half]).astype(bf16)
        chip_copy(rel, half).start()

    for rel in (1, 2):
        for part in range(CHUNKS):
            near_copy(rel, part).wait_recv()
        forward_copy(rel).start()
    for load in loads:
        load.wait()
    forward_arrived(1)
    normed_rows(1, 0)
    forward_arrived(2)
    normed_rows(2, 2 * rows)
    contract(activation(4 * rows), (1, 2))
    for part in range(CHUNKS):
        near_copy(3, part).wait_recv()
    forward_copy(3).start()
    sibling_rows_arrived()
    normed_rows(0, 2 * rows)

    forward_arrived(3)
    normed_rows(3, 0)
    contract(activation(4 * rows, ((1, 0), (2, 0), (1, 1), (2, 1))), (3, 0))
    send_sum(3, 0)
    send_sum(3, 1)
    totals = []
    for half in range(2):
        pair_copy(0, half).wait_recv()
        residual = jnp.concatenate([h_scr[2 * half].astype(f32), h_scr[2 * half + 1].astype(f32)], axis=1)
        totals.append(residual + (keep[0, half] + s1_recv[0, half]))
    for rel in (1, 2, 3):
        for half in range(2):
            chip_copy(rel, half).wait_recv()
            totals[half] = totals[half] + s2_recv[rel, half].astype(f32)
    for half in range(2):
        out_ref[:, half * half_width:(half + 1) * half_width] = totals[half].astype(bf16)
    for rel in (1, 2, 3):
        for part in range(CHUNKS):
            near_copy(rel, part).wait_send()
    far_copy(0).wait_send()
    for half in range(2):
        for rel in range(4):
            pair_copy(rel, half).wait_send()
        for rel in (1, 2, 3):
            chip_copy(rel, half).wait_send()
    for rel in (1, 2, 3):
        forward_copy(rel).wait_send()


def mlp_call(o_lat, hidden, w_uv, wo_low, gain_mlp, w_o, w_gate, w_up, w_down):
    rows, width = hidden.shape
    cols = w_gate.shape[1]
    bf16, f32 = jnp.bfloat16, jnp.float32
    vmem = pl.BlockSpec(memory_space=pltpu.VMEM)
    hbm = pl.BlockSpec(memory_space=pltpu.HBM)
    dma = pltpu.SemaphoreType.DMA
    part_width = width // CHUNKS
    held = [pltpu.with_memory_space_constraint(x, pltpu.VMEM) for x in (o_lat, hidden, w_uv, wo_low)]
    streamed = [pltpu.with_memory_space_constraint(x, pltpu.HBM) for x in (w_o, w_gate, w_up, w_down)]
    return pl.pallas_call(
        mlp_kernel,
        out_shape=pltpu.VMEM((rows, width), bf16),
        in_specs=[vmem, vmem, vmem, vmem, hbm, hbm, hbm, hbm, hbm],
        out_specs=vmem,
        scratch_shapes=[
            pltpu.VMEM(gain_mlp.shape, bf16),
            pltpu.VMEM((2, w_o.shape[0], part_width), bf16),
            pltpu.VMEM((width, cols), bf16),
            pltpu.VMEM((width, cols), bf16),
            pltpu.VMEM((cols, width), bf16),
            pltpu.VMEM((rows, w_o.shape[0]), bf16),
            pltpu.VMEM((CHUNKS, rows, part_width), bf16),
            pltpu.VMEM((4, CHUNKS, 2 * rows, part_width), bf16),
            pltpu.VMEM((4 * rows, width), bf16),
            pltpu.VMEM((4, 2, rows, width // 2), f32),
            pltpu.VMEM((4, 2, rows, width // 2), f32),
            pltpu.VMEM((4, 2, rows, width // 2), f32),
            pltpu.VMEM((4, 2, rows, width // 2), bf16),
            pltpu.VMEM((4, 2, rows, width // 2), bf16),
            dma((4,)), dma((2,)), dma((4, CHUNKS)), dma((4, CHUNKS)), dma((4,)), dma((4,)), dma((4,)), dma((4,)), dma((4, 2)), dma((4, 2)), dma((4, 2)), dma((4, 2)),
        ],
        compiler_params=pltpu.CompilerParams(collective_id=0, has_side_effects=True, vmem_limit_bytes=VMEM_LIMIT),
        name="mlp_exchange",
    )(*held, gain_mlp, *streamed)


def solution(mesh):
    row_spec = P(("rep", "g"))
    full_spec = P()
    in_specs = (row_spec, row_spec, row_spec, row_spec, full_spec, full_spec, full_spec, full_spec, full_spec, full_spec, full_spec, full_spec, full_spec, full_spec, full_spec, P(None, "g"), P(None, "g"), P("g", None))

    def local_step(hidden, cache_lat, cache_rope, seq_lens, gain_attn, w_dq, gain_q, w_uq, w_qr, w_dkv, gain_kv, w_uk, w_uv, w_o, gain_mlp, w_gate, w_up, w_down):
        new_lat, new_rope, o_lat, hid_rows, uv_held, wo_held = attn_call(hidden, cache_lat, cache_rope, seq_lens, gain_attn, w_dq, gain_q, w_uq, w_qr, w_dkv, gain_kv, w_uk, w_uv, w_o)
        out_hidden = mlp_call(o_lat, hid_rows, uv_held, wo_held, gain_mlp, w_o, w_gate, w_up, w_down)
        return out_hidden, new_lat, new_rope

    return jax.shard_map(local_step, mesh=mesh, in_specs=in_specs, out_specs=(row_spec, row_spec, row_spec), check_vma=False)
```

```python
import functools

import jax
import jax.numpy as jnp
from jax import lax
from jax.experimental import pallas as pl
from jax.experimental.pallas import tpu as pltpu
from jax.sharding import PartitionSpec as P


HEADS = 20
HEAD_PAD = 24
RING = 20
GROUP = 4
SPANS = (384, 512, 640, 768, 896, 1024)
VMEM_LIMIT = 39 * 1024 * 1024
WO_PARTS = 16
WO_STEP = 3


def attn_kernel(lens_hbm, hid_hbm, ga_hbm, gq_hbm, gkv_hbm, lat_hbm, rope_hbm, wdq_hbm, wdkv_hbm, wqr_hbm, wuq_hbm, wuk_hbm, wuv_hbm, wo_hbm,
                newlat_hbm, newrope_hbm, o_scr, hid_ref, wuv, wo,
                wdq, wdkv, wuk, lat_buf, rope_buf, q_scr, qr_scr, nl_scr, nr_scr, s_scr,
                ga_ref, gq_ref, gkv_ref, newlat_ref, newrope_ref, lens_ref, order, fill, w_sems, o_sems, in_sems, new_sems, lat_sems, rope_sems):
    rows = hid_ref.shape[0]
    kv_dim = lat_buf.shape[2]
    rope_dim = rope_buf.shape[1]
    cache_len = lat_buf.shape[1]
    nope_dim = wuk.shape[1]
    q_dim = wdq.shape[1]
    half = rope_dim // 2
    groups = rows // GROUP
    f32, bf16 = jnp.float32, jnp.bfloat16
    nt = (((1,), (1,)), ((), ()))

    wqr = wo.at[pl.ds(HEADS * nope_dim, HEADS * rope_dim), pl.ds(0, q_dim)]
    cut = 8 * nope_dim
    uq_low = wo.at[pl.ds(0, cut), pl.ds(0, q_dim)]
    uq_high = wo.at[pl.ds(cut, HEADS * nope_dim - cut), pl.ds(0, q_dim)]
    pairs = ((wdq_hbm, wdq), (wdkv_hbm, wdkv), (wqr_hbm, wqr), (wuq_hbm.at[pl.ds(0, cut)], uq_low), (wuq_hbm.at[pl.ds(cut, HEADS * nope_dim - cut)], uq_high), (wuk_hbm, wuk))
    early = [pltpu.make_async_copy(src, dst, w_sems.at[k]) for k, (src, dst) in enumerate(pairs)]
    small = [pltpu.make_async_copy(src, dst, in_sems.at[k]) for k, (src, dst) in enumerate(((lens_hbm, lens_ref), (hid_hbm, hid_ref), (ga_hbm, ga_ref), (gq_hbm, gq_ref), (gkv_hbm, gkv_ref)))]
    for copy in small + early[:2]:
        copy.start()
    small[0].wait()

    def bucket(row):
        return 8 - ((lens_ref[row] + 127) >> 7)

    for k in range(9):
        fill[k] = 0

    def count(row, _):
        k = bucket(row)
        fill[k] = fill[k] + 1
        return 0

    lax.fori_loop(0, rows, count, 0)
    running = jnp.int32(0)
    for k in range(9):
        size = fill[k]
        fill[k] = running
        running = running + size

    def place(row, _):
        k = bucket(row)
        order[fill[k]] = row
        fill[k] = fill[k] + 1
        return 0

    lax.fori_loop(0, rows, place, 0)

    def group_blocks(group):
        return (lens_ref[order[group * GROUP]] + 127) >> 7

    def group_copies(group):
        count = pl.multiple_of(jnp.maximum(group_blocks(group), SPANS[0] // 128) << 7, 128)
        base = lax.rem(group * GROUP, RING)
        copies = []
        for sub in range(GROUP):
            row, slot = order[group * GROUP + sub], base + sub
            copies.append(pltpu.make_async_copy(lat_hbm.at[row, pl.ds(0, count)], lat_buf.at[slot, pl.ds(0, count)], lat_sems.at[slot]))
            copies.append(pltpu.make_async_copy(rope_hbm.at[row, :, pl.ds(0, count)], rope_buf.at[slot, :, pl.ds(0, count)], rope_sems.at[slot]))
        return copies

    def start_group(group):
        for copy in group_copies(group):
            copy.start()

    wo_rows = wo.shape[0] // WO_PARTS

    def wo_copy(part):
        span = pl.ds(pl.multiple_of(part * wo_rows, 32), wo_rows)
        return pltpu.make_async_copy(wo_hbm.at[span, pl.ds(0, wo.shape[1])], wo.at[span], o_sems.at[1])

    uv_copy = pltpu.make_async_copy(wuv_hbm, wuv, o_sems.at[0])

    def norm(values, gain_ref):
        mean_sq = jnp.mean(values * values, axis=-1, keepdims=True)
        return values * lax.rsqrt(mean_sq + 1e-6) * gain_ref[...].astype(f32)

    row_id = lax.broadcasted_iota(jnp.int32, (rows, 128), 0)
    position = jnp.zeros((rows, 128), jnp.int32)
    for row in range(rows):
        position = jnp.where(row_id == row, lens_ref[row], position)
    lane = lax.broadcasted_iota(jnp.int32, (rows, 128), 1)
    freq_id = lane & (half - 1)
    inv_freq = jnp.exp(freq_id.astype(f32) * (-jnp.log(jnp.float32(10000.0)) / half))
    angle = position.astype(f32) * inv_freq
    first_half = (lane & half) == 0
    cos_part = jnp.cos(angle)
    sin_part = jnp.where(first_half, -jnp.sin(angle), jnp.sin(angle))

    def rotate(values):
        swapped = jnp.where(first_half, pltpu.roll(values, 128 - half, 1), pltpu.roll(values, half, 1))
        return values * cos_part + swapped * sin_part

    small[1].wait()
    small[2].wait()
    hidden = hid_ref[...].astype(f32)
    normed = norm(hidden, ga_ref).astype(bf16)
    q_scr[...] = jnp.zeros_like(q_scr)
    qr_scr[...] = jnp.zeros_like(qr_scr)

    small[3].wait()
    small[4].wait()
    early[2].start()
    early[3].start()
    early[0].wait()
    early[4].start()
    early[5].start()
    q_raw = jnp.dot(normed, wdq[...], preferred_element_type=f32)
    early[1].wait()
    start_group(0)
    kv_raw = lax.dot_general(normed, wdkv[...], nt, preferred_element_type=f32)
    q_in = norm(q_raw, gq_ref).astype(bf16)
    early[2].wait()
    rope_raw = lax.dot_general(q_in, wo[pl.ds(HEADS * nope_dim, HEADS * rope_dim), pl.ds(0, q_dim)], nt, preferred_element_type=f32)
    new_lat = norm(kv_raw[:, :kv_dim], gkv_ref).astype(bf16)
    newlat_ref[...] = new_lat
    nl_scr[...] = new_lat.astype(f32)
    kv_rope = jnp.concatenate([kv_raw[:, kv_dim:], jnp.zeros((rows, 128 - rope_dim), f32)], axis=1)
    new_rope = rotate(kv_rope).astype(bf16)
    newrope_ref[...] = new_rope[:, :rope_dim]
    outgoing = [pltpu.make_async_copy(newlat_ref, newlat_hbm, new_sems.at[0]), pltpu.make_async_copy(newrope_ref, newrope_hbm, new_sems.at[1])]
    nr_scr[...] = jnp.where(lane < rope_dim, new_rope.astype(f32), 0.0)

    def nope_quad(quad):
        return lax.dot_general(q_in, wo[pl.ds(quad * 4 * nope_dim, 4 * nope_dim), pl.ds(0, q_dim)], nt, preferred_element_type=f32)

    def absorb_quad(quad, q_nope):
        for sub in range(4):
            head = quad * 4 + sub
            one = q_nope[:, sub * nope_dim:(sub + 1) * nope_dim].astype(bf16)
            q_abs = jnp.dot(one, wuk[head], preferred_element_type=f32).astype(bf16).astype(f32)
            for col in range(kv_dim // 128):
                q_scr[col, pl.ds(head, rows, stride=HEAD_PAD), :] = q_abs[:, col * 128:(col + 1) * 128]

    early[3].wait()
    start_group(1)
    quads = HEADS // 4
    ahead = nope_quad(0)
    for pair in range(HEADS // 2):
        turned = rotate(rope_raw[:, pair * 128:(pair + 1) * 128]).astype(bf16).astype(f32)
        qr_scr[pl.ds(2 * pair, rows, stride=HEAD_PAD), :] = turned
        qr_scr[pl.ds(2 * pair + 1, rows, stride=HEAD_PAD), :] = pltpu.roll(turned, rope_dim, 1)
    ahead2 = nope_quad(1)
    early[4].wait()
    start_group(2)
    pending_quads = [ahead, ahead2, nope_quad(2)]
    early[5].wait()
    for quad in range(quads):
        absorb_quad(quad, pending_quads[quad])
        if quad + 3 < quads:
            pending_quads.append(nope_quad(quad + 3))

    for copy in outgoing:
        copy.start()
    scale = (nope_dim + rope_dim) ** -0.5

    def head_rows(row):
        return pl.ds(pl.multiple_of(row * HEAD_PAD, 8), HEAD_PAD)

    def query(row):
        return jnp.concatenate([q_scr[col, head_rows(row), :] for col in range(kv_dim // 128)], axis=1)

    def score_part(row, slot, span):
        lat = lat_buf[slot, pl.ds(0, span)]
        score = lax.dot_general(query(row).astype(bf16), lat, nt, preferred_element_type=f32)
        q_rope = qr_scr[head_rows(row), :][:, :rope_dim].astype(bf16)
        return score + jnp.dot(q_rope, rope_buf[slot, :, pl.ds(0, span)], preferred_element_type=f32)

    def soft_part(row, score):
        key_pos = lax.broadcasted_iota(jnp.int32, score.shape, 1)
        score = jnp.where(key_pos < lens_ref[row], score * scale, -jnp.inf)
        q_rope = qr_scr[head_rows(row), :]
        own = jnp.sum(query(row) * nl_scr[pl.ds(row, 1), :], axis=-1, keepdims=True) + jnp.sum(q_rope * nr_scr[pl.ds(row, 1), :], axis=-1, keepdims=True)
        own = own * scale
        top = jnp.maximum(jnp.max(score, axis=-1, keepdims=True), own)
        weight = jnp.exp(score - top)
        own_weight = jnp.exp(own - top)
        total = jnp.sum(weight, axis=-1, keepdims=True) + own_weight
        return (weight / total).astype(bf16), (own_weight / total).astype(bf16).astype(f32)

    def mix_part(row, slot, prob, own_prob, span):
        mixed = jnp.dot(prob, lat_buf[slot, pl.ds(0, span)], preferred_element_type=f32) + own_prob * nl_scr[pl.ds(row, 1), :]
        mixed = mixed.astype(bf16).astype(f32)
        for col in range(kv_dim // 128):
            o_scr[col, head_rows(row), :] = mixed[:, col * 128:(col + 1) * 128]

    def members(group):
        return [(order[group * GROUP + sub], lax.rem(group * GROUP, RING) + sub) for sub in range(GROUP)]

    def wait_members(group):
        for copy in group_copies(group):
            copy.wait()

    def by_span(blocks, run, spans):
        for index, span in enumerate(spans):
            low = spans[index - 1] // 128 if index else 0
            pl.when((blocks > low) & (blocks <= span // 128))(functools.partial(run, span))

    first = members(0)
    wait_members(0)
    start_group(3)

    def first_scores(span):
        for sub, (row, slot) in enumerate(first):
            s_scr[sub, :, pl.ds(0, span)] = score_part(row, slot, span)

    by_span(group_blocks(0), first_scores, (512, 768, 1024))

    def group_step(group, _):
        now = members(group)
        later = members(group + 1)
        wait_members(group + 1)
        pl.when(group + 4 < groups)(lambda: start_group(group + 4))
        pl.when(group == 0)(uv_copy.start)
        for extra in range(WO_STEP):
            part = group * WO_STEP + extra
            pl.when(part < WO_PARTS)(lambda part=part: wo_copy(part).start())

        def run(span):
            pending = None
            for sub in range(GROUP):
                fresh = score_part(*later[sub], span)
                probs = soft_part(now[sub][0], s_scr[sub, :, pl.ds(0, span)])
                s_scr[sub, :, pl.ds(0, span)] = fresh
                if pending is not None:
                    mix_part(*pending, span)
                pending = (*now[sub], *probs)
            mix_part(*pending, span)

        by_span(group_blocks(group), run, SPANS)

        return 0

    lax.fori_loop(0, groups - 1, group_step, 0)
    last = members(groups - 1)

    def last_mix(span):
        pending = None
        for sub in range(GROUP):
            probs = soft_part(last[sub][0], s_scr[sub, :, pl.ds(0, span)])
            if pending is not None:
                mix_part(*pending, span)
            pending = (*last[sub], *probs)
        mix_part(*pending, span)

    by_span(group_blocks(groups - 1), last_mix, SPANS)
    uv_copy.wait()
    pltpu.make_async_copy(wo_hbm.at[:, pl.ds(0, wo.shape[1])], wo, o_sems.at[1]).wait()
    for copy in outgoing:
        copy.wait()


def attn_call(hidden, cache_lat, cache_rope, seq_lens, gain_attn, w_dq, gain_q, w_uq, w_qr, w_dkv, gain_kv, w_uk, w_uv, w_o):
    rows, width = hidden.shape
    cache_len, kv_dim = cache_lat.shape[1:]
    rope_dim = cache_rope.shape[2]
    q_dim, heads, nope_dim = w_uq.shape
    bf16, f32 = jnp.bfloat16, jnp.float32
    vmem = pl.BlockSpec(memory_space=pltpu.VMEM)
    hbm = pl.BlockSpec(memory_space=pltpu.HBM)
    dma = pltpu.SemaphoreType.DMA
    rope_keys = jnp.swapaxes(cache_rope, 1, 2)
    dkv_t = w_dkv.T
    qr_t = jnp.transpose(w_qr, (1, 2, 0)).reshape(heads * rope_dim, q_dim)
    uq_t = jnp.transpose(w_uq, (1, 2, 0)).reshape(heads * nope_dim, q_dim)
    uk_t = jnp.transpose(w_uk, (1, 2, 0))
    uv_t = jnp.swapaxes(w_uv, 0, 1)
    handed = (
        pltpu.VMEM((kv_dim // 128, rows * HEAD_PAD, 128), f32),
        pltpu.VMEM(hidden.shape, bf16),
        pltpu.VMEM(uv_t.shape, bf16),
        pltpu.VMEM((w_o.shape[0], width * 3 // 4), bf16),
    )
    return pl.pallas_call(
        attn_kernel,
        out_shape=(jax.ShapeDtypeStruct((rows, kv_dim), bf16), jax.ShapeDtypeStruct((rows, rope_dim), bf16)) + handed,
        in_specs=[hbm] * 14,
        out_specs=(hbm, hbm, vmem, vmem, vmem, vmem),
        scratch_shapes=[
            pltpu.VMEM(w_dq.shape, bf16),
            pltpu.VMEM(dkv_t.shape, bf16),
            pltpu.VMEM(uk_t.shape, bf16),
            pltpu.VMEM((RING, cache_len, kv_dim), bf16),
            pltpu.VMEM((RING, rope_dim, cache_len), bf16),
            pltpu.VMEM((kv_dim // 128, rows * HEAD_PAD, 128), f32),
            pltpu.VMEM((rows * HEAD_PAD, 128), f32),
            pltpu.VMEM((rows, kv_dim), f32),
            pltpu.VMEM((rows, 128), f32),
            pltpu.VMEM((GROUP, HEAD_PAD, cache_len), f32),
            pltpu.VMEM(gain_attn.shape, bf16),
            pltpu.VMEM(gain_q.shape, bf16),
            pltpu.VMEM(gain_kv.shape, bf16),
            pltpu.VMEM((rows, kv_dim), bf16),
            pltpu.VMEM((rows, rope_dim), bf16),
            pltpu.SMEM((rows,), jnp.int32),
            pltpu.SMEM((rows,), jnp.int32),
            pltpu.SMEM((9,), jnp.int32),
            dma((6,)), dma((2,)), dma((5,)), dma((2,)), dma((RING,)), dma((RING,)),
        ],
        compiler_params=pltpu.CompilerParams(vmem_limit_bytes=VMEM_LIMIT),
        name="attention",
    )(seq_lens, hidden, gain_attn, gain_q, gain_kv, cache_lat, rope_keys, w_dq, dkv_t, qr_t, uq_t, uk_t, uv_t, w_o)


MESH = pl.DeviceIdType.MESH
CHUNKS = 4


def mlp_kernel(o_ref, hid_ref, wuv, wo_low, gm_hbm, wo_hbm, wg_hbm, wu_hbm, wd_hbm, out_ref,
               gm_ref, wo_high, wg, wu, wd, heads_scr, h_scr, gath, m_scr, keep, s1_send, s1_recv, s2_send, s2_recv,
               w_sems, wo_sems, near_send, near_recv, far_send, far_recv, fw_send, fw_recv, p1_send, p1_recv, p2_send, p2_recv):
    rows, width = hid_ref.shape
    part_width = width // CHUNKS
    heads, kv_dim, v_dim = wuv.shape
    f32, bf16 = jnp.float32, jnp.bfloat16
    me = lax.axis_index("g")
    core = lax.rem(me, 2)
    chip_x = lax.rem(me // 2, 2)
    chip_y = me // 4
    is_low = core == 0
    sibling = me + 1 - 2 * core
    mine = pl.ds(pl.multiple_of(core * rows, rows), rows)
    theirs = pl.ds(pl.multiple_of((1 - core) * rows, rows), rows)

    def peer(rel):
        return me + (rel % 2) * (2 - 4 * chip_x) + (rel // 2) * (4 - 8 * chip_y)

    def remote(src, dst, send, recv, target):
        return pltpu.make_async_remote_copy(src, dst, send, recv, device_id={"g": target}, device_id_type=MESH)

    def near_copy(rel, part):
        return remote(h_scr.at[part], gath.at[rel, part, mine], near_send.at[rel, part], near_recv.at[rel, part], peer(rel))

    def far_copy(rel):
        return remote(h_scr, gath.at[rel, :, mine], far_send.at[rel], far_recv.at[rel], sibling)

    def sibling_rows_arrived():
        remote(h_scr, gath.at[0, :, theirs], far_send.at[0], far_recv.at[0], sibling).wait_recv()

    def forward_copy(rel):
        return remote(gath.at[rel, :, mine], gath.at[rel, :, mine], fw_send.at[rel], fw_recv.at[rel], sibling)

    def forward_arrived(rel):
        remote(gath.at[rel, :, theirs], gath.at[rel, :, theirs], fw_send.at[rel], fw_recv.at[rel], sibling).wait_recv()

    def pair_copy(rel, half):
        return remote(s1_send.at[rel, half], s1_recv.at[rel, half], p1_send.at[rel, half], p1_recv.at[rel, half], sibling)

    def chip_copy(rel, half):
        return remote(s2_send.at[rel, half], s2_recv.at[rel, half], p2_send.at[rel, half], p2_recv.at[rel, half], peer(rel))

    held_width = wo_low.shape[1]
    late = [pltpu.make_async_copy(wo_hbm.at[:, pl.ds(held_width + k * part_width, part_width)], wo_high.at[k], wo_sems.at[k]) for k in range(1)]
    loads = [pltpu.make_async_copy(src, dst, w_sems.at[k]) for k, (src, dst) in enumerate(((wg_hbm, wg), (wu_hbm, wu), (wd_hbm, wd), (gm_hbm, gm_ref)))]
    late[0].start()
    barrier = pltpu.get_barrier_semaphore()
    for target in (sibling, peer(1), peer(2), peer(3)):
        pl.semaphore_signal(barrier, inc=1, device_id={"g": target}, device_id_type=MESH)

    for head in range(heads):
        cols = [o_ref[col, pl.ds(head, rows, stride=HEAD_PAD), :] for col in range(kv_dim // 128)]
        mixed = jnp.concatenate(cols, axis=1).astype(bf16)
        heads_scr[:, head * v_dim:(head + 1) * v_dim] = jnp.dot(mixed, wuv[head], preferred_element_type=f32).astype(bf16)

    def columns(part):
        return pl.ds(part * part_width, part_width)

    for part in range(CHUNKS):
        if part < CHUNKS - 1:
            weights = wo_low[:, columns(part)]
        else:
            late[0].wait()
            weights = wo_high[0]
        attn_out = jnp.dot(heads_scr[...], weights, preferred_element_type=f32)
        resid = (hid_ref[:, columns(part)].astype(f32) + attn_out).astype(bf16)
        h_scr[part] = resid
        gath[0, part, mine] = resid
        if part == 0:
            for load in loads:
                load.start()
            pl.semaphore_wait(barrier, 4)
        near_copy(1, part).start()
        near_copy(2, part).start()
        if part > 0:
            near_copy(3, part - 1).start()
    near_copy(3, CHUNKS - 1).start()
    far_copy(0).start()

    def normed_rows(rel, at):
        square = jnp.zeros((2 * rows, 1), f32)
        for part in range(CHUNKS):
            piece = gath[rel, part].astype(f32)
            square = square + jnp.sum(piece * piece, axis=-1, keepdims=True)
        factor = lax.rsqrt(square / width + 1e-6)
        for part in range(CHUNKS):
            piece = gath[rel, part].astype(f32) * factor * gm_ref[columns(part)].astype(f32)
            m_scr[pl.ds(at, 2 * rows), columns(part)] = piece.astype(bf16)

    def activation(count, between=()):
        block = m_scr[pl.ds(0, count)]
        gate = jnp.dot(block, wg[...], preferred_element_type=f32)
        for rel, half in between:
            send_sum(rel, half)
        up = jnp.dot(block, wu[...], preferred_element_type=f32)
        return (jax.nn.silu(gate) * up).astype(bf16)

    half_width = width // 2

    def contract(act, rels):
        for half in range(2):
            part = jnp.dot(act, wd[:, pl.ds(half * half_width, half_width)], preferred_element_type=f32)
            for index, rel in enumerate(rels):
                low = part[2 * index * rows:(2 * index + 1) * rows]
                high = part[(2 * index + 1) * rows:(2 * index + 2) * rows]
                s1_send[rel, half] = jnp.where(is_low, high, low)
                keep[rel, half] = jnp.where(is_low, low, high)
                pair_copy(rel, half).start()

    def send_sum(rel, half):
        pair_copy(rel, half).wait_recv()
        s2_send[rel, half] = (keep[rel, half] + s1_recv[rel, half]).astype(bf16)
        chip_copy(rel, half).start()

    for rel in (1, 2):
        for part in range(CHUNKS):
            near_copy(rel, part).wait_recv()
        forward_copy(rel).start()
    for load in loads:
        load.wait()
    forward_arrived(1)
    normed_rows(1, 0)
    forward_arrived(2)
    normed_rows(2, 2 * rows)
    contract(activation(4 * rows), (1, 2))
    for part in range(CHUNKS):
        near_copy(3, part).wait_recv()
    forward_copy(3).start()
    sibling_rows_arrived()
    normed_rows(0, 2 * rows)

    forward_arrived(3)
    normed_rows(3, 0)
    contract(activation(4 * rows, ((1, 0), (2, 0), (1, 1), (2, 1))), (3, 0))
    send_sum(3, 0)
    send_sum(3, 1)
    totals = []
    for half in range(2):
        pair_copy(0, half).wait_recv()
        residual = jnp.concatenate([h_scr[2 * half].astype(f32), h_scr[2 * half + 1].astype(f32)], axis=1)
        totals.append(residual + (keep[0, half] + s1_recv[0, half]))
    for rel in (1, 2, 3):
        for half in range(2):
            chip_copy(rel, half).wait_recv()
            totals[half] = totals[half] + s2_recv[rel, half].astype(f32)
    for half in range(2):
        out_ref[:, half * half_width:(half + 1) * half_width] = totals[half].astype(bf16)
    for rel in (1, 2, 3):
        for part in range(CHUNKS):
            near_copy(rel, part).wait_send()
    far_copy(0).wait_send()
    for half in range(2):
        for rel in range(4):
            pair_copy(rel, half).wait_send()
        for rel in (1, 2, 3):
            chip_copy(rel, half).wait_send()
    for rel in (1, 2, 3):
        forward_copy(rel).wait_send()


def mlp_call(o_lat, hidden, w_uv, wo_low, gain_mlp, w_o, w_gate, w_up, w_down):
    rows, width = hidden.shape
    cols = w_gate.shape[1]
    bf16, f32 = jnp.bfloat16, jnp.float32
    vmem = pl.BlockSpec(memory_space=pltpu.VMEM)
    hbm = pl.BlockSpec(memory_space=pltpu.HBM)
    dma = pltpu.SemaphoreType.DMA
    part_width = width // CHUNKS
    held = [pltpu.with_memory_space_constraint(x, pltpu.VMEM) for x in (o_lat, hidden, w_uv, wo_low)]
    streamed = [pltpu.with_memory_space_constraint(x, pltpu.HBM) for x in (w_o, w_gate, w_up, w_down)]
    return pl.pallas_call(
        mlp_kernel,
        out_shape=pltpu.VMEM((rows, width), bf16),
        in_specs=[vmem, vmem, vmem, vmem, hbm, hbm, hbm, hbm, hbm],
        out_specs=vmem,
        scratch_shapes=[
            pltpu.VMEM(gain_mlp.shape, bf16),
            pltpu.VMEM((1, w_o.shape[0], part_width), bf16),
            pltpu.VMEM((width, cols), bf16),
            pltpu.VMEM((width, cols), bf16),
            pltpu.VMEM((cols, width), bf16),
            pltpu.VMEM((rows, w_o.shape[0]), bf16),
            pltpu.VMEM((CHUNKS, rows, part_width), bf16),
            pltpu.VMEM((4, CHUNKS, 2 * rows, part_width), bf16),
            pltpu.VMEM((4 * rows, width), bf16),
            pltpu.VMEM((4, 2, rows, width // 2), f32),
            pltpu.VMEM((4, 2, rows, width // 2), f32),
            pltpu.VMEM((4, 2, rows, width // 2), f32),
            pltpu.VMEM((4, 2, rows, width // 2), bf16),
            pltpu.VMEM((4, 2, rows, width // 2), bf16),
            dma((4,)), dma((1,)), dma((4, CHUNKS)), dma((4, CHUNKS)), dma((4,)), dma((4,)), dma((4,)), dma((4,)), dma((4, 2)), dma((4, 2)), dma((4, 2)), dma((4, 2)),
        ],
        compiler_params=pltpu.CompilerParams(collective_id=0, has_side_effects=True, vmem_limit_bytes=VMEM_LIMIT),
        name="mlp_exchange",
    )(*held, gain_mlp, *streamed)


def solution(mesh):
    row_spec = P(("rep", "g"))
    full_spec = P()
    in_specs = (row_spec, row_spec, row_spec, row_spec, full_spec, full_spec, full_spec, full_spec, full_spec, full_spec, full_spec, full_spec, full_spec, full_spec, full_spec, P(None, "g"), P(None, "g"), P("g", None))

    def local_step(hidden, cache_lat, cache_rope, seq_lens, gain_attn, w_dq, gain_q, w_uq, w_qr, w_dkv, gain_kv, w_uk, w_uv, w_o, gain_mlp, w_gate, w_up, w_down):
        new_lat, new_rope, o_lat, hid_rows, uv_held, wo_held = attn_call(hidden, cache_lat, cache_rope, seq_lens, gain_attn, w_dq, gain_q, w_uq, w_qr, w_dkv, gain_kv, w_uk, w_uv, w_o)
        out_hidden = mlp_call(o_lat, hid_rows, uv_held, wo_held, gain_mlp, w_o, w_gate, w_up, w_down)
        return out_hidden, new_lat, new_rope

    return jax.shard_map(local_step, mesh=mesh, in_specs=in_specs, out_specs=(row_spec, row_spec, row_spec), check_vma=False)
```

```python
import functools

import jax
import jax.numpy as jnp
from jax import lax
from jax.experimental import pallas as pl
from jax.experimental.pallas import tpu as pltpu
from jax.sharding import PartitionSpec as P


HEADS = 20
HEAD_PAD = 24
RING = 20
GROUP = 4
SPANS = (384, 512, 640, 768, 896, 1024)
VMEM_LIMIT = 39 * 1024 * 1024
WO_PARTS = 16
WO_STEP = 3


def attn_kernel(lens_hbm, hid_hbm, ga_hbm, gq_hbm, gkv_hbm, lat_hbm, rope_hbm, wdq_hbm, wdkv_hbm, wqr_hbm, wuq_hbm, wuk_hbm, wuv_hbm, wo_hbm,
                newlat_hbm, newrope_hbm, o_scr, hid_ref, wuv, wo,
                wdq, wdkv, wuk, lat_buf, rope_buf, q_scr, qr_scr, nl_scr, nr_scr, s_scr,
                ga_ref, gq_ref, gkv_ref, newlat_ref, newrope_ref, lens_ref, order, fill, w_sems, o_sems, in_sems, new_sems, lat_sems, rope_sems):
    rows = hid_ref.shape[0]
    kv_dim = lat_buf.shape[2]
    rope_dim = rope_buf.shape[1]
    cache_len = lat_buf.shape[1]
    nope_dim = wuk.shape[1]
    q_dim = wdq.shape[1]
    half = rope_dim // 2
    groups = rows // GROUP
    f32, bf16 = jnp.float32, jnp.bfloat16
    nt = (((1,), (1,)), ((), ()))

    wqr = wo.at[pl.ds(HEADS * nope_dim, HEADS * rope_dim), pl.ds(0, q_dim)]
    cut = 8 * nope_dim
    uq_low = wo.at[pl.ds(0, cut), pl.ds(0, q_dim)]
    uq_high = wo.at[pl.ds(cut, HEADS * nope_dim - cut), pl.ds(0, q_dim)]
    pairs = ((wdq_hbm, wdq), (wdkv_hbm, wdkv), (wqr_hbm, wqr), (wuq_hbm.at[pl.ds(0, cut)], uq_low), (wuq_hbm.at[pl.ds(cut, HEADS * nope_dim - cut)], uq_high), (wuk_hbm, wuk))
    early = [pltpu.make_async_copy(src, dst, w_sems.at[k]) for k, (src, dst) in enumerate(pairs)]
    small = [pltpu.make_async_copy(src, dst, in_sems.at[k]) for k, (src, dst) in enumerate(((lens_hbm, lens_ref), (hid_hbm, hid_ref), (ga_hbm, ga_ref), (gq_hbm, gq_ref), (gkv_hbm, gkv_ref)))]
    for copy in small + early[:2]:
        copy.start()
    small[0].wait()

    def bucket(row):
        return 8 - ((lens_ref[row] + 127) >> 7)

    for k in range(9):
        fill[k] = 0

    def count(row, _):
        k = bucket(row)
        fill[k] = fill[k] + 1
        return 0

    lax.fori_loop(0, rows, count, 0)
    running = jnp.int32(0)
    for k in range(9):
        size = fill[k]
        fill[k] = running
        running = running + size

    def place(row, _):
        k = bucket(row)
        order[fill[k]] = row
        fill[k] = fill[k] + 1
        return 0

    lax.fori_loop(0, rows, place, 0)

    def group_blocks(group):
        return (lens_ref[order[group * GROUP]] + 127) >> 7

    def group_copies(group):
        count = pl.multiple_of(jnp.maximum(group_blocks(group), SPANS[0] // 128) << 7, 128)
        base = lax.rem(group * GROUP, RING)
        copies = []
        for sub in range(GROUP):
            row, slot = order[group * GROUP + sub], base + sub
            copies.append(pltpu.make_async_copy(lat_hbm.at[row, pl.ds(0, count)], lat_buf.at[slot, pl.ds(0, count)], lat_sems.at[slot]))
            copies.append(pltpu.make_async_copy(rope_hbm.at[row, :, pl.ds(0, count)], rope_buf.at[slot, :, pl.ds(0, count)], rope_sems.at[slot]))
        return copies

    def start_group(group):
        for copy in group_copies(group):
            copy.start()

    wo_rows = wo.shape[0] // WO_PARTS

    def wo_copy(part):
        span = pl.ds(pl.multiple_of(part * wo_rows, 32), wo_rows)
        return pltpu.make_async_copy(wo_hbm.at[span, pl.ds(0, wo.shape[1])], wo.at[span], o_sems.at[1])

    uv_copy = pltpu.make_async_copy(wuv_hbm, wuv, o_sems.at[0])

    def norm(values, gain_ref):
        mean_sq = jnp.mean(values * values, axis=-1, keepdims=True)
        return values * lax.rsqrt(mean_sq + 1e-6) * gain_ref[...].astype(f32)

    row_id = lax.broadcasted_iota(jnp.int32, (rows, 128), 0)
    position = jnp.zeros((rows, 128), jnp.int32)
    for row in range(rows):
        position = jnp.where(row_id == row, lens_ref[row], position)
    lane = lax.broadcasted_iota(jnp.int32, (rows, 128), 1)
    freq_id = lane & (half - 1)
    inv_freq = jnp.exp(freq_id.astype(f32) * (-jnp.log(jnp.float32(10000.0)) / half))
    angle = position.astype(f32) * inv_freq
    first_half = (lane & half) == 0
    cos_part = jnp.cos(angle)
    sin_part = jnp.where(first_half, -jnp.sin(angle), jnp.sin(angle))

    def rotate(values):
        swapped = jnp.where(first_half, pltpu.roll(values, 128 - half, 1), pltpu.roll(values, half, 1))
        return values * cos_part + swapped * sin_part

    small[1].wait()
    small[2].wait()
    hidden = hid_ref[...].astype(f32)
    normed = norm(hidden, ga_ref).astype(bf16)
    q_scr[...] = jnp.zeros_like(q_scr)
    qr_scr[...] = jnp.zeros_like(qr_scr)

    small[3].wait()
    small[4].wait()
    early[2].start()
    early[3].start()
    early[0].wait()
    early[4].start()
    early[5].start()
    q_raw = jnp.dot(normed, wdq[...], preferred_element_type=f32)
    early[1].wait()
    start_group(0)
    kv_raw = lax.dot_general(normed, wdkv[...], nt, preferred_element_type=f32)
    q_in = norm(q_raw, gq_ref).astype(bf16)
    early[2].wait()
    rope_raw = lax.dot_general(q_in, wo[pl.ds(HEADS * nope_dim, HEADS * rope_dim), pl.ds(0, q_dim)], nt, preferred_element_type=f32)
    new_lat = norm(kv_raw[:, :kv_dim], gkv_ref).astype(bf16)
    newlat_ref[...] = new_lat
    nl_scr[...] = new_lat.astype(f32)
    kv_rope = jnp.concatenate([kv_raw[:, kv_dim:], jnp.zeros((rows, 128 - rope_dim), f32)], axis=1)
    new_rope = rotate(kv_rope).astype(bf16)
    newrope_ref[...] = new_rope[:, :rope_dim]
    outgoing = [pltpu.make_async_copy(newlat_ref, newlat_hbm, new_sems.at[0]), pltpu.make_async_copy(newrope_ref, newrope_hbm, new_sems.at[1])]
    nr_scr[...] = jnp.where(lane < rope_dim, new_rope.astype(f32), 0.0)

    def nope_quad(quad):
        return lax.dot_general(q_in, wo[pl.ds(quad * 4 * nope_dim, 4 * nope_dim), pl.ds(0, q_dim)], nt, preferred_element_type=f32)

    def absorb_quad(quad, q_nope):
        for sub in range(4):
            head = quad * 4 + sub
            one = q_nope[:, sub * nope_dim:(sub + 1) * nope_dim].astype(bf16)
            q_abs = jnp.dot(one, wuk[head], preferred_element_type=f32).astype(bf16).astype(f32)
            for col in range(kv_dim // 128):
                q_scr[col, pl.ds(head, rows, stride=HEAD_PAD), :] = q_abs[:, col * 128:(col + 1) * 128]

    early[3].wait()
    start_group(1)
    quads = HEADS // 4
    ahead = nope_quad(0)
    for pair in range(HEADS // 2):
        turned = rotate(rope_raw[:, pair * 128:(pair + 1) * 128]).astype(bf16).astype(f32)
        qr_scr[pl.ds(2 * pair, rows, stride=HEAD_PAD), :] = turned
        qr_scr[pl.ds(2 * pair + 1, rows, stride=HEAD_PAD), :] = pltpu.roll(turned, rope_dim, 1)
    ahead2 = nope_quad(1)
    early[4].wait()
    start_group(2)
    pending_quads = [ahead, ahead2, nope_quad(2)]
    early[5].wait()
    for quad in range(quads):
        absorb_quad(quad, pending_quads[quad])
        if quad + 3 < quads:
            pending_quads.append(nope_quad(quad + 3))

    for copy in outgoing:
        copy.start()
    scale = (nope_dim + rope_dim) ** -0.5

    def head_rows(row):
        return pl.ds(pl.multiple_of(row * HEAD_PAD, 8), HEAD_PAD)

    def query(row):
        return jnp.concatenate([q_scr[col, head_rows(row), :] for col in range(kv_dim // 128)], axis=1)

    def score_part(row, slot, span):
        lat = lat_buf[slot, pl.ds(0, span)]
        score = lax.dot_general(query(row).astype(bf16), lat, nt, preferred_element_type=f32)
        q_rope = qr_scr[head_rows(row), :][:, :rope_dim].astype(bf16)
        return score + jnp.dot(q_rope, rope_buf[slot, :, pl.ds(0, span)], preferred_element_type=f32)

    def soft_part(row, score):
        key_pos = lax.broadcasted_iota(jnp.int32, score.shape, 1)
        score = jnp.where(key_pos < lens_ref[row], score * scale, -jnp.inf)
        q_rope = qr_scr[head_rows(row), :]
        own = jnp.sum(query(row) * nl_scr[pl.ds(row, 1), :], axis=-1, keepdims=True) + jnp.sum(q_rope * nr_scr[pl.ds(row, 1), :], axis=-1, keepdims=True)
        own = own * scale
        top = jnp.maximum(jnp.max(score, axis=-1, keepdims=True), own)
        weight = jnp.exp(score - top)
        own_weight = jnp.exp(own - top)
        total = jnp.sum(weight, axis=-1, keepdims=True) + own_weight
        return (weight / total).astype(bf16), (own_weight / total).astype(bf16).astype(f32)

    def mix_part(row, slot, prob, own_prob, span):
        mixed = jnp.dot(prob, lat_buf[slot, pl.ds(0, span)], preferred_element_type=f32) + own_prob * nl_scr[pl.ds(row, 1), :]
        mixed = mixed.astype(bf16).astype(f32)
        for col in range(kv_dim // 128):
            o_scr[col, head_rows(row), :] = mixed[:, col * 128:(col + 1) * 128]

    def members(group):
        return [(order[group * GROUP + sub], lax.rem(group * GROUP, RING) + sub) for sub in range(GROUP)]

    def wait_members(group):
        for copy in group_copies(group):
            copy.wait()

    def by_span(blocks, run, spans):
        for index, span in enumerate(spans):
            low = spans[index - 1] // 128 if index else 0
            pl.when((blocks > low) & (blocks <= span // 128))(functools.partial(run, span))

    first = members(0)
    wait_members(0)
    start_group(3)

    def first_scores(span):
        for sub, (row, slot) in enumerate(first):
            s_scr[sub, :, pl.ds(0, span)] = score_part(row, slot, span)

    by_span(group_blocks(0), first_scores, (512, 768, 1024))

    def group_step(group, _):
        now = members(group)
        later = members(group + 1)
        wait_members(group + 1)
        pl.when(group + 4 < groups)(lambda: start_group(group + 4))
        pl.when(group == 0)(uv_copy.start)
        for extra in range(WO_STEP):
            part = group * WO_STEP + extra
            pl.when(part < WO_PARTS)(lambda part=part: wo_copy(part).start())

        def run(span):
            pending = None
            for sub in range(GROUP):
                fresh = score_part(*later[sub], span)
                probs = soft_part(now[sub][0], s_scr[sub, :, pl.ds(0, span)])
                s_scr[sub, :, pl.ds(0, span)] = fresh
                if pending is not None:
                    mix_part(*pending, span)
                pending = (*now[sub], *probs)
            mix_part(*pending, span)

        by_span(group_blocks(group), run, SPANS)

        return 0

    lax.fori_loop(0, groups - 1, group_step, 0)
    last = members(groups - 1)

    def last_mix(span):
        pending = None
        for sub in range(GROUP):
            probs = soft_part(last[sub][0], s_scr[sub, :, pl.ds(0, span)])
            if pending is not None:
                mix_part(*pending, span)
            pending = (*last[sub], *probs)
        mix_part(*pending, span)

    by_span(group_blocks(groups - 1), last_mix, SPANS)
    uv_copy.wait()
    pltpu.make_async_copy(wo_hbm.at[:, pl.ds(0, wo.shape[1])], wo, o_sems.at[1]).wait()
    for copy in outgoing:
        copy.wait()


def attn_call(hidden, cache_lat, cache_rope, seq_lens, gain_attn, w_dq, gain_q, w_uq, w_qr, w_dkv, gain_kv, w_uk, w_uv, w_o):
    rows, width = hidden.shape
    cache_len, kv_dim = cache_lat.shape[1:]
    rope_dim = cache_rope.shape[2]
    q_dim, heads, nope_dim = w_uq.shape
    bf16, f32 = jnp.bfloat16, jnp.float32
    vmem = pl.BlockSpec(memory_space=pltpu.VMEM)
    hbm = pl.BlockSpec(memory_space=pltpu.HBM)
    dma = pltpu.SemaphoreType.DMA
    rope_keys = jnp.swapaxes(cache_rope, 1, 2)
    dkv_t = w_dkv.T
    qr_t = jnp.transpose(w_qr, (1, 2, 0)).reshape(heads * rope_dim, q_dim)
    uq_t = jnp.transpose(w_uq, (1, 2, 0)).reshape(heads * nope_dim, q_dim)
    uk_t = jnp.transpose(w_uk, (1, 2, 0))
    uv_t = jnp.swapaxes(w_uv, 0, 1)
    handed = (
        pltpu.VMEM((kv_dim // 128, rows * HEAD_PAD, 128), f32),
        pltpu.VMEM(hidden.shape, bf16),
        pltpu.VMEM(uv_t.shape, bf16),
        pltpu.VMEM((w_o.shape[0], width * 3 // 4), bf16),
    )
    return pl.pallas_call(
        attn_kernel,
        out_shape=(jax.ShapeDtypeStruct((rows, kv_dim), bf16), jax.ShapeDtypeStruct((rows, rope_dim), bf16)) + handed,
        in_specs=[hbm] * 14,
        out_specs=(hbm, hbm, vmem, vmem, vmem, vmem),
        scratch_shapes=[
            pltpu.VMEM(w_dq.shape, bf16),
            pltpu.VMEM(dkv_t.shape, bf16),
            pltpu.VMEM(uk_t.shape, bf16),
            pltpu.VMEM((RING, cache_len, kv_dim), bf16),
            pltpu.VMEM((RING, rope_dim, cache_len), bf16),
            pltpu.VMEM((kv_dim // 128, rows * HEAD_PAD, 128), f32),
            pltpu.VMEM((rows * HEAD_PAD, 128), f32),
            pltpu.VMEM((rows, kv_dim), f32),
            pltpu.VMEM((rows, 128), f32),
            pltpu.VMEM((GROUP, HEAD_PAD, cache_len), f32),
            pltpu.VMEM(gain_attn.shape, bf16),
            pltpu.VMEM(gain_q.shape, bf16),
            pltpu.VMEM(gain_kv.shape, bf16),
            pltpu.VMEM((rows, kv_dim), bf16),
            pltpu.VMEM((rows, rope_dim), bf16),
            pltpu.SMEM((rows,), jnp.int32),
            pltpu.SMEM((rows,), jnp.int32),
            pltpu.SMEM((9,), jnp.int32),
            dma((6,)), dma((2,)), dma((5,)), dma((2,)), dma((RING,)), dma((RING,)),
        ],
        compiler_params=pltpu.CompilerParams(vmem_limit_bytes=VMEM_LIMIT),
        name="attention",
    )(seq_lens, hidden, gain_attn, gain_q, gain_kv, cache_lat, rope_keys, w_dq, dkv_t, qr_t, uq_t, uk_t, uv_t, w_o)


MESH = pl.DeviceIdType.MESH
CHUNKS = 4


def mlp_kernel(o_ref, hid_ref, wuv, wo_low, gm_hbm, wo_hbm, wg_hbm, wu_hbm, wd_hbm, out_ref,
               gm_ref, wo_high, wg, wu, wd, heads_scr, h_scr, gath, m_scr, keep, s1_send, s1_recv, s2_send, s2_recv,
               w_sems, wo_sems, near_send, near_recv, far_send, far_recv, fw_send, fw_recv, p1_send, p1_recv, p2_send, p2_recv):
    rows, width = hid_ref.shape
    part_width = width // CHUNKS
    heads, kv_dim, v_dim = wuv.shape
    f32, bf16 = jnp.float32, jnp.bfloat16
    me = lax.axis_index("g")
    core = lax.rem(me, 2)
    chip_x = lax.rem(me // 2, 2)
    chip_y = me // 4
    is_low = core == 0
    sibling = me + 1 - 2 * core
    mine = pl.ds(pl.multiple_of(core * rows, rows), rows)
    theirs = pl.ds(pl.multiple_of((1 - core) * rows, rows), rows)

    def peer(rel):
        return me + (rel % 2) * (2 - 4 * chip_x) + (rel // 2) * (4 - 8 * chip_y)

    def remote(src, dst, send, recv, target):
        return pltpu.make_async_remote_copy(src, dst, send, recv, device_id={"g": target}, device_id_type=MESH)

    def near_copy(rel, part):
        return remote(h_scr.at[part], gath.at[rel, part, mine], near_send.at[rel, part], near_recv.at[rel, part], peer(rel))

    def far_copy(rel):
        return remote(h_scr, gath.at[rel, :, mine], far_send.at[rel], far_recv.at[rel], sibling)

    def sibling_rows_arrived():
        remote(h_scr, gath.at[0, :, theirs], far_send.at[0], far_recv.at[0], sibling).wait_recv()

    def forward_copy(rel, part):
        return remote(gath.at[rel, part, mine], gath.at[rel, part, mine], fw_send.at[rel, part], fw_recv.at[rel, part], sibling)

    def pass_on(rel, part):
        near_copy(rel, part).wait_recv()
        forward_copy(rel, part).start()

    def forward_arrived(rel):
        for part in range(CHUNKS):
            remote(gath.at[rel, part, theirs], gath.at[rel, part, theirs], fw_send.at[rel, part], fw_recv.at[rel, part], sibling).wait_recv()

    def pair_copy(rel, half):
        return remote(s1_send.at[rel, half], s1_recv.at[rel, half], p1_send.at[rel, half], p1_recv.at[rel, half], sibling)

    def chip_copy(rel, half):
        return remote(s2_send.at[rel, half], s2_recv.at[rel, half], p2_send.at[rel, half], p2_recv.at[rel, half], peer(rel))

    held_width = wo_low.shape[1]
    late = [pltpu.make_async_copy(wo_hbm.at[:, pl.ds(held_width + k * part_width, part_width)], wo_high.at[k], wo_sems.at[k]) for k in range(1)]
    loads = [pltpu.make_async_copy(src, dst, w_sems.at[k]) for k, (src, dst) in enumerate(((wg_hbm, wg), (wu_hbm, wu), (wd_hbm, wd), (gm_hbm, gm_ref)))]
    loads[3].start()
    late[0].start()
    barrier = pltpu.get_barrier_semaphore()
    for target in (sibling, peer(1), peer(2), peer(3)):
        pl.semaphore_signal(barrier, inc=1, device_id={"g": target}, device_id_type=MESH)

    for head in range(heads):
        cols = [o_ref[col, pl.ds(head, rows, stride=HEAD_PAD), :] for col in range(kv_dim // 128)]
        mixed = jnp.concatenate(cols, axis=1).astype(bf16)
        heads_scr[:, head * v_dim:(head + 1) * v_dim] = jnp.dot(mixed, wuv[head], preferred_element_type=f32).astype(bf16)

    def columns(part):
        return pl.ds(part * part_width, part_width)

    for part in range(CHUNKS):
        if part < CHUNKS - 1:
            weights = wo_low[:, columns(part)]
        else:
            late[0].wait()
            weights = wo_high[0]
        attn_out = jnp.dot(heads_scr[...], weights, preferred_element_type=f32)
        resid = (hid_ref[:, columns(part)].astype(f32) + attn_out).astype(bf16)
        h_scr[part] = resid
        gath[0, part, mine] = resid
        if part == 0:
            for load in loads[:3]:
                load.start()
            pl.semaphore_wait(barrier, 4)
        near_copy(1, part).start()
        near_copy(2, part).start()
        if part > 0:
            near_copy(3, part - 1).start()
    near_copy(3, CHUNKS - 1).start()
    far_copy(0).start()

    def normed_rows(rel, at):
        square = jnp.zeros((2 * rows, 1), f32)
        for part in range(CHUNKS):
            piece = gath[rel, part].astype(f32)
            square = square + jnp.sum(piece * piece, axis=-1, keepdims=True)
        factor = lax.rsqrt(square / width + 1e-6)
        for part in range(CHUNKS):
            piece = gath[rel, part].astype(f32) * factor * gm_ref[columns(part)].astype(f32)
            m_scr[pl.ds(at, 2 * rows), columns(part)] = piece.astype(bf16)

    def activation(at, between):
        block = m_scr[pl.ds(at, 4 * rows)]
        gate = jnp.dot(block, wg[...], preferred_element_type=f32)
        between()
        up = jnp.dot(block, wu[...], preferred_element_type=f32)
        return (jax.nn.silu(gate) * up).astype(bf16)

    half_width = width // 2

    def contract(act, rels):
        for half in range(2):
            part = jnp.dot(act, wd[:, pl.ds(half * half_width, half_width)], preferred_element_type=f32)
            for index, rel in enumerate(rels):
                low = part[2 * index * rows:(2 * index + 1) * rows]
                high = part[(2 * index + 1) * rows:(2 * index + 2) * rows]
                s1_send[rel, half] = jnp.where(is_low, high, low)
                keep[rel, half] = jnp.where(is_low, low, high)
                pair_copy(rel, half).start()

    def send_sum(rel, half):
        pair_copy(rel, half).wait_recv()
        s2_send[rel, half] = (keep[rel, half] + s1_recv[rel, half]).astype(bf16)
        chip_copy(rel, half).start()

    def pass_diagonal():
        for part in range(CHUNKS):
            pass_on(3, part)

    def send_neighbour_sums():
        for half in range(2):
            send_sum(1, half)
            send_sum(2, half)

    for part in range(CHUNKS - 1):
        pass_on(1, part)
        pass_on(2, part)
    loads[3].wait()
    sibling_rows_arrived()
    normed_rows(0, 6 * rows)
    pass_on(1, CHUNKS - 1)
    pass_on(2, CHUNKS - 1)
    for load in loads[:3]:
        load.wait()
    forward_arrived(1)
    normed_rows(1, 0)
    forward_arrived(2)
    normed_rows(2, 2 * rows)
    contract(activation(0, pass_diagonal), (1, 2))

    forward_arrived(3)
    normed_rows(3, 4 * rows)
    contract(activation(4 * rows, send_neighbour_sums), (3, 0))
    send_sum(3, 0)
    send_sum(3, 1)
    totals = []
    for half in range(2):
        pair_copy(0, half).wait_recv()
        residual = jnp.concatenate([h_scr[2 * half].astype(f32), h_scr[2 * half + 1].astype(f32)], axis=1)
        totals.append(residual + (keep[0, half] + s1_recv[0, half]))
    for rel in (1, 2, 3):
        for half in range(2):
            chip_copy(rel, half).wait_recv()
            totals[half] = totals[half] + s2_recv[rel, half].astype(f32)
    for half in range(2):
        out_ref[:, half * half_width:(half + 1) * half_width] = totals[half].astype(bf16)
    for rel in (1, 2, 3):
        for part in range(CHUNKS):
            near_copy(rel, part).wait_send()
    far_copy(0).wait_send()
    for half in range(2):
        for rel in range(4):
            pair_copy(rel, half).wait_send()
        for rel in (1, 2, 3):
            chip_copy(rel, half).wait_send()
    for rel in (1, 2, 3):
        for part in range(CHUNKS):
            forward_copy(rel, part).wait_send()


def mlp_call(o_lat, hidden, w_uv, wo_low, gain_mlp, w_o, w_gate, w_up, w_down):
    rows, width = hidden.shape
    cols = w_gate.shape[1]
    bf16, f32 = jnp.bfloat16, jnp.float32
    vmem = pl.BlockSpec(memory_space=pltpu.VMEM)
    hbm = pl.BlockSpec(memory_space=pltpu.HBM)
    dma = pltpu.SemaphoreType.DMA
    part_width = width // CHUNKS
    held = [pltpu.with_memory_space_constraint(x, pltpu.VMEM) for x in (o_lat, hidden, w_uv, wo_low)]
    streamed = [pltpu.with_memory_space_constraint(x, pltpu.HBM) for x in (w_o, w_gate, w_up, w_down)]
    return pl.pallas_call(
        mlp_kernel,
        out_shape=pltpu.VMEM((rows, width), bf16),
        in_specs=[vmem, vmem, vmem, vmem, hbm, hbm, hbm, hbm, hbm],
        out_specs=vmem,
        scratch_shapes=[
            pltpu.VMEM(gain_mlp.shape, bf16),
            pltpu.VMEM((1, w_o.shape[0], part_width), bf16),
            pltpu.VMEM((width, cols), bf16),
            pltpu.VMEM((width, cols), bf16),
            pltpu.VMEM((cols, width), bf16),
            pltpu.VMEM((rows, w_o.shape[0]), bf16),
            pltpu.VMEM((CHUNKS, rows, part_width), bf16),
            pltpu.VMEM((4, CHUNKS, 2 * rows, part_width), bf16),
            pltpu.VMEM((8 * rows, width), bf16),
            pltpu.VMEM((4, 2, rows, width // 2), f32),
            pltpu.VMEM((4, 2, rows, width // 2), f32),
            pltpu.VMEM((4, 2, rows, width // 2), f32),
            pltpu.VMEM((4, 2, rows, width // 2), bf16),
            pltpu.VMEM((4, 2, rows, width // 2), bf16),
            dma((4,)), dma((1,)), dma((4, CHUNKS)), dma((4, CHUNKS)), dma((4,)), dma((4,)), dma((4, CHUNKS)), dma((4, CHUNKS)), dma((4, 2)), dma((4, 2)), dma((4, 2)), dma((4, 2)),
        ],
        compiler_params=pltpu.CompilerParams(collective_id=0, has_side_effects=True, vmem_limit_bytes=VMEM_LIMIT),
        name="mlp_exchange",
    )(*held, gain_mlp, *streamed)


def solution(mesh):
    row_spec = P(("rep", "g"))
    full_spec = P()
    in_specs = (row_spec, row_spec, row_spec, row_spec, full_spec, full_spec, full_spec, full_spec, full_spec, full_spec, full_spec, full_spec, full_spec, full_spec, full_spec, P(None, "g"), P(None, "g"), P("g", None))

    def local_step(hidden, cache_lat, cache_rope, seq_lens, gain_attn, w_dq, gain_q, w_uq, w_qr, w_dkv, gain_kv, w_uk, w_uv, w_o, gain_mlp, w_gate, w_up, w_down):
        new_lat, new_rope, o_lat, hid_rows, uv_held, wo_held = attn_call(hidden, cache_lat, cache_rope, seq_lens, gain_attn, w_dq, gain_q, w_uq, w_qr, w_dkv, gain_kv, w_uk, w_uv, w_o)
        out_hidden = mlp_call(o_lat, hid_rows, uv_held, wo_held, gain_mlp, w_o, w_gate, w_up, w_down)
        return out_hidden, new_lat, new_rope

    return jax.shard_map(local_step, mesh=mesh, in_specs=in_specs, out_specs=(row_spec, row_spec, row_spec), check_vma=False)
```

```python
import functools

import jax
import jax.numpy as jnp
from jax import lax
from jax.experimental import pallas as pl
from jax.experimental.pallas import tpu as pltpu
from jax.sharding import PartitionSpec as P


HEADS = 20
HEAD_PAD = 24
RING = 20
GROUP = 4
SPANS = (384, 512, 640, 768, 896, 1024)
VMEM_LIMIT = 39 * 1024 * 1024
WO_PARTS = 16
WO_STEP = 3


def attn_kernel(lens_hbm, hid_hbm, ga_hbm, gq_hbm, gkv_hbm, lat_hbm, rope_hbm, wdq_hbm, wdkv_hbm, wqr_hbm, wuq_hbm, wuk_hbm, wuv_hbm, wo_hbm,
                newlat_hbm, newrope_hbm, o_scr, hid_ref, wuv, wo,
                wdq, wdkv, wuk, lat_buf, rope_buf, q_scr, qr_scr, nl_scr, nr_scr, s_scr,
                ga_ref, gq_ref, gkv_ref, newlat_ref, newrope_ref, lens_ref, order, fill, w_sems, o_sems, in_sems, new_sems, lat_sems, rope_sems):
    rows = hid_ref.shape[0]
    kv_dim = lat_buf.shape[2]
    rope_dim = rope_buf.shape[1]
    cache_len = lat_buf.shape[1]
    nope_dim = wuk.shape[1]
    q_dim = wdq.shape[1]
    half = rope_dim // 2
    groups = rows // GROUP
    f32, bf16 = jnp.float32, jnp.bfloat16
    nt = (((1,), (1,)), ((), ()))

    wqr = wo.at[pl.ds(HEADS * nope_dim, HEADS * rope_dim), pl.ds(0, q_dim)]
    cut = 8 * nope_dim
    uq_low = wo.at[pl.ds(0, cut), pl.ds(0, q_dim)]
    uq_high = wo.at[pl.ds(cut, HEADS * nope_dim - cut), pl.ds(0, q_dim)]
    pairs = ((wdq_hbm, wdq), (wdkv_hbm, wdkv), (wqr_hbm, wqr), (wuq_hbm.at[pl.ds(0, cut)], uq_low), (wuq_hbm.at[pl.ds(cut, HEADS * nope_dim - cut)], uq_high), (wuk_hbm, wuk))
    early = [pltpu.make_async_copy(src, dst, w_sems.at[k]) for k, (src, dst) in enumerate(pairs)]
    small = [pltpu.make_async_copy(src, dst, in_sems.at[k]) for k, (src, dst) in enumerate(((lens_hbm, lens_ref), (hid_hbm, hid_ref), (ga_hbm, ga_ref), (gq_hbm, gq_ref), (gkv_hbm, gkv_ref)))]
    for copy in small + early[:2]:
        copy.start()
    small[0].wait()

    def bucket(row):
        return 8 - ((lens_ref[row] + 127) >> 7)

    for k in range(9):
        fill[k] = 0

    def count(row, _):
        k = bucket(row)
        fill[k] = fill[k] + 1
        return 0

    lax.fori_loop(0, rows, count, 0)
    running = jnp.int32(0)
    for k in range(9):
        size = fill[k]
        fill[k] = running
        running = running + size

    def place(row, _):
        k = bucket(row)
        order[fill[k]] = row
        fill[k] = fill[k] + 1
        return 0

    lax.fori_loop(0, rows, place, 0)

    def group_blocks(group):
        return (lens_ref[order[group * GROUP]] + 127) >> 7

    def group_copies(group):
        count = pl.multiple_of(jnp.maximum(group_blocks(group), SPANS[0] // 128) << 7, 128)
        base = lax.rem(group * GROUP, RING)
        copies = []
        for sub in range(GROUP):
            row, slot = order[group * GROUP + sub], base + sub
            copies.append(pltpu.make_async_copy(lat_hbm.at[row, pl.ds(0, count)], lat_buf.at[slot, pl.ds(0, count)], lat_sems.at[slot]))
            copies.append(pltpu.make_async_copy(rope_hbm.at[row, :, pl.ds(0, count)], rope_buf.at[slot, :, pl.ds(0, count)], rope_sems.at[slot]))
        return copies

    def start_group(group):
        for copy in group_copies(group):
            copy.start()

    wo_rows = wo.shape[0] // WO_PARTS

    def wo_copy(part):
        span = pl.ds(pl.multiple_of(part * wo_rows, 32), wo_rows)
        return pltpu.make_async_copy(wo_hbm.at[span, pl.ds(0, wo.shape[1])], wo.at[span], o_sems.at[1])

    uv_copy = pltpu.make_async_copy(wuv_hbm, wuv, o_sems.at[0])

    def norm(values, gain_ref):
        mean_sq = jnp.mean(values * values, axis=-1, keepdims=True)
        return values * lax.rsqrt(mean_sq + 1e-6) * gain_ref[...].astype(f32)

    row_id = lax.broadcasted_iota(jnp.int32, (rows, 128), 0)
    position = jnp.zeros((rows, 128), jnp.int32)
    for row in range(rows):
        position = jnp.where(row_id == row, lens_ref[row], position)
    lane = lax.broadcasted_iota(jnp.int32, (rows, 128), 1)
    freq_id = lane & (half - 1)
    inv_freq = jnp.exp(freq_id.astype(f32) * (-jnp.log(jnp.float32(10000.0)) / half))
    angle = position.astype(f32) * inv_freq
    first_half = (lane & half) == 0
    cos_part = jnp.cos(angle)
    sin_part = jnp.where(first_half, -jnp.sin(angle), jnp.sin(angle))

    def rotate(values):
        swapped = jnp.where(first_half, pltpu.roll(values, 128 - half, 1), pltpu.roll(values, half, 1))
        return values * cos_part + swapped * sin_part

    small[1].wait()
    small[2].wait()
    hidden = hid_ref[...].astype(f32)
    normed = norm(hidden, ga_ref).astype(bf16)
    q_scr[...] = jnp.zeros_like(q_scr)
    qr_scr[...] = jnp.zeros_like(qr_scr)

    small[3].wait()
    small[4].wait()
    early[2].start()
    early[3].start()
    early[0].wait()
    early[4].start()
    early[5].start()
    q_raw = jnp.dot(normed, wdq[...], preferred_element_type=f32)
    early[1].wait()
    start_group(0)
    kv_raw = lax.dot_general(normed, wdkv[...], nt, preferred_element_type=f32)
    q_in = norm(q_raw, gq_ref).astype(bf16)
    early[2].wait()
    rope_raw = lax.dot_general(q_in, wo[pl.ds(HEADS * nope_dim, HEADS * rope_dim), pl.ds(0, q_dim)], nt, preferred_element_type=f32)
    new_lat = norm(kv_raw[:, :kv_dim], gkv_ref).astype(bf16)
    newlat_ref[...] = new_lat
    nl_scr[...] = new_lat.astype(f32)
    kv_rope = jnp.concatenate([kv_raw[:, kv_dim:], jnp.zeros((rows, 128 - rope_dim), f32)], axis=1)
    new_rope = rotate(kv_rope).astype(bf16)
    newrope_ref[...] = new_rope[:, :rope_dim]
    outgoing = [pltpu.make_async_copy(newlat_ref, newlat_hbm, new_sems.at[0]), pltpu.make_async_copy(newrope_ref, newrope_hbm, new_sems.at[1])]
    nr_scr[...] = jnp.where(lane < rope_dim, new_rope.astype(f32), 0.0)

    def nope_quad(quad):
        return lax.dot_general(q_in, wo[pl.ds(quad * 4 * nope_dim, 4 * nope_dim), pl.ds(0, q_dim)], nt, preferred_element_type=f32)

    def absorb_quad(quad, q_nope):
        for sub in range(4):
            head = quad * 4 + sub
            one = q_nope[:, sub * nope_dim:(sub + 1) * nope_dim].astype(bf16)
            q_abs = jnp.dot(one, wuk[head], preferred_element_type=f32).astype(bf16).astype(f32)
            for col in range(kv_dim // 128):
                q_scr[col, pl.ds(head, rows, stride=HEAD_PAD), :] = q_abs[:, col * 128:(col + 1) * 128]

    early[3].wait()
    start_group(1)
    quads = HEADS // 4
    ahead = nope_quad(0)
    for pair in range(HEADS // 2):
        turned = rotate(rope_raw[:, pair * 128:(pair + 1) * 128]).astype(bf16).astype(f32)
        qr_scr[pl.ds(2 * pair, rows, stride=HEAD_PAD), :] = turned
        qr_scr[pl.ds(2 * pair + 1, rows, stride=HEAD_PAD), :] = pltpu.roll(turned, rope_dim, 1)
    ahead2 = nope_quad(1)
    early[4].wait()
    start_group(2)
    pending_quads = [ahead, ahead2, nope_quad(2)]
    early[5].wait()
    for quad in range(quads):
        absorb_quad(quad, pending_quads[quad])
        if quad + 3 < quads:
            pending_quads.append(nope_quad(quad + 3))

    for copy in outgoing:
        copy.start()
    scale = (nope_dim + rope_dim) ** -0.5

    def head_rows(row):
        return pl.ds(pl.multiple_of(row * HEAD_PAD, 8), HEAD_PAD)

    def query(row):
        return jnp.concatenate([q_scr[col, head_rows(row), :] for col in range(kv_dim // 128)], axis=1)

    def score_part(row, slot, span):
        lat = lat_buf[slot, pl.ds(0, span)]
        score = lax.dot_general(query(row).astype(bf16), lat, nt, preferred_element_type=f32)
        q_rope = qr_scr[head_rows(row), :][:, :rope_dim].astype(bf16)
        return score + jnp.dot(q_rope, rope_buf[slot, :, pl.ds(0, span)], preferred_element_type=f32)

    def soft_part(row, score):
        key_pos = lax.broadcasted_iota(jnp.int32, score.shape, 1)
        score = jnp.where(key_pos < lens_ref[row], score * scale, -jnp.inf)
        q_rope = qr_scr[head_rows(row), :]
        own = jnp.sum(query(row) * nl_scr[pl.ds(row, 1), :], axis=-1, keepdims=True) + jnp.sum(q_rope * nr_scr[pl.ds(row, 1), :], axis=-1, keepdims=True)
        own = own * scale
        top = jnp.maximum(jnp.max(score, axis=-1, keepdims=True), own)
        weight = jnp.exp(score - top)
        own_weight = jnp.exp(own - top)
        total = jnp.sum(weight, axis=-1, keepdims=True) + own_weight
        return (weight / total).astype(bf16), (own_weight / total).astype(bf16).astype(f32)

    def mix_part(row, slot, prob, own_prob, span):
        mixed = jnp.dot(prob, lat_buf[slot, pl.ds(0, span)], preferred_element_type=f32) + own_prob * nl_scr[pl.ds(row, 1), :]
        mixed = mixed.astype(bf16).astype(f32)
        for col in range(kv_dim // 128):
            o_scr[col, head_rows(row), :] = mixed[:, col * 128:(col + 1) * 128]

    def members(group):
        return [(order[group * GROUP + sub], lax.rem(group * GROUP, RING) + sub) for sub in range(GROUP)]

    def wait_members(group):
        for copy in group_copies(group):
            copy.wait()

    def by_span(blocks, run, spans):
        for index, span in enumerate(spans):
            low = spans[index - 1] // 128 if index else 0
            pl.when((blocks > low) & (blocks <= span // 128))(functools.partial(run, span))

    first = members(0)
    wait_members(0)
    start_group(3)

    def first_scores(span):
        for sub, (row, slot) in enumerate(first):
            s_scr[sub, :, pl.ds(0, span)] = score_part(row, slot, span)

    by_span(group_blocks(0), first_scores, (512, 768, 1024))

    def group_step(group, _):
        now = members(group)
        later = members(group + 1)
        wait_members(group + 1)
        pl.when(group + 4 < groups)(lambda: start_group(group + 4))
        pl.when(group == 0)(uv_copy.start)
        for extra in range(WO_STEP):
            part = group * WO_STEP + extra
            pl.when(part < WO_PARTS)(lambda part=part: wo_copy(part).start())

        def run(span):
            pending = None
            for sub in range(GROUP):
                fresh = score_part(*later[sub], span)
                probs = soft_part(now[sub][0], s_scr[sub, :, pl.ds(0, span)])
                s_scr[sub, :, pl.ds(0, span)] = fresh
                if pending is not None:
                    mix_part(*pending, span)
                pending = (*now[sub], *probs)
            mix_part(*pending, span)

        by_span(group_blocks(group), run, SPANS)

        return 0

    lax.fori_loop(0, groups - 1, group_step, 0)
    last = members(groups - 1)

    def last_mix(span):
        pending = None
        for sub in range(GROUP):
            probs = soft_part(last[sub][0], s_scr[sub, :, pl.ds(0, span)])
            if pending is not None:
                mix_part(*pending, span)
            pending = (*last[sub], *probs)
        mix_part(*pending, span)

    by_span(group_blocks(groups - 1), last_mix, SPANS)
    uv_copy.wait()
    pltpu.make_async_copy(wo_hbm.at[:, pl.ds(0, wo.shape[1])], wo, o_sems.at[1]).wait()
    for copy in outgoing:
        copy.wait()


def attn_call(hidden, cache_lat, cache_rope, seq_lens, gain_attn, w_dq, gain_q, w_uq, w_qr, w_dkv, gain_kv, w_uk, w_uv, w_o):
    rows, width = hidden.shape
    cache_len, kv_dim = cache_lat.shape[1:]
    rope_dim = cache_rope.shape[2]
    q_dim, heads, nope_dim = w_uq.shape
    bf16, f32 = jnp.bfloat16, jnp.float32
    vmem = pl.BlockSpec(memory_space=pltpu.VMEM)
    hbm = pl.BlockSpec(memory_space=pltpu.HBM)
    dma = pltpu.SemaphoreType.DMA
    rope_keys = jnp.swapaxes(cache_rope, 1, 2)
    dkv_t = w_dkv.T
    qr_t = jnp.transpose(w_qr, (1, 2, 0)).reshape(heads * rope_dim, q_dim)
    uq_t = jnp.transpose(w_uq, (1, 2, 0)).reshape(heads * nope_dim, q_dim)
    uk_t = jnp.transpose(w_uk, (1, 2, 0))
    uv_t = jnp.swapaxes(w_uv, 0, 1)
    handed = (
        pltpu.VMEM((kv_dim // 128, rows * HEAD_PAD, 128), f32),
        pltpu.VMEM(hidden.shape, bf16),
        pltpu.VMEM(uv_t.shape, bf16),
        pltpu.VMEM((w_o.shape[0], width * 3 // 4), bf16),
    )
    return pl.pallas_call(
        attn_kernel,
        out_shape=(jax.ShapeDtypeStruct((rows, kv_dim), bf16), jax.ShapeDtypeStruct((rows, rope_dim), bf16)) + handed,
        in_specs=[hbm] * 14,
        out_specs=(hbm, hbm, vmem, vmem, vmem, vmem),
        scratch_shapes=[
            pltpu.VMEM(w_dq.shape, bf16),
            pltpu.VMEM(dkv_t.shape, bf16),
            pltpu.VMEM(uk_t.shape, bf16),
            pltpu.VMEM((RING, cache_len, kv_dim), bf16),
            pltpu.VMEM((RING, rope_dim, cache_len), bf16),
            pltpu.VMEM((kv_dim // 128, rows * HEAD_PAD, 128), f32),
            pltpu.VMEM((rows * HEAD_PAD, 128), f32),
            pltpu.VMEM((rows, kv_dim), f32),
            pltpu.VMEM((rows, 128), f32),
            pltpu.VMEM((GROUP, HEAD_PAD, cache_len), f32),
            pltpu.VMEM(gain_attn.shape, bf16),
            pltpu.VMEM(gain_q.shape, bf16),
            pltpu.VMEM(gain_kv.shape, bf16),
            pltpu.VMEM((rows, kv_dim), bf16),
            pltpu.VMEM((rows, rope_dim), bf16),
            pltpu.SMEM((rows,), jnp.int32),
            pltpu.SMEM((rows,), jnp.int32),
            pltpu.SMEM((9,), jnp.int32),
            dma((6,)), dma((2,)), dma((5,)), dma((2,)), dma((RING,)), dma((RING,)),
        ],
        compiler_params=pltpu.CompilerParams(vmem_limit_bytes=VMEM_LIMIT),
        name="attention",
    )(seq_lens, hidden, gain_attn, gain_q, gain_kv, cache_lat, rope_keys, w_dq, dkv_t, qr_t, uq_t, uk_t, uv_t, w_o)


MESH = pl.DeviceIdType.MESH
CHUNKS = 4


def mlp_kernel(o_ref, hid_ref, wuv, wo_low, gm_hbm, wo_hbm, wg_hbm, wu_hbm, wd_hbm, out_ref,
               gm_ref, wo_high, wg, wu, wd, heads_scr, h_scr, gath, m_scr, keep, s1_send, s1_recv, s2_send, s2_recv,
               w_sems, wo_sems, near_send, near_recv, far_send, far_recv, fw_send, fw_recv, p1_send, p1_recv, p2_send, p2_recv):
    rows, width = hid_ref.shape
    part_width = width // CHUNKS
    heads, kv_dim, v_dim = wuv.shape
    f32, bf16 = jnp.float32, jnp.bfloat16
    me = lax.axis_index("g")
    core = lax.rem(me, 2)
    chip_x = lax.rem(me // 2, 2)
    chip_y = me // 4
    is_low = core == 0
    sibling = me + 1 - 2 * core
    mine = pl.ds(pl.multiple_of(core * rows, rows), rows)
    theirs = pl.ds(pl.multiple_of((1 - core) * rows, rows), rows)

    def peer(rel):
        return me + (rel % 2) * (2 - 4 * chip_x) + (rel // 2) * (4 - 8 * chip_y)

    def remote(src, dst, send, recv, target):
        return pltpu.make_async_remote_copy(src, dst, send, recv, device_id={"g": target}, device_id_type=MESH)

    def near_copy(rel, part):
        return remote(h_scr.at[part], gath.at[rel, part, mine], near_send.at[rel, part], near_recv.at[rel, part], peer(rel))

    def far_copy(rel):
        return remote(h_scr, gath.at[rel, :, mine], far_send.at[rel], far_recv.at[rel], sibling)

    def sibling_rows_arrived():
        remote(h_scr, gath.at[0, :, theirs], far_send.at[0], far_recv.at[0], sibling).wait_recv()

    def forward_copy(rel, part):
        return remote(gath.at[rel, part, mine], gath.at[rel, part, mine], fw_send.at[rel, part], fw_recv.at[rel, part], sibling)

    def pass_on(rel, part):
        near_copy(rel, part).wait_recv()
        forward_copy(rel, part).start()

    def forward_arrived(rel):
        for part in range(CHUNKS):
            remote(gath.at[rel, part, theirs], gath.at[rel, part, theirs], fw_send.at[rel, part], fw_recv.at[rel, part], sibling).wait_recv()

    def pair_copy(rel, half):
        return remote(s1_send.at[rel, half], s1_recv.at[rel, half], p1_send.at[rel, half], p1_recv.at[rel, half], sibling)

    def chip_copy(rel, half):
        return remote(s2_send.at[rel, half], s2_recv.at[rel, half], p2_send.at[rel, half], p2_recv.at[rel, half], peer(rel))

    held_width = wo_low.shape[1]
    late = [pltpu.make_async_copy(wo_hbm.at[:, pl.ds(held_width + k * part_width, part_width)], wo_high.at[k], wo_sems.at[k]) for k in range(1)]
    loads = [pltpu.make_async_copy(src, dst, w_sems.at[k]) for k, (src, dst) in enumerate(((wg_hbm, wg), (wu_hbm, wu), (wd_hbm, wd), (gm_hbm, gm_ref)))]
    loads[3].start()
    late[0].start()
    barrier = pltpu.get_barrier_semaphore()
    for target in (sibling, peer(1), peer(2), peer(3)):
        pl.semaphore_signal(barrier, inc=1, device_id={"g": target}, device_id_type=MESH)

    for head in range(heads):
        cols = [o_ref[col, pl.ds(head, rows, stride=HEAD_PAD), :] for col in range(kv_dim // 128)]
        mixed = jnp.concatenate(cols, axis=1).astype(bf16)
        heads_scr[:, head * v_dim:(head + 1) * v_dim] = jnp.dot(mixed, wuv[head], preferred_element_type=f32).astype(bf16)

    def columns(part):
        return pl.ds(part * part_width, part_width)

    for part in range(CHUNKS):
        if part < CHUNKS - 1:
            weights = wo_low[:, columns(part)]
        else:
            late[0].wait()
            weights = wo_high[0]
        attn_out = jnp.dot(heads_scr[...], weights, preferred_element_type=f32)
        resid = (hid_ref[:, columns(part)].astype(f32) + attn_out).astype(bf16)
        h_scr[part] = resid
        gath[0, part, mine] = resid
        if part == 0:
            for load in loads[:3]:
                load.start()
            pl.semaphore_wait(barrier, 4)
        near_copy(1, part).start()
        near_copy(2, part).start()
    far_copy(0).start()
    for part in range(CHUNKS):
        near_copy(3, part).start()

    def normed_rows(rel, at):
        square = jnp.zeros((2 * rows, 1), f32)
        for part in range(CHUNKS):
            piece = gath[rel, part].astype(f32)
            square = square + jnp.sum(piece * piece, axis=-1, keepdims=True)
        factor = lax.rsqrt(square / width + 1e-6)
        for part in range(CHUNKS):
            piece = gath[rel, part].astype(f32) * factor * gm_ref[columns(part)].astype(f32)
            m_scr[pl.ds(at, 2 * rows), columns(part)] = piece.astype(bf16)

    def activation(at, between):
        block = m_scr[pl.ds(at, 4 * rows)]
        gate = jnp.dot(block, wg[...], preferred_element_type=f32)
        between()
        up = jnp.dot(block, wu[...], preferred_element_type=f32)
        return (jax.nn.silu(gate) * up).astype(bf16)

    half_width = width // 2

    def contract(act, rels):
        for half in range(2):
            part = jnp.dot(act, wd[:, pl.ds(half * half_width, half_width)], preferred_element_type=f32)
            for index, rel in enumerate(rels):
                low = part[2 * index * rows:(2 * index + 1) * rows]
                high = part[(2 * index + 1) * rows:(2 * index + 2) * rows]
                s1_send[rel, half] = jnp.where(is_low, high, low)
                keep[rel, half] = jnp.where(is_low, low, high)
                pair_copy(rel, half).start()

    def send_sum(rel, half):
        pair_copy(rel, half).wait_recv()
        s2_send[rel, half] = (keep[rel, half] + s1_recv[rel, half]).astype(bf16)
        chip_copy(rel, half).start()

    def pass_diagonal():
        for part in range(CHUNKS):
            pass_on(3, part)

    def send_neighbour_sums():
        for half in range(2):
            send_sum(1, half)
            send_sum(2, half)

    for part in range(CHUNKS - 1):
        pass_on(1, part)
        pass_on(2, part)
    loads[3].wait()
    sibling_rows_arrived()
    normed_rows(0, 6 * rows)
    pass_on(1, CHUNKS - 1)
    pass_on(2, CHUNKS - 1)
    for load in loads[:3]:
        load.wait()
    forward_arrived(1)
    normed_rows(1, 0)
    forward_arrived(2)
    normed_rows(2, 2 * rows)
    contract(activation(0, pass_diagonal), (1, 2))

    forward_arrived(3)
    normed_rows(3, 4 * rows)
    contract(activation(4 * rows, send_neighbour_sums), (3, 0))
    send_sum(3, 0)
    send_sum(3, 1)
    totals = []
    for half in range(2):
        pair_copy(0, half).wait_recv()
        residual = jnp.concatenate([h_scr[2 * half].astype(f32), h_scr[2 * half + 1].astype(f32)], axis=1)
        totals.append(residual + (keep[0, half] + s1_recv[0, half]))
    for rel in (1, 2, 3):
        for half in range(2):
            chip_copy(rel, half).wait_recv()
            totals[half] = totals[half] + s2_recv[rel, half].astype(f32)
    for half in range(2):
        out_ref[:, half * half_width:(half + 1) * half_width] = totals[half].astype(bf16)
    for rel in (1, 2, 3):
        for part in range(CHUNKS):
            near_copy(rel, part).wait_send()
    far_copy(0).wait_send()
    for half in range(2):
        for rel in range(4):
            pair_copy(rel, half).wait_send()
        for rel in (1, 2, 3):
            chip_copy(rel, half).wait_send()
    for rel in (1, 2, 3):
        for part in range(CHUNKS):
            forward_copy(rel, part).wait_send()


def mlp_call(o_lat, hidden, w_uv, wo_low, gain_mlp, w_o, w_gate, w_up, w_down):
    rows, width = hidden.shape
    cols = w_gate.shape[1]
    bf16, f32 = jnp.bfloat16, jnp.float32
    vmem = pl.BlockSpec(memory_space=pltpu.VMEM)
    hbm = pl.BlockSpec(memory_space=pltpu.HBM)
    dma = pltpu.SemaphoreType.DMA
    part_width = width // CHUNKS
    held = [pltpu.with_memory_space_constraint(x, pltpu.VMEM) for x in (o_lat, hidden, w_uv, wo_low)]
    streamed = [pltpu.with_memory_space_constraint(x, pltpu.HBM) for x in (w_o, w_gate, w_up, w_down)]
    return pl.pallas_call(
        mlp_kernel,
        out_shape=pltpu.VMEM((rows, width), bf16),
        in_specs=[vmem, vmem, vmem, vmem, hbm, hbm, hbm, hbm, hbm],
        out_specs=vmem,
        scratch_shapes=[
            pltpu.VMEM(gain_mlp.shape, bf16),
            pltpu.VMEM((1, w_o.shape[0], part_width), bf16),
            pltpu.VMEM((width, cols), bf16),
            pltpu.VMEM((width, cols), bf16),
            pltpu.VMEM((cols, width), bf16),
            pltpu.VMEM((rows, w_o.shape[0]), bf16),
            pltpu.VMEM((CHUNKS, rows, part_width), bf16),
            pltpu.VMEM((4, CHUNKS, 2 * rows, part_width), bf16),
            pltpu.VMEM((8 * rows, width), bf16),
            pltpu.VMEM((4, 2, rows, width // 2), f32),
            pltpu.VMEM((4, 2, rows, width // 2), f32),
            pltpu.VMEM((4, 2, rows, width // 2), f32),
            pltpu.VMEM((4, 2, rows, width // 2), bf16),
            pltpu.VMEM((4, 2, rows, width // 2), bf16),
            dma((4,)), dma((1,)), dma((4, CHUNKS)), dma((4, CHUNKS)), dma((4,)), dma((4,)), dma((4, CHUNKS)), dma((4, CHUNKS)), dma((4, 2)), dma((4, 2)), dma((4, 2)), dma((4, 2)),
        ],
        compiler_params=pltpu.CompilerParams(collective_id=0, has_side_effects=True, vmem_limit_bytes=VMEM_LIMIT),
        name="mlp_exchange",
    )(*held, gain_mlp, *streamed)


def solution(mesh):
    row_spec = P(("rep", "g"))
    full_spec = P()
    in_specs = (row_spec, row_spec, row_spec, row_spec, full_spec, full_spec, full_spec, full_spec, full_spec, full_spec, full_spec, full_spec, full_spec, full_spec, full_spec, P(None, "g"), P(None, "g"), P("g", None))

    def local_step(hidden, cache_lat, cache_rope, seq_lens, gain_attn, w_dq, gain_q, w_uq, w_qr, w_dkv, gain_kv, w_uk, w_uv, w_o, gain_mlp, w_gate, w_up, w_down):
        new_lat, new_rope, o_lat, hid_rows, uv_held, wo_held = attn_call(hidden, cache_lat, cache_rope, seq_lens, gain_attn, w_dq, gain_q, w_uq, w_qr, w_dkv, gain_kv, w_uk, w_uv, w_o)
        out_hidden = mlp_call(o_lat, hid_rows, uv_held, wo_held, gain_mlp, w_o, w_gate, w_up, w_down)
        return out_hidden, new_lat, new_rope

    return jax.shard_map(local_step, mesh=mesh, in_specs=in_specs, out_specs=(row_spec, row_spec, row_spec), check_vma=False)
```
